32 devices in a mesh: data: 2 (over x), model: 16 (over z, y, core).
Axes of the slice: x: 2, y: 2, z: 4, core: 2. Of those that a mesh axis runs over, the one named last changes fastest.
Arguments:
- x_in: bfloat16 [2, 256, 4096], P('data'), parts along dimension 0
- seg_ids: int32 [2, 256], P('data'), parts along dimension 0
- gain_one: bfloat16 [4096], replicated
- w_qkv: bfloat16 [4096, 12288], P(None, 'model')
- w_out: bfloat16 [32, 128, 4096], P('model')
- gain_two: bfloat16 [4096], replicated
- w_up: bfloat16 [4096, 14336], P(None, 'model')
- w_down: bfloat16 [14336, 4096], P('model')
- d_y: bfloat16 [2, 256, 4096], P('data'), parts along dimension 0
Outputs:
- output 1: bfloat16 [2, 256, 4096], P('data'), parts along dimension 0
- output 2: bfloat16 [2, 256, 4096], P('data'), parts along dimension 0
- output 3: bfloat16 [8192, 12288], P('data', 'model'), parts along dimension 0
- output 4: bfloat16 [64, 128, 4096], P(('data', 'model')), parts along dimension 0
- output 5: bfloat16 [8192, 14336], P('data', 'model'), parts along dimension 0
- output 6: bfloat16 [28672, 4096], P(('data', 'model')), parts along dimension 0
- output 7: bfloat16 [8192], P('data'), parts along dimension 0
- output 8: bfloat16 [8192], P('data'), parts along dimension 0
There are 2 independent parts. The reference program is written for one: setup_inputs(seed, part) draws one part's arguments, and reference() takes and returns one part's arrays. A program takes and returns all parts, laid end to end along the dimension named above; an argument that names none is the same for every part.
All inputs are finite; a program needn't handle non-finite values.
Results may differ from the reference program's by a relative error of at most 0.02.
Values are sent between devices in bfloat16 or wider.
A program may use at most 1 GiB of HBM per device.

```python
import jax
import jax.numpy as jnp
from jax import lax

BATCH_ROWS = 1
SEQ_LEN = 256
MODEL_DIM = 4096
NUM_HEADS = 32
HEAD_DIM = 128
FFN_DIM = 14336
LN_EPS = 1e-5
TOKEN_COUNT = BATCH_ROWS * SEQ_LEN
QKV_WIDTH = 3 * NUM_HEADS * HEAD_DIM
INNER_WIDTH = NUM_HEADS * HEAD_DIM


def draw_segments(seg_key):
    seg_keys = jax.random.split(seg_key, 3)
    rate_table = jnp.array([0, 2, 8, 32], jnp.int32)
    row_rate = rate_table[jax.random.randint(seg_keys[0], (BATCH_ROWS,), 0, 4)]
    pos_draws = jax.random.randint(seg_keys[1], (BATCH_ROWS, SEQ_LEN), 0, SEQ_LEN)
    forced_pos = jax.random.randint(seg_keys[2], (BATCH_ROWS,), 1, SEQ_LEN)
    positions = jnp.arange(SEQ_LEN, dtype=jnp.int32)
    breaks = ((pos_draws < row_rate[:, None]) | (positions[None, :] == forced_pos[:, None])).astype(jnp.int32)
    breaks = breaks.at[:, 0].set(0)
    return jnp.cumsum(breaks, axis=1).astype(jnp.int32)


def setup_inputs(seed: int = 0, part: int = 0) -> dict:
    base_key = jax.random.key(seed)
    part_key = jax.random.fold_in(base_key, part)
    weight_keys = jax.random.split(base_key, 6)
    part_keys = jax.random.split(part_key, 4)
    x_in = jax.random.normal(part_keys[0], (BATCH_ROWS, SEQ_LEN, MODEL_DIM), jnp.float32)
    seg_ids = draw_segments(part_keys[1])
    gain_one = 1.0 + 0.3 * jax.random.normal(weight_keys[0], (MODEL_DIM,), jnp.float32)
    gain_two = 1.0 + 0.3 * jax.random.normal(weight_keys[1], (MODEL_DIM,), jnp.float32)
    w_qkv = jax.random.normal(weight_keys[2], (MODEL_DIM, QKV_WIDTH), jnp.float32) * (1.5 * MODEL_DIM ** -0.5)
    w_out = jax.random.normal(weight_keys[3], (NUM_HEADS, HEAD_DIM, MODEL_DIM), jnp.float32) * INNER_WIDTH ** -0.5
    w_up = jax.random.normal(weight_keys[4], (MODEL_DIM, FFN_DIM), jnp.float32) * MODEL_DIM ** -0.5
    w_down = jax.random.normal(weight_keys[5], (FFN_DIM, MODEL_DIM), jnp.float32) * FFN_DIM ** -0.5
    d_y = jax.random.normal(part_keys[3], (BATCH_ROWS, SEQ_LEN, MODEL_DIM), jnp.float32)
    return {'x_in': x_in.astype(jnp.bfloat16), 'seg_ids': seg_ids, 'gain_one': gain_one.astype(jnp.bfloat16), 'w_qkv': w_qkv.astype(jnp.bfloat16), 'w_out': w_out.astype(jnp.bfloat16), 'gain_two': gain_two.astype(jnp.bfloat16), 'w_up': w_up.astype(jnp.bfloat16), 'w_down': w_down.astype(jnp.bfloat16), 'd_y': d_y.astype(jnp.bfloat16)}


def layer_norm(x_in, gain):
    x_wide = x_in.astype(jnp.float32)
    row_mean = jnp.mean(x_wide, axis=-1, keepdims=True)
    centered = x_wide - row_mean
    row_var = jnp.mean(centered * centered, axis=-1, keepdims=True)
    return (centered * lax.rsqrt(row_var + LN_EPS) * gain.astype(jnp.float32)).astype(jnp.bfloat16)


def head_attention(q_head, k_head, v_head, seg_ids):
    positions = jnp.arange(SEQ_LEN)
    allowed = (positions[:, None] >= positions[None, :])[None] & (seg_ids[:, :, None] == seg_ids[:, None, :])
    scores = jnp.einsum('bqd,bkd->bqk', q_head.astype(jnp.float32), k_head.astype(jnp.float32)) * (HEAD_DIM ** -0.5)
    scores = jnp.where(allowed, scores, -1e30)
    attn_prob = jax.nn.softmax(scores, axis=-1).astype(jnp.bfloat16)
    result = jnp.einsum('bqk,bkd->bqd', attn_prob.astype(jnp.float32), v_head.astype(jnp.float32))
    return result.astype(jnp.bfloat16)


def layer_forward(x_in, seg_ids, gain_one, w_qkv, w_out, gain_two, w_up, w_down):
    x_flat = x_in.reshape(TOKEN_COUNT, MODEL_DIM)
    normed_one = layer_norm(x_flat, gain_one)
    qkv_proj = jnp.dot(normed_one, w_qkv, preferred_element_type=jnp.float32).astype(jnp.bfloat16)
    qkv_heads = jnp.moveaxis(qkv_proj.reshape(BATCH_ROWS, SEQ_LEN, NUM_HEADS, 3, HEAD_DIM), 2, 0)

    def one_head(head_qkv):
        return head_attention(head_qkv[:, :, 0], head_qkv[:, :, 1], head_qkv[:, :, 2], seg_ids)

    attn_heads = lax.map(jax.checkpoint(one_head), qkv_heads)
    attn_flat = jnp.moveaxis(attn_heads, 0, 2).reshape(TOKEN_COUNT, INNER_WIDTH)
    proj_one = jnp.dot(attn_flat, w_out.reshape(INNER_WIDTH, MODEL_DIM), preferred_element_type=jnp.float32)
    resid = (x_flat.astype(jnp.float32) + proj_one).astype(jnp.bfloat16)
    normed_two = layer_norm(resid, gain_two)
    up_proj = jnp.dot(normed_two, w_up, preferred_element_type=jnp.float32).astype(jnp.bfloat16)
    gelu_out = jax.nn.gelu(up_proj.astype(jnp.float32), approximate=True).astype(jnp.bfloat16)
    proj_two = jnp.dot(gelu_out, w_down, preferred_element_type=jnp.float32)
    y_flat = (resid.astype(jnp.float32) + proj_two).astype(jnp.bfloat16)
    return y_flat.reshape(BATCH_ROWS, SEQ_LEN, MODEL_DIM)


def reference(x_in, seg_ids, gain_one, w_qkv, w_out, gain_two, w_up, w_down, d_y):
    def forward_fn(x_arg, g_one, wq_arg, wo_arg, g_two, wu_arg, wd_arg):
        return layer_forward(x_arg, seg_ids, g_one, wq_arg, wo_arg, g_two, wu_arg, wd_arg)

    y_out, pullback = jax.vjp(forward_fn, x_in, gain_one, w_qkv, w_out, gain_two, w_up, w_down)
    d_x, d_gain_one, d_w_qkv, d_w_out, d_gain_two, d_w_up, d_w_down = pullback(d_y)
    return (y_out, d_x, d_w_qkv, d_w_out, d_w_up, d_w_down, d_gain_one, d_gain_two)
```

```python
import functools

import jax
import jax.numpy as jnp
from jax import lax
from jax.experimental import pallas as pl
from jax.experimental.pallas import tpu as pltpu
from jax.sharding import PartitionSpec as P

LN_EPS = 1e-5
MESH = pl.DeviceIdType.MESH
COLS = 1024


def flip(z, k):
    return (z // 2 + k // 2) % 2 * 2 + (z % 2 + k % 2) % 2


def all_reduce_kernel(part, full, buf_core, buf_y, out_y, sum_z, buf_z, send_core, recv_core, send_y, recv_y, send_z, recv_z, gat_zs, gat_zr, gat_ys, gat_yr, gat_cs, gat_cr):
    me = lax.axis_index('model')
    core, y_pos, z_pos = me % 2, me // 2 % 2, me // 4

    def device(z, y, c):
        return {'model': (z * 2 + y) * 2 + c}

    def block(c, y, z):
        return c * 8 + y * 4 + z

    def copy(src, dst, s, r, dev):
        return pltpu.make_async_remote_copy(src_ref=src, dst_ref=dst, send_sem=s, recv_sem=r, device_id=dev, device_id_type=MESH)

    partner = device(z_pos, y_pos, 1 - core)
    y_peer = device(z_pos, 1 - y_pos, core)
    z_peers = [None] + [device(flip(z_pos, k), y_pos, core) for k in (1, 2, 3)]

    barrier = pltpu.get_barrier_semaphore()
    for dev in [partner, y_peer] + z_peers[1:]:
        pl.semaphore_signal(barrier, inc=1, device_id=dev, device_id_type=MESH)
    pl.semaphore_wait(barrier, 5)

    def by_columns(body):
        def step(i, carry):
            body(pl.ds(pl.multiple_of(i * COLS, COLS), COLS))
            return carry
        lax.fori_loop(0, 4096 // COLS, step, 0)

    core_copies, y_copies, z_copies = {}, {}, {}
    for k in (3, 2, 1, 0):
        z_to = flip(z_pos, k)
        for j in (1, 0):
            y_to = (y_pos + j) % 2
            cp = copy(part.at[block(1 - core, y_to, z_to)], buf_core.at[k, j], send_core.at[k, j], recv_core.at[k, j], partner)
            cp.start()
            core_copies[k, j] = cp
    for k in (3, 2, 1, 0):
        z_to = flip(z_pos, k)
        core_copies[k, 1].wait_recv()
        mine = block(core, 1 - y_pos, z_to)

        def add_core(c, k=k, mine=mine):
            out_y[k, :, c] = (part[mine, :, c].astype(jnp.float32) + buf_core[k, 1, :, c].astype(jnp.float32)).astype(jnp.bfloat16)
        by_columns(add_core)
        cp = copy(out_y.at[k], buf_y.at[k], send_y.at[k], recv_y.at[k], y_peer)
        cp.start()
        y_copies[k] = cp
    for k in (3, 2, 1):
        z_to = flip(z_pos, k)
        core_copies[k, 0].wait_recv()
        y_copies[k].wait_recv()
        mine = block(core, y_pos, z_to)

        def add_y(c, k=k, mine=mine):
            sum_z[k - 1, :, c] = (part[mine, :, c].astype(jnp.float32) + buf_core[k, 0, :, c].astype(jnp.float32) + buf_y[k, :, c].astype(jnp.float32)).astype(jnp.bfloat16)
        by_columns(add_y)
        cp = copy(sum_z.at[k - 1], buf_z.at[k - 1], send_z.at[k - 1], recv_z.at[k - 1], z_peers[k])
        cp.start()
        z_copies[k] = cp
    core_copies[0, 0].wait_recv()
    y_copies[0].wait_recv()
    for k in (3, 2, 1):
        z_copies[k].wait_recv()
    own = block(core, y_pos, z_pos)

    def add_all(c):
        total = part[own, :, c].astype(jnp.float32) + buf_core[0, 0, :, c].astype(jnp.float32) + buf_y[0, :, c].astype(jnp.float32)
        for k in (3, 2, 1):
            total = total + buf_z[k - 1, :, c].astype(jnp.float32)
        full[own, :, c] = total.astype(jnp.bfloat16)
    by_columns(add_all)

    gather = []

    def pass_on(b, s, r, dev):
        cp = copy(full.at[b], full.at[b], s, r, dev)
        cp.start()
        gather.append(cp)
        return cp
    z_out = {k: pass_on(own, gat_zs.at[k - 1], gat_zr.at[k - 1], z_peers[k]) for k in (3, 2, 1)}
    y_out = {0: pass_on(own, gat_ys.at[0], gat_yr.at[0], y_peer)}
    c_out = [pass_on(own, gat_cs.at[0, 0], gat_cr.at[0, 0], partner)]
    for k in (1, 2, 3):
        z_out[k].wait_recv()
        b = block(core, y_pos, flip(z_pos, k))
        y_out[k] = pass_on(b, gat_ys.at[k], gat_yr.at[k], y_peer)
        c_out.append(pass_on(b, gat_cs.at[0, k], gat_cr.at[0, k], partner))
    for k in (0, 1, 2, 3):
        y_out[k].wait_recv()
        b = block(core, 1 - y_pos, flip(z_pos, k))
        c_out.append(pass_on(b, gat_cs.at[1, k], gat_cr.at[1, k], partner))
    for cp in c_out:
        cp.wait_recv()
    for cp in list(core_copies.values()) + list(y_copies.values()) + list(z_copies.values()) + gather:
        cp.wait_send()


def all_reduce(part, ident):
    blocks = part.reshape(16, 16, 4096)
    vmem = pl.BlockSpec(memory_space=pltpu.VMEM)
    dma = pltpu.SemaphoreType.DMA
    bf16 = jnp.bfloat16
    out = pl.pallas_call(
        all_reduce_kernel,
        out_shape=jax.ShapeDtypeStruct(blocks.shape, bf16),
        in_specs=[vmem],
        out_specs=vmem,
        scratch_shapes=[
            pltpu.VMEM((4, 2, 16, 4096), bf16),
            pltpu.VMEM((4, 16, 4096), bf16),
            pltpu.VMEM((4, 16, 4096), bf16),
            pltpu.VMEM((3, 16, 4096), bf16),
            pltpu.VMEM((3, 16, 4096), bf16),
            dma((4, 2)), dma((4, 2)), dma((4,)), dma((4,)), dma((3,)), dma((3,)),
            dma((3,)), dma((3,)), dma((4,)), dma((4,)), dma((2, 4)), dma((2, 4)),
        ],
        compiler_params=pltpu.CompilerParams(collective_id=ident, has_side_effects=True, vmem_limit_bytes=16 * 2 ** 20),
        name=f'all_reduce_{ident}',
    )(blocks)
    return out.reshape(part.shape)


def layer_norm(x_in, gain):
    x_wide = x_in.astype(jnp.float32)
    row_mean = jnp.mean(x_wide, axis=-1, keepdims=True)
    centered = x_wide - row_mean
    row_var = jnp.mean(centered * centered, axis=-1, keepdims=True)
    return (centered * lax.rsqrt(row_var + LN_EPS) * gain.astype(jnp.float32)).astype(jnp.bfloat16)


def gelu_tanh(up_proj):
    return jax.nn.gelu(up_proj.astype(jnp.float32), approximate=True).astype(jnp.bfloat16)


def block_mask(seg_ids, start, stop):
    q_pos = jnp.arange(start, stop)
    k_pos = jnp.arange(stop)
    causal = q_pos[:, None] >= k_pos[None, :]
    same_doc = seg_ids[:, start:stop, None] == seg_ids[:, None, :stop]
    return (causal[None] & same_doc)[:, None]


def attention_forward(q_all, k_all, v_all, seg_ids, block_len):
    seq_len = q_all.shape[1]
    score_scale = q_all.shape[-1] ** -0.5
    outputs = []
    log_sums = []
    for start in range(0, seq_len, block_len):
        stop = start + block_len
        scores = jnp.einsum('bqnd,bknd->bnqk', q_all[:, start:stop], k_all[:, :stop], preferred_element_type=jnp.float32) * score_scale
        scores = jnp.where(block_mask(seg_ids, start, stop), scores, -1e30)
        row_max = jnp.max(scores, axis=-1, keepdims=True)
        exp_scores = jnp.exp(scores - row_max)
        row_sum = jnp.sum(exp_scores, axis=-1, keepdims=True)
        attn_prob = (exp_scores / row_sum).astype(jnp.bfloat16)
        outputs.append(jnp.einsum('bnqk,bknd->bqnd', attn_prob, v_all[:, :stop], preferred_element_type=jnp.float32).astype(jnp.bfloat16))
        log_sums.append(row_max + jnp.log(row_sum))
    return jnp.concatenate(outputs, axis=1), log_sums


def attention_backward(q_all, k_all, v_all, d_attn, seg_ids, log_sums, block_len):
    seq_len = q_all.shape[1]
    score_scale = q_all.shape[-1] ** -0.5
    d_q_blocks = []
    d_k_sum = jnp.zeros(k_all.shape, jnp.float32)
    d_v_sum = jnp.zeros(v_all.shape, jnp.float32)
    for index, start in enumerate(range(0, seq_len, block_len)):
        stop = start + block_len
        q_blk = q_all[:, start:stop]
        d_out_blk = d_attn[:, start:stop]
        scores = jnp.einsum('bqnd,bknd->bnqk', q_blk, k_all[:, :stop], preferred_element_type=jnp.float32) * score_scale
        scores = jnp.where(block_mask(seg_ids, start, stop), scores, -1e30)
        attn_prob = jnp.exp(scores - log_sums[index])
        d_prob = jnp.einsum('bqnd,bknd->bnqk', d_out_blk, v_all[:, :stop], preferred_element_type=jnp.float32)
        d_score = attn_prob * (d_prob - jnp.sum(attn_prob * d_prob, axis=-1, keepdims=True)) * score_scale
        d_score = d_score.astype(jnp.bfloat16)
        d_q_blocks.append(jnp.einsum('bnqk,bknd->bqnd', d_score, k_all[:, :stop], preferred_element_type=jnp.float32).astype(jnp.bfloat16))
        pad_width = ((0, 0), (0, seq_len - stop), (0, 0), (0, 0))
        d_k_blk = jnp.einsum('bnqk,bqnd->bknd', d_score, q_blk, preferred_element_type=jnp.float32)
        d_v_blk = jnp.einsum('bnqk,bqnd->bknd', attn_prob.astype(jnp.bfloat16), d_out_blk, preferred_element_type=jnp.float32)
        d_k_sum = d_k_sum + jnp.pad(d_k_blk, pad_width)
        d_v_sum = d_v_sum + jnp.pad(d_v_blk, pad_width)
    return jnp.concatenate(d_q_blocks, axis=1), d_k_sum.astype(jnp.bfloat16), d_v_sum.astype(jnp.bfloat16)


def solution(mesh):
    def local_step(x_in, seg_ids, gain_one, w_qkv, w_out, gain_two, w_up, w_down, d_y):
        rows, seq_len = x_in.shape[:2]
        n_local, head_dim = w_out.shape[:2]
        block_len = min(seq_len, 256)
        normed_one, ln_one_pull = jax.vjp(layer_norm, x_in, gain_one)
        qkv_proj = jnp.einsum('bsh,hc->bsc', normed_one, w_qkv, preferred_element_type=jnp.float32).astype(jnp.bfloat16)
        qkv_heads = qkv_proj.reshape(rows, seq_len, n_local, 3, head_dim)
        q_all = qkv_heads[:, :, :, 0]
        k_all = qkv_heads[:, :, :, 1]
        v_all = qkv_heads[:, :, :, 2]
        attn_out, log_sums = attention_forward(q_all, k_all, v_all, seg_ids, block_len)
        part_one = jnp.einsum('bsnd,ndh->bsh', attn_out, w_out, preferred_element_type=jnp.float32).astype(jnp.bfloat16)
        sum_one = all_reduce(part_one, 0)
        resid = (x_in.astype(jnp.float32) + sum_one.astype(jnp.float32)).astype(jnp.bfloat16)
        normed_two, ln_two_pull = jax.vjp(layer_norm, resid, gain_two)
        up_proj = jnp.einsum('bsh,hf->bsf', normed_two, w_up, preferred_element_type=jnp.float32).astype(jnp.bfloat16)
        gelu_out, gelu_pull = jax.vjp(gelu_tanh, up_proj)
        part_two = jnp.einsum('bsf,fh->bsh', gelu_out, w_down, preferred_element_type=jnp.float32).astype(jnp.bfloat16)
        sum_two = all_reduce(part_two, 1)
        y_out = (resid.astype(jnp.float32) + sum_two.astype(jnp.float32)).astype(jnp.bfloat16)
        d_w_down = jnp.einsum('bsf,bsh->fh', gelu_out, d_y, preferred_element_type=jnp.float32).astype(jnp.bfloat16)
        d_gelu = jnp.einsum('bsh,fh->bsf', d_y, w_down, preferred_element_type=jnp.float32).astype(jnp.bfloat16)
        (d_up,) = gelu_pull(d_gelu)
        d_w_up = jnp.einsum('bsh,bsf->hf', normed_two, d_up, preferred_element_type=jnp.float32).astype(jnp.bfloat16)
        d_norm_part = jnp.einsum('bsf,hf->bsh', d_up, w_up, preferred_element_type=jnp.float32).astype(jnp.bfloat16)
        d_norm_two = all_reduce(d_norm_part, 2)
        d_resid_ln, d_gain_two = ln_two_pull(d_norm_two)
        d_resid = d_y + d_resid_ln
        d_w_out = jnp.einsum('bsnd,bsh->ndh', attn_out, d_resid, preferred_element_type=jnp.float32).astype(jnp.bfloat16)
        d_attn = jnp.einsum('bsh,ndh->bsnd', d_resid, w_out, preferred_element_type=jnp.float32).astype(jnp.bfloat16)
        d_q, d_k, d_v = attention_backward(q_all, k_all, v_all, d_attn, seg_ids, log_sums, block_len)
        d_qkv = jnp.stack([d_q, d_k, d_v], axis=3).reshape(rows, seq_len, 3 * n_local * head_dim)
        d_w_qkv = jnp.einsum('bsh,bsc->hc', normed_one, d_qkv, preferred_element_type=jnp.float32).astype(jnp.bfloat16)
        d_input_part = jnp.einsum('bsc,hc->bsh', d_qkv, w_qkv, preferred_element_type=jnp.float32).astype(jnp.bfloat16)
        d_norm_one = all_reduce(d_input_part, 3)
        d_x_ln, d_gain_one = ln_one_pull(d_norm_one)
        d_x = d_resid + d_x_ln
        return y_out, d_x, d_w_qkv, d_w_out, d_w_up, d_w_down, d_gain_one, d_gain_two

    in_specs = (P('data'), P('data'), P(), P(None, 'model'), P('model'), P(), P(None, 'model'), P('model'), P('data'))
    out_specs = (P('data'), P('data'), P('data', 'model'), P(('data', 'model')), P('data', 'model'), P(('data', 'model')), P('data'), P('data'))
    return jax.shard_map(local_step, mesh=mesh, in_specs=in_specs, out_specs=out_specs, check_vma=False)
```

```python
import jax
import jax.numpy as jnp
from jax import lax
from jax.experimental import pallas as pl
from jax.experimental.pallas import tpu as pltpu
from jax.sharding import PartitionSpec as P

LN_EPS = 1e-5
MESH = pl.DeviceIdType.MESH
BF16 = jnp.bfloat16
F32 = jnp.float32
WIDTH = 4096
CHUNK = 512
CHUNKS = WIDTH // CHUNK
SCALE = 128 ** -0.5
GELU_A = 0.7978845608028654
GELU_B = 0.044715


def flip(z, k):
    return (z // 2 + k // 2) % 2 * 2 + (z % 2 + k % 2) % 2


def dot_nn(a, b):
    return jnp.dot(a, b, preferred_element_type=F32)


def dot_nt(a, b):
    return lax.dot_general(a, b, (((1,), (1,)), ((), ())), preferred_element_type=F32)


def span(j):
    return pl.ds(j * CHUNK, CHUNK)


def fold(v):
    return sum(v[..., i * 128:(i + 1) * 128] for i in range(CHUNK // 128))


def row_stats(wide):
    total = sum(fold(wide(j)) for j in range(CHUNKS))
    mean = jnp.sum(total, axis=-1, keepdims=True) / WIDTH

    def square(j):
        centered = wide(j) - mean
        return fold(centered * centered)
    total = sum(square(j) for j in range(CHUNKS))
    var = jnp.sum(total, axis=-1, keepdims=True) / WIDTH
    return mean, lax.rsqrt(var + LN_EPS)


class Place:
    def __init__(self):
        me = lax.axis_index('model')
        self.core, self.y, self.z = me % 2, me // 2 % 2, me // 4
        self.partner = self.device(self.z, self.y, 1 - self.core)
        self.y_peer = self.device(self.z, 1 - self.y, self.core)
        self.z_peers = [None] + [self.device(flip(self.z, k), self.y, self.core) for k in (1, 2, 3)]
        self.own = self.block(self.core, self.y, self.z)

    def device(self, z, y, c):
        return {'model': (z * 2 + y) * 2 + c}

    def block(self, c, y, z):
        return c * 8 + y * 4 + z


def remote(src, dst, sems, dev):
    cp = pltpu.make_async_remote_copy(src_ref=src, dst_ref=dst, send_sem=sems[0], recv_sem=sems[1], device_id=dev, device_id_type=MESH)
    cp.start()
    return cp


class ReduceScatter:
    def __init__(self, place, part, bufs, sems):
        self.place, self.part = place, part
        self.buf_core, self.out_y, self.buf_y, self.sum_z, self.buf_z = bufs
        self.sems = sems
        self.core_copies, self.y_copies, self.z_copies = {}, {}, {}

    def sem(self, i):
        return self.sems.at[0, i], self.sems.at[1, i]

    def start(self):
        p = self.place
        for k in (3, 2, 1, 0):
            for j in (1, 0):
                b = p.block(1 - p.core, (p.y + j) % 2, flip(p.z, k))
                self.core_copies[k, j] = remote(self.part.at[b], self.buf_core.at[k, j], self.sem(k * 2 + j), p.partner)

    def core_step(self, k):
        p = self.place
        self.core_copies[k, 1].wait_recv()
        b = p.block(p.core, 1 - p.y, flip(p.z, k))
        for j in range(CHUNKS):
            c = span(j)
            self.out_y[k, :, c] = (self.part[b, :, c].astype(F32) + self.buf_core[k, 1, :, c].astype(F32)).astype(BF16)
        self.y_copies[k] = remote(self.out_y.at[k], self.buf_y.at[k], self.sem(8 + k), p.y_peer)

    def chip_sum(self, k, b, c):
        return self.part[b, :, c].astype(F32) + self.buf_core[k, 0, :, c].astype(F32) + self.buf_y[k, :, c].astype(F32)

    def y_step(self, k):
        p = self.place
        self.core_copies[k, 0].wait_recv()
        self.y_copies[k].wait_recv()
        b = p.block(p.core, p.y, flip(p.z, k))
        for j in range(CHUNKS):
            c = span(j)
            self.sum_z[k - 1, :, c] = self.chip_sum(k, b, c).astype(BF16)
        self.z_copies[k] = remote(self.sum_z.at[k - 1], self.buf_z.at[k - 1], self.sem(12 + k), p.z_peers[k])

    def finish(self):
        self.core_copies[0, 0].wait_recv()
        self.y_copies[0].wait_recv()
        for k in (3, 2, 1):
            self.z_copies[k].wait_recv()

    def total(self, c):
        t = self.chip_sum(0, self.place.own, c)
        for k in (3, 2, 1):
            t = t + self.buf_z[k - 1, :, c].astype(F32)
        return t

    def drain(self):
        for group in (self.core_copies, self.y_copies, self.z_copies):
            for cp in group.values():
                cp.wait_send()


class Gather:
    def __init__(self, place, full, sems):
        self.place, self.full, self.sems = place, full, sems
        self.z_out, self.y_out, self.c_out, self.sent = {}, {}, {}, []

    def send(self, b, i, dev):
        cp = remote(self.full.at[b], self.full.at[b], (self.sems.at[0, i], self.sems.at[1, i]), dev)
        self.sent.append(cp)
        return cp

    def start(self):
        p = self.place
        for k in (3, 2, 1):
            self.z_out[k] = self.send(p.own, k, p.z_peers[k])
        self.y_out[0] = self.send(p.own, 4, p.y_peer)
        self.c_out[0, 0] = self.send(p.own, 8, p.partner)

    def z_step(self, k):
        p = self.place
        self.z_out[k].wait_recv()
        b = p.block(p.core, p.y, flip(p.z, k))
        self.y_out[k] = self.send(b, 4 + k, p.y_peer)
        self.c_out[0, k] = self.send(b, 8 + k, p.partner)

    def y_step(self, k):
        p = self.place
        self.y_out[k].wait_recv()
        self.c_out[1, k] = self.send(p.block(p.core, 1 - p.y, flip(p.z, k)), 12 + k, p.partner)

    def finish(self):
        for cp in self.c_out.values():
            cp.wait_recv()

    def drain(self):
        for cp in self.sent:
            cp.wait_send()


def layer_kernel(
    x_hbm, dy_hbm, g1, g2, seg_row, seg_col, wqkv_hbm, wo_hbm, w1_hbm, w2_hbm,
    y_hbm, dx_hbm, dg_out, a_hbm, dqkv_hbm, o_hbm, dr_hbm, b1_hbm, du_hbm, gelu_hbm,
    x, dy, wqkv, wo, w1, w2, a, f1, f2, fy, fx, part1, part3, part_y,
    core_buf, yout_buf, y_buf, zsum_buf, z_buf,
    qkv, prob, o, up, gelu, d_gelu, d_up, d_attn, dqkv, x1, d_res, wide, dg_part, dg_core, dg_y, dg_sum, dg_z, dg_full,
    rs_sems, ag_sems, dg_sems, in_sems, out_sems,
):
    place = Place()
    own = place.own

    loads = [
        pltpu.make_async_copy(src, dst, in_sems.at[i])
        for i, (src, dst) in enumerate([(x_hbm, x), (wqkv_hbm, wqkv), (wo_hbm, wo), (dy_hbm, dy), (w2_hbm, w2), (w1_hbm, w1)])
    ]
    load_x, load_wqkv, load_wo, load_dy, load_w2, load_w1 = loads
    load_x.start()
    load_wqkv.start()
    stores = []

    def store(src, dst):
        cp = pltpu.make_async_copy(src, dst, out_sems.at[len(stores)])
        cp.start()
        stores.append(cp)

    barrier = pltpu.get_barrier_semaphore()
    for dev in [place.partner, place.y_peer] + place.z_peers[1:]:
        pl.semaphore_signal(barrier, inc=1, device_id=dev, device_id_type=MESH)

    def rs_set(i, part):
        bufs = [ref.at[i] for ref in (core_buf, yout_buf, y_buf, zsum_buf, z_buf)]
        return ReduceScatter(place, part, bufs, rs_sems.at[i])

    rs1, rs3, rsy, rs4 = rs_set(0, part1), rs_set(1, part3), rs_set(2, part_y), rs_set(3, part1)
    ag1, ag3, agy, ag4 = [Gather(place, ref, ag_sems.at[i]) for i, ref in enumerate((f1, f2, fy, fx))]

    def gain(ref, j):
        return ref[:, span(j)].astype(F32)

    load_x.wait()
    for cp in (load_wo, load_dy, load_w2, load_w1):
        cp.start()

    def ln_one(i, carry):
        rows = pl.ds(i * 2, 2)
        mean, rstd = row_stats(lambda j: x[rows, :, span(j)].astype(F32))
        for j in range(CHUNKS):
            c = span(j)
            normed = (x[rows, :, c].astype(F32) - mean) * rstd * gain(g1, j)[None]
            a[rows, :, c] = normed.astype(BF16)
        return carry
    lax.fori_loop(0, 8, ln_one, 0)
    store(a, a_hbm)

    load_wqkv.wait()
    qkv[...] = dot_nn(a[...].reshape(256, WIDTH), wqkv[...]).astype(BF16)

    q_pos = lax.broadcasted_iota(jnp.int32, (256, 256), 0)
    k_pos = lax.broadcasted_iota(jnp.int32, (256, 256), 1)
    allowed = (q_pos >= k_pos) & (seg_col[...] == seg_row[...])
    for h in range(2):
        q, k, v = [qkv[:, pl.ds(h * 384 + i * 128, 128)] for i in range(3)]
        scores = jnp.where(allowed, dot_nt(q, k) * SCALE, -1e30)
        exp_scores = jnp.exp(scores - jnp.max(scores, axis=-1, keepdims=True))
        p = exp_scores / jnp.sum(exp_scores, axis=-1, keepdims=True)
        prob[h] = p
        o[:, pl.ds(h * 128, 128)] = dot_nn(p.astype(BF16), v).astype(BF16)

    def project(lhs, weight, part, tile, transposed, lo=0, hi=WIDTH):
        def step(i, carry):
            c = pl.ds(pl.multiple_of(lo + i * tile, tile), tile)
            r = dot_nt(lhs[...], weight[c, :]) if transposed else dot_nn(lhs[...], weight[:, c])
            part[:, :, c] = r.astype(BF16).reshape(16, 16, tile)
            return carry
        lax.fori_loop(0, (hi - lo) // tile, step, 0)

    load_wo.wait()
    project(o, wo, part1, 512, False)
    store(o, o_hbm)
    pl.semaphore_wait(barrier, 5)

    rs1.start()
    for k in (3, 2, 1, 0):
        rs1.core_step(k)

    def d_gelu_tile(lo, n):
        c = pl.ds(lo, n)
        d_gelu[:, c] = dot_nt(dy[...].reshape(256, WIDTH), w2[c, :]).astype(BF16)
    load_dy.wait()
    load_w2.wait()
    d_gelu_tile(0, 256)
    rs1.y_step(3)
    d_gelu_tile(256, 256)
    rs1.y_step(2)
    d_gelu_tile(512, 256)
    rs1.y_step(1)
    d_gelu_tile(768, 128)
    rs1.finish()

    for j in range(CHUNKS):
        c = span(j)
        x1[:, c] = (x[own, :, c].astype(F32) + rs1.total(c)).astype(BF16)
    mean2, rstd2 = row_stats(lambda j: x1[:, span(j)].astype(F32))
    for j in range(CHUNKS):
        c = span(j)
        f1[own, :, c] = ((x1[:, c].astype(F32) - mean2) * rstd2 * gain(g2, j)).astype(BF16)
    ag1.start()
    for k in (1, 2, 3):
        ag1.z_step(k)
    for k in (0, 1, 2, 3):
        ag1.y_step(k)
    load_w1.wait()
    ag1.finish()
    store(f1, b1_hbm)

    for lo, n in ((0, 512), (512, 384)):
        c = pl.ds(lo, n)
        up[:, c] = dot_nn(f1[...].reshape(256, WIDTH), w1[:, c]).astype(BF16)

    def activation(i, carry):
        rows = pl.ds(pl.multiple_of(i * 16, 16), 16)
        u = up[rows, :].astype(F32)
        t = jnp.tanh(GELU_A * (u + GELU_B * (u * u * u)))
        gelu[rows, :] = (0.5 * u * (1.0 + t)).astype(BF16)
        slope = 0.5 * (1.0 + t) + 0.5 * u * (1.0 - t * t) * (GELU_A * (1.0 + 3.0 * GELU_B * (u * u)))
        d_up[rows, :] = (d_gelu[rows, :].astype(F32) * slope).astype(BF16)
        return carry
    lax.fori_loop(0, 16, activation, 0)
    store(gelu, gelu_hbm)
    store(d_up, du_hbm)
    project(d_up, w1, part3, 1024, True)

    rs3.start()
    for k in (3, 2, 1, 0):
        rs3.core_step(k)
    project(gelu, w2, part_y, 1024, False, 0, 2048)
    rs3.y_step(3)
    project(gelu, w2, part_y, 1024, False, 2048, 4096)
    rsy.start()
    rs3.y_step(2)
    rsy.core_step(3)
    rs3.y_step(1)
    rsy.core_step(2)
    rs3.finish()

    def ln_backward(rs, z, mean, rstd, gain_ref, dg_row):
        sum_a = jnp.zeros((16, 128), F32)
        sum_b = jnp.zeros((16, 128), F32)
        for j in range(CHUNKS):
            d_norm = rs.total(span(j)).astype(BF16).astype(F32)
            x_hat = (z(j) - mean) * rstd
            grad_row = jnp.sum(d_norm * x_hat, axis=0, keepdims=True)
            for i in range(CHUNK // 128):
                at = j * (CHUNK // 128) + i
                dg_part[at // 2, pl.ds(dg_row + at % 2, 1), :] = grad_row[:, i * 128:(i + 1) * 128]
            scaled = d_norm * gain(gain_ref, j)
            wide[:, span(j)] = scaled
            sum_a = sum_a + fold(scaled)
            sum_b = sum_b + fold(scaled * x_hat)
        mean_a = jnp.sum(sum_a, axis=-1, keepdims=True) / WIDTH
        mean_b = jnp.sum(sum_b, axis=-1, keepdims=True) / WIDTH
        for j in range(CHUNKS):
            c = span(j)
            x_hat = (z(j) - mean) * rstd
            wide[:, c] = rstd * (wide[:, c] - mean_a - x_hat * mean_b)

    ln_backward(rs3, lambda j: x1[:, span(j)].astype(F32), mean2, rstd2, g2, 2)
    for j in range(CHUNKS):
        c = span(j)
        value = (dy[own, :, c].astype(F32) + wide[:, c].astype(BF16).astype(F32)).astype(BF16)
        d_res[:, c] = value
        f2[own, :, c] = value
    ag3.start()
    for k in (1, 2, 3):
        ag3.z_step(k)
    rsy.core_step(1)
    rsy.core_step(0)
    for k in (0, 1, 2, 3):
        ag3.y_step(k)
    rsy.y_step(3)
    rsy.y_step(2)
    ag3.finish()
    store(f2, dr_hbm)

    d_attn[...] = dot_nt(f2[...].reshape(256, WIDTH), wo[...]).astype(BF16)
    for h in range(2):
        q, k, v = [qkv[:, pl.ds(h * 384 + i * 128, 128)] for i in range(3)]
        d_o = d_attn[:, pl.ds(h * 128, 128)]
        p = prob[h]
        d_prob = dot_nt(d_o, v)
        d_score = p * (d_prob - jnp.sum(p * d_prob, axis=-1, keepdims=True)) * SCALE
        dqkv[:, pl.ds(h * 384, 128)] = dot_nn(d_score.astype(BF16), k).astype(BF16)
        dqkv[:, pl.ds(h * 384 + 128, 128)] = dot_nn(d_score.T.astype(BF16), q).astype(BF16)
        dqkv[:, pl.ds(h * 384 + 256, 128)] = dot_nn(p.T.astype(BF16), d_o).astype(BF16)
    store(dqkv, dqkv_hbm)
    rs1.drain()
    project(dqkv, wqkv, part1, 1024, True)

    rs4.start()
    for k in (3, 2, 1, 0):
        rs4.core_step(k)
    rsy.y_step(1)
    rsy.finish()
    for j in range(CHUNKS):
        c = span(j)
        fy[own, :, c] = (x1[:, c].astype(F32) + rsy.total(c)).astype(BF16)
    agy.start()
    rs4.y_step(3)
    rs4.y_step(2)
    agy.z_step(1)
    rs4.y_step(1)
    agy.z_step(2)
    agy.z_step(3)
    rs4.finish()

    mean1, rstd1 = row_stats(lambda j: x[own, :, span(j)].astype(F32))
    ln_backward(rs4, lambda j: x[own, :, span(j)].astype(F32), mean1, rstd1, g1, 0)
    for j in range(CHUNKS):
        c = span(j)
        fx[own, :, c] = (d_res[:, c].astype(F32) + wide[:, c].astype(BF16).astype(F32)).astype(BF16)
    ag4.start()

    def dg_sem(i):
        return dg_sems.at[0, i], dg_sems.at[1, i]
    dg_copies = []

    def dg_send(src, dst, i, dev):
        cp = remote(src, dst, dg_sem(i), dev)
        dg_copies.append(cp)
        return cp
    half = pl.ds((1 - place.core) * 8, 8)
    dg_send(dg_part.at[half], dg_core, 0, place.partner).wait_recv()
    dg_core[...] = dg_core[...] + dg_part[pl.ds(place.core * 8, 8)]
    dg_send(dg_core.at[pl.ds((1 - place.y) * 4, 4)], dg_y, 1, place.y_peer).wait_recv()
    dg_sum[...] = dg_core[pl.ds(place.y * 4, 4)] + dg_y[...]
    arrivals = [dg_send(dg_sum.at[flip(place.z, k)], dg_z.at[k - 1], 1 + k, place.z_peers[k]) for k in (1, 2, 3)]
    for k in (1, 2, 3):
        ag4.z_step(k)
    for cp in arrivals:
        cp.wait_recv()
    dg_full[own] = dg_sum[place.z] + dg_z[0] + dg_z[1] + dg_z[2]
    arrivals = [dg_send(dg_full.at[own], dg_full.at[own], 4 + k, place.z_peers[k]) for k in (1, 2, 3)]
    for k in (0, 1, 2, 3):
        agy.y_step(k)
    for k in (0, 1):
        ag4.y_step(k)
    for cp in arrivals:
        cp.wait_recv()
    quarter = pl.ds(place.core * 8 + place.y * 4, 4)
    cp = dg_send(dg_full.at[quarter], dg_full.at[quarter], 8, place.y_peer)
    ag4.y_step(2)
    cp.wait_recv()
    mine = pl.ds(place.core * 8, 8)
    cp = dg_send(dg_full.at[mine], dg_full.at[mine], 9, place.partner)
    ag4.y_step(3)
    agy.finish()
    store(fy, y_hbm)
    cp.wait_recv()
    dg_out[...] = dg_full[...].astype(BF16)
    ag4.finish()
    store(fx, dx_hbm)

    for rs in (rs3, rsy, rs4):
        rs.drain()
    for ag in (ag1, ag3, agy, ag4):
        ag.drain()
    for cp in dg_copies:
        cp.wait_send()
    for cp in stores:
        cp.wait()


def layer(x_in, d_y, gain_one, gain_two, seg_ids, w_qkv, w_out, w_up, w_down):
    hbm = pl.BlockSpec(memory_space=pl.ANY)
    vmem = pl.BlockSpec(memory_space=pltpu.VMEM)
    dma = pltpu.SemaphoreType.DMA

    def shape(*dims, dtype=BF16):
        return jax.ShapeDtypeStruct(dims, dtype)
    blocks = (16, 16, WIDTH)
    return pl.pallas_call(
        layer_kernel,
        out_shape=[
            shape(*blocks), shape(*blocks), shape(16, 4, 128), shape(*blocks), shape(256, 768), shape(256, 256), shape(*blocks),
            shape(*blocks), shape(256, 896), shape(256, 896),
        ],
        in_specs=[hbm, hbm, vmem, vmem, vmem, vmem, hbm, hbm, hbm, hbm],
        out_specs=[hbm, hbm, vmem] + [hbm] * 7,
        scratch_shapes=[
            pltpu.VMEM(blocks, BF16), pltpu.VMEM(blocks, BF16),
            pltpu.VMEM((WIDTH, 768), BF16), pltpu.VMEM((256, WIDTH), BF16), pltpu.VMEM((WIDTH, 896), BF16), pltpu.VMEM((896, WIDTH), BF16),
        ] + [pltpu.VMEM(blocks, BF16)] * 8 + [
            pltpu.VMEM((4, 4, 2, 16, WIDTH), BF16), pltpu.VMEM((4, 4, 16, WIDTH), BF16), pltpu.VMEM((4, 4, 16, WIDTH), BF16),
            pltpu.VMEM((4, 3, 16, WIDTH), BF16), pltpu.VMEM((4, 3, 16, WIDTH), BF16),
            pltpu.VMEM((256, 768), BF16), pltpu.VMEM((2, 256, 256), F32), pltpu.VMEM((256, 256), BF16),
        ] + [pltpu.VMEM((256, 896), BF16)] * 4 + [
            pltpu.VMEM((256, 256), BF16), pltpu.VMEM((256, 768), BF16), pltpu.VMEM((16, WIDTH), BF16), pltpu.VMEM((16, WIDTH), BF16),
            pltpu.VMEM((16, WIDTH), F32),
            pltpu.VMEM((16, 4, 128), F32), pltpu.VMEM((8, 4, 128), F32), pltpu.VMEM((4, 4, 128), F32), pltpu.VMEM((4, 4, 128), F32),
            pltpu.VMEM((3, 4, 128), F32), pltpu.VMEM((16, 4, 128), F32),
            dma((4, 2, 16)), dma((4, 2, 16)), dma((2, 10)), dma((6,)), dma((9,)),
        ],
        compiler_params=pltpu.CompilerParams(collective_id=0, has_side_effects=True, vmem_limit_bytes=66 * 10 ** 6),
        name='layer',
    )(
        x_in.reshape(blocks), d_y.reshape(blocks), gain_one.reshape(1, WIDTH), gain_two.reshape(1, WIDTH), seg_ids.reshape(1, 256), seg_ids.reshape(256, 1),
        w_qkv, w_out.reshape(256, WIDTH), w_up, w_down,
    )


def solution(mesh):
    def local_step(x_in, seg_ids, gain_one, w_qkv, w_out, gain_two, w_up, w_down, d_y):
        y_out, d_x, d_gains, normed_one, d_qkv, attn_out, d_resid, normed_two, d_up, gelu_out = layer(x_in, d_y, gain_one, gain_two, seg_ids, w_qkv, w_out, w_up, w_down)

        def weight_grad(a, b):
            return lax.dot_general(a.reshape(256, -1), b.reshape(256, -1), (((0,), (0,)), ((), ())), preferred_element_type=F32).astype(BF16)
        d_w_qkv = weight_grad(normed_one, d_qkv)
        d_w_out = weight_grad(attn_out, d_resid).reshape(w_out.shape)
        d_w_up = weight_grad(normed_two, d_up)
        d_w_down = weight_grad(gelu_out, d_y)
        d_gain_one = d_gains[:, 0:2].reshape(WIDTH)
        d_gain_two = d_gains[:, 2:4].reshape(WIDTH)
        return y_out.reshape(x_in.shape), d_x.reshape(x_in.shape), d_w_qkv, d_w_out, d_w_up, d_w_down, d_gain_one, d_gain_two

    in_specs = (P('data'), P('data'), P(), P(None, 'model'), P('model'), P(), P(None, 'model'), P('model'), P('data'))
    out_specs = (P('data'), P('data'), P('data', 'model'), P(('data', 'model')), P('data', 'model'), P(('data', 'model')), P('data'), P('data'))
    return jax.shard_map(local_step, mesh=mesh, in_specs=in_specs, out_specs=out_specs, check_vma=False)
```

```python
import jax
import jax.numpy as jnp
from jax import lax
from jax.experimental import pallas as pl
from jax.experimental.pallas import tpu as pltpu
from jax.sharding import PartitionSpec as P

LN_EPS = 1e-5
MESH = pl.DeviceIdType.MESH
BF16 = jnp.bfloat16
F32 = jnp.float32
WIDTH = 4096
CHUNK = 512
WO_TILE = 2048
LAYER_VMEM = 49 * 2 ** 20
GRADS_VMEM = 28 * 2 ** 20
TOKENS = 256
LANES = 128
BLOCKS = 16
FFN = 896
QKV_COLS = 768
CHUNKS = WIDTH // CHUNK
SCALE = LANES ** -0.5
GELU_A = 0.7978845608028654
GELU_B = 0.044715


def flip(z, k):
    high, low = lax.div(z, 2), lax.rem(z, 2)
    return (1 - high if k >= 2 else high) * 2 + (1 - low if k % 2 else low)


def dot_nn(a, b):
    return jnp.dot(a, b, preferred_element_type=F32)


def dot_nt(a, b):
    return lax.dot_general(a, b, (((1,), (1,)), ((), ())), preferred_element_type=F32)


def span(j):
    return pl.ds(j * CHUNK, CHUNK)


def half(h):
    return pl.ds(h * (WIDTH // 2), WIDTH // 2)


def half_spans(h):
    return [(span(h * (CHUNKS // 2) + j), span(j)) for j in range(CHUNKS // 2)]


def fold(v):
    return sum(v[..., i * LANES:(i + 1) * LANES] for i in range(CHUNK // LANES))


def row_stats(wide):
    total = sum(fold(wide(j)) for j in range(CHUNKS))
    mean = jnp.sum(total, axis=-1, keepdims=True) / WIDTH

    def square(j):
        centered = wide(j) - mean
        return fold(centered * centered)
    total = sum(square(j) for j in range(CHUNKS))
    var = jnp.sum(total, axis=-1, keepdims=True) / WIDTH
    return mean, lax.rsqrt(var + LN_EPS)


class Place:
    def __init__(self):
        me = lax.axis_index('model')
        self.core, self.y, self.z = lax.rem(me, 2), lax.rem(lax.div(me, 2), 2), lax.div(me, 4)
        self.partner = {'model': me + 1 - 2 * self.core}
        self.y_peer = {'model': me + 2 - 4 * self.y}
        self.z_at = [flip(self.z, k) for k in range(4)]
        self.z_peers = [{'model': me + (at - self.z) * 4} for at in self.z_at]
        self.blocks = {
            (i, j, k): (1 - self.core if i else self.core) * 8 + (1 - self.y if j else self.y) * 4 + self.z_at[k]
            for i in (0, 1) for j in (0, 1) for k in range(4)
        }
        self.own = self.blocks[0, 0, 0]

    def block(self, i, j, k):
        return self.blocks[i, j, k]


def remote(src, dst, sems, dev):
    cp = pltpu.make_async_remote_copy(src_ref=src, dst_ref=dst, send_sem=sems[0], recv_sem=sems[1], device_id=dev, device_id_type=MESH)
    cp.start()
    return cp


class ReduceScatter:
    def __init__(self, place, part, bufs, sems):
        self.place, self.part, self.sems = place, part, sems
        self.buf_core, self.out_y, self.buf_y, self.out_z, self.buf_z, self.out_first, self.buf_first = bufs
        self.core_in, self.y_in, self.z_in, self.first_in = {}, {}, {}, {}
        self.ready = set()

    def sem(self, i):
        return self.sems.at[0, i], self.sems.at[1, i]

    def block(self, k, j):
        return self.place.block(0, j, k)

    def start(self):
        p = self.place
        for k in (3, 1, 2, 0):
            for j in (1, 0):
                b = p.block(1, j, k)
                self.core_in[k, j] = remote(self.part.at[b], self.buf_core.at[k, j], self.sem(k * 2 + j), p.partner)

    def core_ready(self, k, j):
        if (k, j) not in self.ready:
            self.core_in[k, j].wait_recv()
            self.ready.add((k, j))

    def pair_sum(self, k, j, c):
        return self.part[self.block(k, j), :, c].astype(F32) + self.buf_core[k, j, :, c].astype(F32)

    def chip_sum(self, k, c):
        return self.pair_sum(k, 0, c) + self.buf_y[k, :, c].astype(F32)

    def send_y(self, k, h):
        self.core_ready(k, 1)
        if (k, h) == (0, 1):
            self.first_in[1].wait_recv()
        for c, d in half_spans(h):
            t = self.pair_sum(k, 1, c)
            if (k, h) == (0, 1):
                t = t + self.buf_first[1, :, d].astype(F32)
            self.out_y[k, :, c] = t.astype(BF16)
        self.y_in[k, h] = remote(self.out_y.at[k, :, half(h)], self.buf_y.at[k, :, half(h)], self.sem(8 + k * 2 + h), self.place.y_peer)

    def send_first(self):
        for j in (1, 0):
            self.core_ready(1, j)
            for c, d in half_spans(1):
                self.out_first[j, :, d] = self.pair_sum(1, j, c).astype(BF16)
            self.first_in[j] = remote(self.out_first.at[j], self.buf_first.at[j], self.sem(22 + j), self.place.z_peers[1])

    def send_z(self, k, h):
        self.core_ready(k, 0)
        self.y_in[k, h].wait_recv()
        if k == 2:
            self.z_in[3, h].wait_recv()
        for c, _ in half_spans(h):
            t = self.chip_sum(k, c)
            if k == 2:
                t = t + self.buf_z[2, :, c].astype(F32)
            self.out_z[k - 1, :, c] = t.astype(BF16)
        self.z_in[k, h] = remote(self.out_z.at[k - 1, :, half(h)], self.buf_z.at[k - 1, :, half(h)], self.sem(14 + k * 2 + h), self.place.z_peers[2 if k == 2 else 1])

    def head(self):
        return [
            lambda: self.send_y(3, 0), lambda: self.send_y(3, 1), self.send_first, lambda: self.send_y(1, 0),
            lambda: self.send_y(2, 0), lambda: self.send_y(2, 1), lambda: self.send_y(0, 0),
        ]

    def tail(self):
        return [
            lambda: self.send_z(3, 0), lambda: self.send_z(3, 1), lambda: self.send_y(0, 1),
            lambda: self.send_z(1, 0), lambda: self.send_z(2, 0), lambda: self.send_z(2, 1),
        ]

    def finish(self):
        self.core_ready(0, 0)
        self.y_in[0, 0].wait_recv()
        self.y_in[0, 1].wait_recv()
        self.first_in[0].wait_recv()
        self.z_in[1, 0].wait_recv()
        self.z_in[2, 0].wait_recv()
        self.z_in[2, 1].wait_recv()

    def total(self, j):
        c = span(j)
        near = self.buf_z[0, :, c] if j < CHUNKS // 2 else self.buf_first[0, :, span(j - CHUNKS // 2)]
        return self.chip_sum(0, c) + near.astype(F32) + self.buf_z[1, :, c].astype(F32)

    def drain(self):
        for group in (self.core_in, self.y_in, self.z_in, self.first_in):
            for cp in group.values():
                cp.wait_send()


class Gather:
    def __init__(self, place, full, sems):
        self.place, self.full, self.sems = place, full, sems
        self.z_in, self.y_in, self.core_in, self.last_in, self.sent = {}, {}, {}, {}, []

    def send(self, j, k, h, i, dev):
        b = self.place.block(0, j, k)
        ref = self.full.at[b] if h is None else self.full.at[b, :, half(h)]
        cp = remote(ref, ref, (self.sems.at[0, i], self.sems.at[1, i]), dev)
        self.sent.append(cp)
        return cp

    def to_core(self, j, k, h):
        self.core_in[j, k, h] = self.send(j, k, h, 14 + j * 8 + k * 2 + h, self.place.partner)

    def to_y(self, k, h):
        self.y_in[k, h] = self.send(0, k, h, 6 + k * 2 + h, self.place.y_peer)

    def to_z(self, k, h):
        self.z_in[k, h] = self.send(0, 2 if k == 3 else 0, h, (k - 1) * 2 + h, self.place.z_peers[2 if k == 2 else 1])

    def start_far(self):
        for h in (0, 1):
            self.to_z(2, h)

    def start_near(self):
        for h in (0, 1):
            self.to_y(0, h)
            self.to_z(1, h)
        self.core_in[0, 0, None] = self.send(0, 0, None, 30, self.place.partner)

    def from_z(self, k, h):
        self.z_in[k, h].wait_recv()
        if k == 2:
            self.to_z(3, h)
        if (k, h) != (1, 1):
            self.to_y(k, h)
        self.to_core(0, k, h)

    def from_y(self, k, h):
        self.y_in[k, h].wait_recv()
        self.to_core(1, k, h)

    def send_last(self):
        self.last_in[0] = self.send(1, 0, 1, 31, self.place.z_peers[1])

    def from_last(self):
        self.last_in[0].wait_recv()
        self.to_core(1, 1, 1)

    def steps(self):
        return [
            lambda: self.from_y(0, 0), lambda: self.from_z(2, 0), lambda: self.from_y(0, 1), lambda: self.from_z(2, 1), self.send_last,
            lambda: self.from_z(1, 0), lambda: self.from_z(1, 1), lambda: self.from_y(2, 0), lambda: self.from_y(2, 1), lambda: self.from_z(3, 0),
            lambda: self.from_y(1, 0), lambda: self.from_z(3, 1), self.from_last, lambda: self.from_y(3, 0), lambda: self.from_y(3, 1),
        ]

    def late_steps(self):
        near = [lambda: self.from_y(0, 0), lambda: self.from_y(0, 1), lambda: self.from_z(1, 0), lambda: self.from_z(1, 1)]
        far = [
            lambda: self.from_z(2, 0), lambda: self.from_z(2, 1), lambda: self.from_y(1, 0), lambda: self.from_z(3, 0), lambda: self.from_z(3, 1),
            lambda: self.from_y(2, 0), lambda: self.from_y(2, 1), self.from_last, lambda: self.from_y(3, 0), lambda: self.from_y(3, 1),
        ]
        return near, far

    def finish(self):
        for cp in self.core_in.values():
            cp.wait_recv()

    def drain(self):
        for cp in self.sent:
            cp.wait_send()


def run(steps):
    for step in steps:
        step()


def layer_kernel(
    x_hbm, dy_hbm, g1, g2, seg, wqkv_hbm, wo_hbm, w1_hbm, w2_hbm,
    fy, fx, dg1_out, dg2_out, a, dqkv, o, f2, f1, d_up, gelu, dy,
    x, wqkv, wo, w1, w2, part1, part3, part_y,
    core_buf, yout_buf, y_buf, zout_buf, z_buf, fout_buf, first_buf,
    qkv, prob, up, d_gelu, d_attn, x1, d_res, wide, dg_part, dg_core, dg_y, dg_z, dg_full,
    rs_sems, ag_sems, dg_sems, in_sems,
):
    place = Place()
    own = place.own

    loads = [
        pltpu.make_async_copy(src, dst, in_sems.at[i])
        for i, (src, dst) in enumerate([(x_hbm, x), (wqkv_hbm, wqkv), (wo_hbm, wo), (dy_hbm, dy), (w2_hbm, w2), (w1_hbm, w1)])
    ]
    load_x, load_wqkv, load_wo, load_dy, load_w2, load_w1 = loads
    load_x.start()
    load_wqkv.start()
    barrier = pltpu.get_barrier_semaphore()
    for dev in [place.partner, place.y_peer] + place.z_peers[1:]:
        pl.semaphore_signal(barrier, inc=1, device_id=dev, device_id_type=MESH)

    def rs_set(i, part):
        bufs = [ref.at[i] for ref in (core_buf, yout_buf, y_buf, zout_buf, z_buf, fout_buf, first_buf)]
        return ReduceScatter(place, part, bufs, rs_sems.at[i])

    rs1, rs3, rsy, rs4 = rs_set(0, part1), rs_set(1, part3), rs_set(2, part_y), rs_set(3, part1)
    ag1, ag3, agy, ag4 = [Gather(place, ref, ag_sems.at[i]) for i, ref in enumerate((f1, f2, fy, fx))]

    def gain(ref, j):
        return ref[span(j)].astype(F32).reshape(1, CHUNK)

    load_x.wait()
    for cp in (load_wo, load_dy, load_w2, load_w1):
        cp.start()

    def ln_one(i, carry):
        rows = pl.ds(i * 2, 2)
        mean, rstd = row_stats(lambda j: x[rows, :, span(j)].astype(F32))
        for j in range(CHUNKS):
            c = span(j)
            normed = (x[rows, :, c].astype(F32) - mean) * rstd * gain(g1, j)[None]
            a[rows, :, c] = normed.astype(BF16)
        return carry
    lax.fori_loop(0, 8, ln_one, 0)

    load_wqkv.wait()
    qkv[...] = dot_nn(a[...].reshape(TOKENS, WIDTH), wqkv[...]).astype(BF16)

    q_pos = lax.broadcasted_iota(jnp.int32, (TOKENS, TOKENS), 0)
    k_pos = lax.broadcasted_iota(jnp.int32, (TOKENS, TOKENS), 1)
    seg_keys = jnp.broadcast_to(seg[...].astype(F32), (TOKENS, TOKENS))
    allowed = (q_pos >= k_pos) & (seg_keys.T == seg_keys)
    for h in range(2):
        q, k, v = [qkv[:, pl.ds(h * 384 + i * LANES, LANES)] for i in range(3)]
        scores = jnp.where(allowed, dot_nt(q, k) * SCALE, -1e30)
        exp_scores = jnp.exp(scores - jnp.max(scores, axis=-1, keepdims=True))
        p = exp_scores / jnp.sum(exp_scores, axis=-1, keepdims=True)
        prob[h] = p
        o[:, pl.ds(h * LANES, LANES)] = dot_nn(p.astype(BF16), v).astype(BF16)

    def project(lhs, weight, part, tile, transposed, lo=0, hi=WIDTH):
        def step(i, carry):
            c = pl.ds(pl.multiple_of(lo + i * tile, tile), tile)
            r = dot_nt(lhs[...], weight[c, :]) if transposed else dot_nn(lhs[...], weight[:, c])
            part[:, :, c] = r.astype(BF16).reshape(BLOCKS, BLOCKS, tile)
            return carry
        lax.fori_loop(0, (hi - lo) // tile, step, 0)

    load_wo.wait()
    project(o, wo, part1, WO_TILE, False)
    pl.semaphore_wait(barrier, 5)

    rs1.start()
    run(rs1.head())

    def d_gelu_tile(lo, n):
        c = pl.ds(lo, n)
        d_gelu[:, c] = dot_nt(dy[...].reshape(TOKENS, WIDTH), w2[c, :]).astype(BF16)
    load_dy.wait()
    load_w2.wait()
    tail = rs1.tail()
    d_gelu_tile(0, TOKENS)
    run(tail[:4])
    d_gelu_tile(TOKENS, TOKENS)
    run(tail[4:5])
    d_gelu_tile(512, TOKENS)
    run(tail[5:])
    d_gelu_tile(QKV_COLS, LANES)
    rs1.finish()

    for j in range(CHUNKS):
        c = span(j)
        x1[:, c] = (x[own, :, c].astype(F32) + rs1.total(j)).astype(BF16)
    mean2, rstd2 = row_stats(lambda j: x1[:, span(j)].astype(F32))
    for j in range(CHUNKS):
        c = span(j)
        f1[own, :, c] = ((x1[:, c].astype(F32) - mean2) * rstd2 * gain(g2, j)).astype(BF16)
    ag1.start_far()
    ag1.start_near()
    run(ag1.steps())
    load_w1.wait()
    ag1.finish()

    for lo, n in ((0, 512), (512, 384)):
        c = pl.ds(lo, n)
        up[:, c] = dot_nn(f1[...].reshape(TOKENS, WIDTH), w1[:, c]).astype(BF16)

    def activation(i, carry):
        rows = pl.ds(pl.multiple_of(i * BLOCKS, BLOCKS), BLOCKS)
        u = up[rows, :].astype(F32)
        t = jnp.tanh(GELU_A * (u + GELU_B * (u * u * u)))
        gelu[rows, :] = (0.5 * u * (1.0 + t)).astype(BF16)
        slope = 0.5 * (1.0 + t) + 0.5 * u * (1.0 - t * t) * (GELU_A * (1.0 + 3.0 * GELU_B * (u * u)))
        d_up[rows, :] = (d_gelu[rows, :].astype(F32) * slope).astype(BF16)
        return carry
    lax.fori_loop(0, BLOCKS, activation, 0)
    project(d_up, w1, part3, WO_TILE, True)

    rs3.start()
    run(rs3.head())
    tail, y_head, y_tail = rs3.tail(), rsy.head(), rsy.tail()
    project(gelu, w2, part_y, 1024, False, 0, 2048)
    run(tail[:4])
    project(gelu, w2, part_y, 1024, False, 2048, 4096)
    rsy.start()
    run(tail[4:])
    run(y_head[:4])
    rs3.finish()

    def ln_backward(rs, z, mean, rstd, gain_ref, dg_row):
        sum_a = jnp.zeros((BLOCKS, LANES), F32)
        sum_b = jnp.zeros((BLOCKS, LANES), F32)
        for j in range(CHUNKS):
            d_norm = rs.total(j).astype(BF16).astype(F32)
            x_hat = (z(j) - mean) * rstd
            grad_row = jnp.sum(d_norm * x_hat, axis=0, keepdims=True)
            for i in range(CHUNK // LANES):
                at = j * (CHUNK // LANES) + i
                dg_part[at // 2, pl.ds(dg_row + at % 2, 1), :] = grad_row[:, i * LANES:(i + 1) * LANES]
            scaled = d_norm * gain(gain_ref, j)
            wide[:, span(j)] = scaled
            sum_a = sum_a + fold(scaled)
            sum_b = sum_b + fold(scaled * x_hat)
        mean_a = jnp.sum(sum_a, axis=-1, keepdims=True) / WIDTH
        mean_b = jnp.sum(sum_b, axis=-1, keepdims=True) / WIDTH
        for j in range(CHUNKS):
            c = span(j)
            x_hat = (z(j) - mean) * rstd
            wide[:, c] = rstd * (wide[:, c] - mean_a - x_hat * mean_b)

    ln_backward(rs3, lambda j: x1[:, span(j)].astype(F32), mean2, rstd2, g2, 2)
    for j in range(CHUNKS):
        c = span(j)
        value = (dy[own, :, c].astype(F32) + wide[:, c].astype(BF16).astype(F32)).astype(BF16)
        d_res[:, c] = value
        f2[own, :, c] = value
    ag3.start_far()
    ag3.start_near()
    steps = ag3.steps()
    run(steps[:12])
    run(y_head[4:])
    run(y_tail[:2])
    run(steps[12:])
    ag3.finish()

    d_attn[...] = dot_nt(f2[...].reshape(TOKENS, WIDTH), wo[...]).astype(BF16)
    run(y_tail[2:5])
    for h in range(2):
        q, k, v = [qkv[:, pl.ds(h * 384 + i * LANES, LANES)] for i in range(3)]
        d_o = d_attn[:, pl.ds(h * LANES, LANES)]
        p = prob[h]
        d_prob = dot_nt(d_o, v)
        d_score = p * (d_prob - jnp.sum(p * d_prob, axis=-1, keepdims=True)) * SCALE
        dqkv[:, pl.ds(h * 384, LANES)] = dot_nn(d_score.astype(BF16), k).astype(BF16)
        dqkv[:, pl.ds(h * 384 + LANES, LANES)] = dot_nn(d_score.T.astype(BF16), q).astype(BF16)
        dqkv[:, pl.ds(h * 384 + TOKENS, LANES)] = dot_nn(p.T.astype(BF16), d_o).astype(BF16)
    run(y_tail[5:])
    rs1.drain()
    project(dqkv, wqkv, part1, WO_TILE, True)

    rs4.start()
    run(rs4.head())
    rsy.finish()
    for j in range(CHUNKS):
        c = span(j)
        fy[own, :, c] = (x1[:, c].astype(F32) + rsy.total(j)).astype(BF16)
    run(rs4.tail())
    agy.start_near()
    rs4.finish()
    mean1, rstd1 = row_stats(lambda j: x[own, :, span(j)].astype(F32))
    ln_backward(rs4, lambda j: x[own, :, span(j)].astype(F32), mean1, rstd1, g1, 0)
    for j in range(CHUNKS):
        c = span(j)
        fx[own, :, c] = (d_res[:, c].astype(F32) + wide[:, c].astype(BF16).astype(F32)).astype(BF16)
    dg_copies = []

    def dg_send(src, dst, i, dev):
        cp = remote(src, dst, (dg_sems.at[0, i], dg_sems.at[1, i]), dev)
        dg_copies.append(cp)
        return cp
    in_core = dg_send(dg_part.at[pl.ds((1 - place.core) * 8, 8)], dg_core, 0, place.partner)
    ag4.start_far()
    agy.start_far()
    ag4.start_near()
    steps = ag4.steps()
    near, far = agy.late_steps()
    in_core.wait_recv()
    dg_core[...] = dg_core[...] + dg_part[pl.ds(place.core * 8, 8)]
    in_y = dg_send(dg_core.at[pl.ds((1 - place.y) * 4, 4)], dg_y, 6, place.y_peer)
    run(near)
    run(steps[:5])
    in_y.wait_recv()
    quarter = pl.ds(place.core * 8 + place.y * 4, 4)
    dg_z[place.z] = dg_core[pl.ds(place.y * 4, 4)] + dg_y[...]
    in_z = [dg_send(dg_z.at[place.z], dg_z.at[place.z], k, place.z_peers[k]) for k in (1, 2, 3)]
    run(steps[5:7])
    run(far[:2])
    agy.send_last()
    run(steps[7:10])
    run(far[2:3])
    for cp in in_z:
        cp.wait_recv()
    dg_full[quarter] = dg_z[0] + dg_z[1] + dg_z[2] + dg_z[3]
    in_y = dg_send(dg_full.at[quarter], dg_full.at[quarter], 4, place.y_peer)
    run(steps[10:13])
    run(far[3:6])
    in_y.wait_recv()
    mine = pl.ds(place.core * 8, 8)
    in_core = dg_send(dg_full.at[mine], dg_full.at[mine], 5, place.partner)
    run(steps[13:])
    in_core.wait_recv()
    for i in range(32):
        for row, out in ((0, dg1_out), (2, dg2_out)):
            out[pl.ds(i * LANES, LANES)] = dg_full[i // 2, row + i % 2].astype(BF16)
    ag4.finish()
    run(far[6:])
    agy.finish()

    for rs in (rs3, rsy, rs4):
        rs.drain()
    for ag in (ag1, ag3, agy, ag4):
        ag.drain()
    for cp in dg_copies:
        cp.wait_send()


def layer(x_in, d_y, gain_one, gain_two, seg_ids, w_qkv, w_out, w_up, w_down):
    hbm = pl.BlockSpec(memory_space=pl.ANY)
    vmem = pl.BlockSpec(memory_space=pltpu.VMEM)
    dma = pltpu.SemaphoreType.DMA

    def shape(*dims):
        return pltpu.VMEM(dims, BF16)

    def scratch(*dims, dtype=BF16):
        return pltpu.VMEM(dims, dtype)
    blocks = (BLOCKS, BLOCKS, WIDTH)
    return pl.pallas_call(
        layer_kernel,
        out_shape=[
            shape(*blocks), shape(*blocks), shape(WIDTH), shape(WIDTH), shape(*blocks), shape(TOKENS, QKV_COLS), shape(TOKENS, TOKENS), shape(*blocks),
            shape(*blocks), shape(TOKENS, FFN), shape(TOKENS, FFN), shape(*blocks),
        ],
        in_specs=[hbm, hbm, vmem, vmem, vmem, hbm, hbm, hbm, hbm],
        out_specs=[vmem] * 12,
        scratch_shapes=[
            scratch(*blocks), scratch(WIDTH, QKV_COLS), scratch(TOKENS, WIDTH), scratch(WIDTH, FFN), scratch(FFN, WIDTH),
        ] + [scratch(*blocks)] * 3 + [
            scratch(4, 4, 2, BLOCKS, WIDTH), scratch(4, 4, BLOCKS, WIDTH), scratch(4, 4, BLOCKS, WIDTH), scratch(4, 3, BLOCKS, WIDTH), scratch(4, 3, BLOCKS, WIDTH),
            scratch(4, 2, BLOCKS, WIDTH // 2), scratch(4, 2, BLOCKS, WIDTH // 2),
            scratch(TOKENS, QKV_COLS), scratch(2, TOKENS, TOKENS, dtype=F32), scratch(TOKENS, FFN), scratch(TOKENS, FFN),
            scratch(TOKENS, TOKENS), scratch(BLOCKS, WIDTH), scratch(BLOCKS, WIDTH), scratch(BLOCKS, WIDTH, dtype=F32),
            scratch(BLOCKS, 4, LANES, dtype=F32), scratch(8, 4, LANES, dtype=F32), scratch(4, 4, LANES, dtype=F32), scratch(4, 4, 4, LANES, dtype=F32),
            scratch(BLOCKS, 4, LANES, dtype=F32),
            dma((4, 2, 24)), dma((4, 2, 32)), dma((2, 7)), dma((6,)),
        ],
        compiler_params=pltpu.CompilerParams(collective_id=0, has_side_effects=True, vmem_limit_bytes=LAYER_VMEM),
        name='layer',
    )(
        x_in.reshape(blocks), d_y.reshape(blocks), gain_one, gain_two, seg_ids, w_qkv, w_out.reshape(TOKENS, WIDTH), w_up, w_down,
    )


TILE = 1024


def weight_grad_kernel(
    a, dqkv, o, dr, b1, du, gelu, dy, y, dx, dg1, dg2,
    dwqkv_hbm, dwo_hbm, dw1_hbm, dw2_hbm, y_out, dx_out, dg1_out, dg2_out,
    dwqkv, dwo, dw1, dw2, gelu_t, o_t, out_sems,
):
    stores = []

    def store(src, dst):
        cp = pltpu.make_async_copy(src, dst, out_sems.at[len(stores)])
        cp.start()
        stores.append(cp)

    def by_rows(lhs, rhs, out, out_hbm):
        for i in range(WIDTH // TILE):
            c = pl.ds(i * TILE, TILE)
            out[c, :] = lax.dot_general(lhs[:, c], rhs[...], (((0,), (0,)), ((), ())), preferred_element_type=F32).astype(BF16)
            store(out.at[c], out_hbm.at[c])

    def by_columns(lhs_t, rhs, out, out_hbm):
        for i in range(WIDTH // TILE):
            c = pl.ds(i * TILE, TILE)
            out[:, c] = dot_nn(lhs_t[...], rhs[:, c]).astype(BF16)
            store(out.at[:, c], out_hbm.at[:, c])

    store(y, y_out)
    store(dx, dx_out)
    store(dg1, dg1_out)
    store(dg2, dg2_out)
    by_rows(a, dqkv, dwqkv, dwqkv_hbm)
    by_rows(b1, du, dw1, dw1_hbm)
    gelu_t[...] = gelu[...].T
    by_columns(gelu_t, dy, dw2, dw2_hbm)
    o_t[...] = o[...].T
    by_columns(o_t, dr, dwo, dwo_hbm)
    for cp in stores:
        cp.wait()


def weight_grads(*operands):
    hbm = pl.BlockSpec(memory_space=pl.ANY)
    vmem = pl.BlockSpec(memory_space=pltpu.VMEM)
    big = (TOKENS, WIDTH)
    ins = [big, (TOKENS, QKV_COLS), (TOKENS, TOKENS), big, big, (TOKENS, FFN), (TOKENS, FFN), big, big, big, (WIDTH,), (WIDTH,)]
    outs = [(WIDTH, QKV_COLS), big, (WIDTH, FFN), (FFN, WIDTH), big, big, (WIDTH,), (WIDTH,)]
    return pl.pallas_call(
        weight_grad_kernel,
        out_shape=[jax.ShapeDtypeStruct(dims, BF16) for dims in outs],
        in_specs=[vmem] * len(ins),
        out_specs=[hbm] * len(outs),
        scratch_shapes=[pltpu.VMEM(dims, BF16) for dims in outs[:4] + [(FFN, TOKENS), (TOKENS, TOKENS)]] + [pltpu.SemaphoreType.DMA((20,))],
        compiler_params=pltpu.CompilerParams(vmem_limit_bytes=GRADS_VMEM),
        name='weight_grads',
    )(*[v.reshape(dims) for v, dims in zip(operands, ins)])


def solution(mesh):
    def local_step(x_in, seg_ids, gain_one, w_qkv, w_out, gain_two, w_up, w_down, d_y):
        y, d_x, gains_one, gains_two, normed_one, d_qkv, attn_out, d_resid, normed_two, d_up, gelu_out, d_y_here = layer(
            x_in, d_y, gain_one, gain_two, seg_ids, w_qkv, w_out, w_up, w_down)
        d_w_qkv, d_w_out, d_w_up, d_w_down, y_out, d_x_out, d_gain_one, d_gain_two = weight_grads(
            normed_one, d_qkv, attn_out, d_resid, normed_two, d_up, gelu_out, d_y_here, y, d_x, gains_one, gains_two)
        return y_out.reshape(x_in.shape), d_x_out.reshape(x_in.shape), d_w_qkv, d_w_out.reshape(w_out.shape), d_w_up, d_w_down, d_gain_one, d_gain_two

    in_specs = (P('data'), P('data'), P(), P(None, 'model'), P('model'), P(), P(None, 'model'), P('model'), P('data'))
    out_specs = (P('data'), P('data'), P('data', 'model'), P(('data', 'model')), P('data', 'model'), P(('data', 'model')), P('data'), P('data'))
    return jax.shard_map(local_step, mesh=mesh, in_specs=in_specs, out_specs=out_specs, check_vma=False)
```

```python
import jax
import jax.numpy as jnp
from jax import lax
from jax.experimental import pallas as pl
from jax.experimental.pallas import tpu as pltpu
from jax.sharding import PartitionSpec as P

LN_EPS = 1e-5
MESH = pl.DeviceIdType.MESH
BF16 = jnp.bfloat16
F32 = jnp.float32
WIDTH = 4096
CHUNK = 512
WO_TILE = 2048
LAYER_VMEM = 49 * 2 ** 20
GRADS_VMEM = 28 * 2 ** 20
TOKENS = 256
LANES = 128
BLOCKS = 16
FFN = 896
QKV_COLS = 768
CHUNKS = WIDTH // CHUNK
HALF = WIDTH // 2
CORE_ORDER = [(3, 1), (1, 1), (1, 0), (2, 1), (0, 1), (3, 0), (2, 0), (0, 0)]
SCALE = LANES ** -0.5
GELU_A = 0.7978845608028654
GELU_B = 0.044715


def flip(z, k):
    high, low = lax.div(z, 2), lax.rem(z, 2)
    return (1 - high if k >= 2 else high) * 2 + (1 - low if k % 2 else low)


def dot_nn(a, b):
    return jnp.dot(a, b, preferred_element_type=F32)


def dot_nt(a, b):
    return lax.dot_general(a, b, (((1,), (1,)), ((), ())), preferred_element_type=F32)


def span(j):
    return pl.ds(j * CHUNK, CHUNK)


class Exchange:
    pieces = 2

    def __init__(self, place, sems):
        self.place, self.sems = place, sems
        self.all = range(self.pieces)
        self.low, self.high = self.all[:self.pieces // 2], self.all[self.pieces // 2:]
        self.width = WIDTH // self.pieces

    def piece(self, h):
        return pl.ds(h * self.width, self.width)

    def spans(self, h):
        n = CHUNKS // self.pieces
        return [span(h * n + j) for j in range(n)]

    def remote(self, src, dst, i, dev):
        cp = pltpu.make_async_remote_copy(src_ref=src, dst_ref=dst, send_sem=self.sems.at[0], recv_sem=self.sems.at[1 + i], device_id=dev, device_id_type=MESH)
        cp.start()
        return cp

    def drain(self):
        sent = self.whole.at[pl.ds(0, BLOCKS - 1)]
        pltpu.make_async_copy(sent, sent, self.sems.at[0]).wait()


def fold(v):
    return sum(v[..., i * LANES:(i + 1) * LANES] for i in range(CHUNK // LANES))


def row_stats(wide):
    total = sum(fold(wide(j)) for j in range(CHUNKS))
    mean = jnp.sum(total, axis=-1, keepdims=True) / WIDTH

    def square(j):
        centered = wide(j) - mean
        return fold(centered * centered)
    total = sum(square(j) for j in range(CHUNKS))
    var = jnp.sum(total, axis=-1, keepdims=True) / WIDTH
    return mean, lax.rsqrt(var + LN_EPS)


class Place:
    def __init__(self):
        me = lax.axis_index('model')
        self.core, self.y, self.z = lax.rem(me, 2), lax.rem(lax.div(me, 2), 2), lax.div(me, 4)
        self.partner = {'model': me + 1 - 2 * self.core}
        self.y_peer = {'model': me + 2 - 4 * self.y}
        self.z_at = [flip(self.z, k) for k in range(4)]
        self.z_peers = [{'model': me + (at - self.z) * 4} for at in self.z_at]
        self.blocks = {
            (i, j, k): (1 - self.core if i else self.core) * 8 + (1 - self.y if j else self.y) * 4 + self.z_at[k]
            for i in (0, 1) for j in (0, 1) for k in range(4)
        }
        self.own = self.blocks[0, 0, 0]

    def block(self, i, j, k):
        return self.blocks[i, j, k]


class ReduceScatter(Exchange):
    def __init__(self, place, part, bufs, sems):
        super().__init__(place, sems)
        self.part = self.whole = part
        self.buf_core, self.out_y, self.buf_y, self.out_z, self.buf_z, self.out_first, self.buf_first = bufs
        self.core_in, self.y_in, self.z_in, self.first_in = {}, {}, {}, {}
        self.ready, self.first_ready = set(), False

    def block(self, k, j):
        return self.place.block(0, j, k)

    def start(self):
        p = self.place
        for k, j in CORE_ORDER:
            b = p.block(1, j, k)
            self.core_in[k, j] = self.remote(self.part.at[b], self.buf_core.at[k, j], k * 2 + j, p.partner)

    def core_ready(self, k, j):
        if (k, j) not in self.ready:
            self.core_in[k, j].wait_recv()
            self.ready.add((k, j))

    def pair_sum(self, k, j, c):
        return self.part[self.block(k, j), :, c].astype(F32) + self.buf_core[k, j, :, c].astype(F32)

    def chip_sum(self, k, c):
        return self.pair_sum(k, 0, c) + self.buf_y[k, :, c].astype(F32)

    def send_y(self, k, h):
        self.core_ready(k, 1)
        with_first = k == 0 and h in self.high
        if with_first and not self.first_ready:
            self.first_in[1].wait_recv()
            self.first_ready = True
        for c in self.spans(h):
            t = self.pair_sum(k, 1, c)
            if with_first:
                t = t + self.buf_first[1, :, pl.ds(c.start - HALF, CHUNK)].astype(F32)
            self.out_y[k, :, c] = t.astype(BF16)
        self.y_in[k, h] = self.remote(self.out_y.at[k, :, self.piece(h)], self.buf_y.at[k, :, self.piece(h)], 8 + k * self.pieces + h, self.place.y_peer)

    def send_first(self):
        for j in (1, 0):
            self.core_ready(1, j)
            for j2 in range(CHUNKS // 2):
                self.out_first[j, :, span(j2)] = self.pair_sum(1, j, span(CHUNKS // 2 + j2)).astype(BF16)
            self.first_in[j] = self.remote(self.out_first.at[j], self.buf_first.at[j], 8 + 7 * self.pieces + j, self.place.z_peers[1])

    def send_z(self, k, h):
        self.core_ready(k, 0)
        self.y_in[k, h].wait_recv()
        if k == 2:
            self.z_in[3, h].wait_recv()
        for c in self.spans(h):
            t = self.chip_sum(k, c)
            if k == 2:
                t = t + self.buf_z[2, :, c].astype(F32)
            self.out_z[k - 1, :, c] = t.astype(BF16)
        i = 8 + (3 + k) * self.pieces + h
        self.z_in[k, h] = self.remote(self.out_z.at[k - 1, :, self.piece(h)], self.buf_z.at[k - 1, :, self.piece(h)], i, self.place.z_peers[2 if k == 2 else 1])

    def head(self):
        y = {(k, h): (lambda k=k, h=h: self.send_y(k, h)) for k in range(4) for h in self.all}
        return [y[3, 0], y[3, 1], self.send_first, y[1, 0], y[2, 0], y[2, 1], y[0, 0]]

    def tail(self):
        z = {(k, h): (lambda k=k, h=h: self.send_z(k, h)) for k in range(4) for h in self.all}
        return [z[3, 0], z[3, 1], lambda: self.send_y(0, 1), z[1, 0], z[2, 0], z[2, 1]]

    def finish(self):
        self.core_ready(0, 0)
        for h in self.all:
            self.y_in[0, h].wait_recv()
        self.first_in[0].wait_recv()
        for h in self.low:
            self.z_in[1, h].wait_recv()
        for h in self.all:
            self.z_in[2, h].wait_recv()

    def total(self, j):
        c = span(j)
        near = self.buf_z[0, :, c] if j < CHUNKS // 2 else self.buf_first[0, :, span(j - CHUNKS // 2)]
        return self.chip_sum(0, c) + near.astype(F32) + self.buf_z[1, :, c].astype(F32)


class Gather(Exchange):
    def __init__(self, place, full, sems):
        super().__init__(place, sems)
        self.full = self.whole = full
        self.z_in, self.y_in, self.core_in, self.last_in = {}, {}, {}, {}

    def send(self, j, k, h, i, dev):
        b = self.place.block(0, j, k)
        ref = self.full.at[b] if h is None else self.full.at[b, :, self.piece(h)]
        return self.remote(ref, ref, i, dev)

    def to_core(self, j, k, h):
        self.core_in[j, k, h] = self.send(j, k, h, (8 + j * 4 + k) * self.pieces + h, self.place.partner)

    def to_y(self, k, h):
        self.y_in[k, h] = self.send(0, k, h, (4 + k) * self.pieces + h, self.place.y_peer)

    def to_z(self, k, h):
        self.z_in[k, h] = self.send(0, 2 if k == 3 else 0, h, k * self.pieces + h, self.place.z_peers[2 if k == 2 else 1])

    def start_far(self):
        for h in self.all:
            self.to_z(2, h)

    def start_near(self):
        for h in self.all:
            self.to_y(0, h)
            self.to_z(1, h)
        self.core_in[0, 0, None] = self.send(0, 0, None, 8 * self.pieces, self.place.partner)

    def from_z(self, k, h):
        self.z_in[k, h].wait_recv()
        if k == 2:
            self.to_z(3, h)
        if k != 1 or h in self.low:
            self.to_y(k, h)
        self.to_core(0, k, h)

    def from_y(self, k, h):
        self.y_in[k, h].wait_recv()
        self.to_core(1, k, h)

    def send_last(self):
        for h in self.high:
            self.last_in[h] = self.send(1, 0, h, h - self.pieces // 2, self.place.z_peers[1])

    def from_last(self):
        for h in self.high:
            self.last_in[h].wait_recv()
            self.to_core(1, 1, h)

    def steps(self):
        y = {(k, h): (lambda k=k, h=h: self.from_y(k, h)) for k in range(4) for h in self.all}
        z = {(k, h): (lambda k=k, h=h: self.from_z(k, h)) for k in range(4) for h in self.all}
        return [
            y[0, 0], z[2, 0], y[0, 1], z[2, 1], self.send_last, z[1, 0], z[1, 1], y[2, 0], y[2, 1], z[3, 0],
            y[1, 0], z[3, 1], self.from_last, y[3, 0], y[3, 1],
        ]

    def late_steps(self):
        near = [(lambda h=h: self.from_y(0, h)) for h in self.all] + [(lambda h=h: self.from_z(1, h)) for h in self.all]
        far = [(lambda h=h: self.from_z(2, h)) for h in self.all]
        end = [(lambda h=h: self.from_y(1, h)) for h in self.low] + [(lambda h=h: self.from_z(3, h)) for h in self.all]
        end += [(lambda h=h: self.from_y(2, h)) for h in self.all] + [self.from_last] + [(lambda h=h: self.from_y(3, h)) for h in self.all]
        return near, far, end

    def finish(self):
        for cp in self.core_in.values():
            cp.wait_recv()


def run(steps):
    for step in steps:
        step()


def layer_kernel(
    x_hbm, dy_hbm, g1, g2, seg, wqkv_hbm, wo_hbm, w1_hbm, w2_hbm,
    fy, fx, dg1_out, dg2_out, a, dqkv, o, f2, f1, d_up, gelu, dy,
    x, wqkv, wo, w1, w2, part1, part3, part_y,
    core_buf, yout_buf, y_buf, zout_buf, z_buf, fout_buf, first_buf,
    qkv, prob, up, d_gelu, d_attn, x1, d_res, wide, dg_part, dg_core, dg_y, dg_z, dg_full,
    rs_sems, ag_sems, dg_sems, in_sems,
):
    place = Place()
    own = place.own

    loads = [
        pltpu.make_async_copy(src, dst, in_sems.at[i])
        for i, (src, dst) in enumerate(
            [(x_hbm.at[pl.ds(r * 4, 4)], x.at[pl.ds(r * 4, 4)]) for r in range(4)]
            + [(wqkv_hbm, wqkv), (wo_hbm, wo), (dy_hbm, dy), (w2_hbm, w2), (w1_hbm, w1)])
    ]
    load_x, (load_wqkv, load_wo, load_dy, load_w2, load_w1) = loads[:4], loads[4:]
    for cp in load_x + [load_wqkv]:
        cp.start()
    barrier = pltpu.get_barrier_semaphore()
    for dev in [place.partner, place.y_peer] + place.z_peers[1:]:
        pl.semaphore_signal(barrier, inc=1, device_id=dev, device_id_type=MESH)

    def rs_set(i, part):
        bufs = [ref.at[i] for ref in (core_buf, yout_buf, y_buf, zout_buf, z_buf, fout_buf, first_buf)]
        return ReduceScatter(place, part, bufs, rs_sems.at[i])

    rs1, rs3, rsy, rs4 = rs_set(0, part1), rs_set(0, part3), rs_set(1, part_y), rs_set(0, part1)
    ag1, ag3, agy, ag4 = [Gather(place, ref, ag_sems.at[i]) for i, ref in ((0, f1), (0, f2), (1, fy), (0, fx))]

    def gain(ref, j):
        return ref[span(j)].astype(F32).reshape(1, CHUNK)

    def ln_one(i, carry):
        rows = pl.ds(i * 2, 2)
        mean, rstd = row_stats(lambda j: x[rows, :, span(j)].astype(F32))
        for j in range(CHUNKS):
            c = span(j)
            normed = (x[rows, :, c].astype(F32) - mean) * rstd * gain(g1, j)[None]
            a[rows, :, c] = normed.astype(BF16)
        return carry
    for r in range(4):
        load_x[r].wait()
        lax.fori_loop(r * 2, r * 2 + 2, ln_one, 0)
    for cp in (load_wo, load_dy, load_w2, load_w1):
        cp.start()

    load_wqkv.wait()
    qkv[...] = dot_nn(a[...].reshape(TOKENS, WIDTH), wqkv[...]).astype(BF16)

    q_pos = lax.broadcasted_iota(jnp.int32, (TOKENS, TOKENS), 0)
    k_pos = lax.broadcasted_iota(jnp.int32, (TOKENS, TOKENS), 1)
    seg_keys = jnp.broadcast_to(seg[...].astype(F32), (TOKENS, TOKENS))
    allowed = (q_pos >= k_pos) & (seg_keys.T == seg_keys)
    for h in range(2):
        q, k, v = [qkv[:, pl.ds(h * 384 + i * LANES, LANES)] for i in range(3)]
        scores = jnp.where(allowed, dot_nt(q, k) * SCALE, -1e30)
        exp_scores = jnp.exp(scores - jnp.max(scores, axis=-1, keepdims=True))
        p = exp_scores / jnp.sum(exp_scores, axis=-1, keepdims=True)
        prob[h] = p
        o[:, pl.ds(h * LANES, LANES)] = dot_nn(p.astype(BF16), v).astype(BF16)

    def project(lhs, weight, part, tile, transposed, lo=0, hi=WIDTH):
        def step(i, carry):
            c = pl.ds(pl.multiple_of(lo + i * tile, tile), tile)
            r = dot_nt(lhs[...], weight[c, :]) if transposed else dot_nn(lhs[...], weight[:, c])
            part[:, :, c] = r.astype(BF16).reshape(BLOCKS, BLOCKS, tile)
            return carry
        lax.fori_loop(0, (hi - lo) // tile, step, 0)

    load_wo.wait()
    project(o, wo, part1, WO_TILE, False)
    pl.semaphore_wait(barrier, 5)

    rs1.start()
    run(rs1.head())

    def d_gelu_tile(lo, n):
        c = pl.ds(lo, n)
        d_gelu[:, c] = dot_nt(dy[...].reshape(TOKENS, WIDTH), w2[c, :]).astype(BF16)
    load_dy.wait()
    load_w2.wait()
    tail = rs1.tail()
    d_gelu_tile(0, TOKENS)
    run(tail[:4])
    d_gelu_tile(TOKENS, TOKENS)
    run(tail[4:5])
    d_gelu_tile(512, TOKENS)
    run(tail[5:])
    d_gelu_tile(QKV_COLS, LANES)
    rs1.finish()

    for j in range(CHUNKS):
        c = span(j)
        x1[:, c] = (x[own, :, c].astype(F32) + rs1.total(j)).astype(BF16)
    mean2, rstd2 = row_stats(lambda j: x1[:, span(j)].astype(F32))
    for j in range(CHUNKS):
        c = span(j)
        f1[own, :, c] = ((x1[:, c].astype(F32) - mean2) * rstd2 * gain(g2, j)).astype(BF16)
    ag1.start_far()
    ag1.start_near()
    run(ag1.steps())
    load_w1.wait()
    ag1.finish()
    rs1.drain()

    for lo, n in ((0, 512), (512, 384)):
        c = pl.ds(lo, n)
        up[:, c] = dot_nn(f1[...].reshape(TOKENS, WIDTH), w1[:, c]).astype(BF16)

    def activation(i, carry):
        rows = pl.ds(pl.multiple_of(i * BLOCKS, BLOCKS), BLOCKS)
        u = up[rows, :].astype(F32)
        t = jnp.tanh(GELU_A * (u + GELU_B * (u * u * u)))
        gelu[rows, :] = (0.5 * u * (1.0 + t)).astype(BF16)
        slope = 0.5 * (1.0 + t) + 0.5 * u * (1.0 - t * t) * (GELU_A * (1.0 + 3.0 * GELU_B * (u * u)))
        d_up[rows, :] = (d_gelu[rows, :].astype(F32) * slope).astype(BF16)
        return carry
    lax.fori_loop(0, BLOCKS, activation, 0)
    project(d_up, w1, part3, WO_TILE, True)

    rs3.start()
    run(rs3.head())
    tail, y_head, y_tail = rs3.tail(), rsy.head(), rsy.tail()
    project(gelu, w2, part_y, 1024, False, 0, 2048)
    run(tail[:4])
    project(gelu, w2, part_y, 1024, False, 2048, 4096)
    rsy.start()
    run(tail[4:])
    run(y_head[:4])
    rs3.finish()

    def ln_backward(rs, z, mean, rstd, gain_ref, dg_row):
        sum_a = jnp.zeros((BLOCKS, LANES), F32)
        sum_b = jnp.zeros((BLOCKS, LANES), F32)
        for j in range(CHUNKS):
            d_norm = rs.total(j).astype(BF16).astype(F32)
            x_hat = (z(j) - mean) * rstd
            grad_row = jnp.sum(d_norm * x_hat, axis=0, keepdims=True)
            for i in range(CHUNK // LANES):
                at = j * (CHUNK // LANES) + i
                dg_part[at // 2, pl.ds(dg_row + at % 2, 1), :] = grad_row[:, i * LANES:(i + 1) * LANES]
            scaled = d_norm * gain(gain_ref, j)
            wide[:, span(j)] = scaled
            sum_a = sum_a + fold(scaled)
            sum_b = sum_b + fold(scaled * x_hat)
        mean_a = jnp.sum(sum_a, axis=-1, keepdims=True) / WIDTH
        mean_b = jnp.sum(sum_b, axis=-1, keepdims=True) / WIDTH
        for j in range(CHUNKS):
            c = span(j)
            x_hat = (z(j) - mean) * rstd
            wide[:, c] = rstd * (wide[:, c] - mean_a - x_hat * mean_b)

    ln_backward(rs3, lambda j: x1[:, span(j)].astype(F32), mean2, rstd2, g2, 2)
    for j in range(CHUNKS):
        c = span(j)
        value = (dy[own, :, c].astype(F32) + wide[:, c].astype(BF16).astype(F32)).astype(BF16)
        d_res[:, c] = value
        f2[own, :, c] = value
    ag1.drain()
    ag3.start_far()
    ag3.start_near()
    steps = ag3.steps()
    last = steps.index(ag3.from_last)
    run(steps[:last])
    run(y_head[4:])
    run(y_tail[:2])
    run(steps[last:])
    ag3.finish()

    d_attn[...] = dot_nt(f2[...].reshape(TOKENS, WIDTH), wo[...]).astype(BF16)
    run(y_tail[2:5])
    for h in range(2):
        q, k, v = [qkv[:, pl.ds(h * 384 + i * LANES, LANES)] for i in range(3)]
        d_o = d_attn[:, pl.ds(h * LANES, LANES)]
        p = prob[h]
        d_prob = dot_nt(d_o, v)
        d_score = p * (d_prob - jnp.sum(p * d_prob, axis=-1, keepdims=True)) * SCALE
        dqkv[:, pl.ds(h * 384, LANES)] = dot_nn(d_score.astype(BF16), k).astype(BF16)
        dqkv[:, pl.ds(h * 384 + LANES, LANES)] = dot_nn(d_score.T.astype(BF16), q).astype(BF16)
        dqkv[:, pl.ds(h * 384 + TOKENS, LANES)] = dot_nn(p.T.astype(BF16), d_o).astype(BF16)
    run(y_tail[5:])
    rs3.drain()
    project(dqkv, wqkv, part1, WO_TILE, True)

    rs4.start()
    run(rs4.head())
    rsy.finish()
    for j in range(CHUNKS):
        c = span(j)
        fy[own, :, c] = (x1[:, c].astype(F32) + rsy.total(j)).astype(BF16)
    run(rs4.tail())
    agy.start_near()
    rs4.finish()
    mean1, rstd1 = row_stats(lambda j: x[own, :, span(j)].astype(F32))
    ln_backward(rs4, lambda j: x[own, :, span(j)].astype(F32), mean1, rstd1, g1, 0)
    for j in range(CHUNKS):
        c = span(j)
        fx[own, :, c] = (d_res[:, c].astype(F32) + wide[:, c].astype(BF16).astype(F32)).astype(BF16)
    dg_copies = []

    def dg_send(src, dst, i, dev):
        cp = pltpu.make_async_remote_copy(src_ref=src, dst_ref=dst, send_sem=dg_sems.at[0, i], recv_sem=dg_sems.at[1, i], device_id=dev, device_id_type=MESH)
        cp.start()
        dg_copies.append(cp)
        return cp
    in_core = dg_send(dg_part.at[pl.ds((1 - place.core) * 8, 8)], dg_core, 0, place.partner)
    ag3.drain()
    ag4.start_far()
    agy.start_far()
    ag4.start_near()
    steps = ag4.steps()
    near, far, end = agy.late_steps()
    last, mid = steps.index(ag4.from_last), steps.index(ag4.send_last)
    in_core.wait_recv()
    dg_core[...] = dg_core[...] + dg_part[pl.ds(place.core * 8, 8)]
    in_y = dg_send(dg_core.at[pl.ds((1 - place.y) * 4, 4)], dg_y, 6, place.y_peer)
    run(near)
    run(steps[:mid + 1])
    in_y.wait_recv()
    quarter = pl.ds(place.core * 8 + place.y * 4, 4)
    dg_z[place.z] = dg_core[pl.ds(place.y * 4, 4)] + dg_y[...]
    in_z = [dg_send(dg_z.at[place.z], dg_z.at[place.z], k, place.z_peers[k]) for k in (1, 2, 3)]
    run(steps[mid + 1:mid + 3])
    run(far)
    agy.send_last()
    run(steps[mid + 3:last - 2])
    run(end[:2 // 2])
    for cp in in_z:
        cp.wait_recv()
    dg_full[quarter] = dg_z[0] + dg_z[1] + dg_z[2] + dg_z[3]
    in_y = dg_send(dg_full.at[quarter], dg_full.at[quarter], 4, place.y_peer)
    run(steps[last - 2:last + 1])
    run(end[2 // 2:2 * 2])
    in_y.wait_recv()
    mine = pl.ds(place.core * 8, 8)
    in_core = dg_send(dg_full.at[mine], dg_full.at[mine], 5, place.partner)
    run(steps[last + 1:])
    in_core.wait_recv()
    for i in range(32):
        for row, out in ((0, dg1_out), (2, dg2_out)):
            out[pl.ds(i * LANES, LANES)] = dg_full[i // 2, row + i % 2].astype(BF16)
    ag4.finish()
    run(end[2 * 2:])
    agy.finish()

    for exchange in (rs4, ag4, rsy, agy):
        exchange.drain()
    for cp in dg_copies:
        cp.wait_send()


def layer(x_in, d_y, gain_one, gain_two, seg_ids, w_qkv, w_out, w_up, w_down):
    hbm = pl.BlockSpec(memory_space=pl.ANY)
    vmem = pl.BlockSpec(memory_space=pltpu.VMEM)
    dma = pltpu.SemaphoreType.DMA

    def shape(*dims):
        return pltpu.VMEM(dims, BF16)

    def scratch(*dims, dtype=BF16):
        return pltpu.VMEM(dims, dtype)
    blocks = (BLOCKS, BLOCKS, WIDTH)
    return pl.pallas_call(
        layer_kernel,
        out_shape=[
            shape(*blocks), shape(*blocks), shape(WIDTH), shape(WIDTH), shape(*blocks), shape(TOKENS, QKV_COLS), shape(TOKENS, TOKENS), shape(*blocks),
            shape(*blocks), shape(TOKENS, FFN), shape(TOKENS, FFN), shape(*blocks),
        ],
        in_specs=[hbm, hbm, vmem, vmem, vmem, hbm, hbm, hbm, hbm],
        out_specs=[vmem] * 12,
        scratch_shapes=[
            scratch(*blocks), scratch(WIDTH, QKV_COLS), scratch(TOKENS, WIDTH), scratch(WIDTH, FFN), scratch(FFN, WIDTH),
        ] + [scratch(*blocks)] * 3 + [
            scratch(2, 4, 2, BLOCKS, WIDTH), scratch(2, 4, BLOCKS, WIDTH), scratch(2, 4, BLOCKS, WIDTH), scratch(2, 3, BLOCKS, WIDTH), scratch(2, 3, BLOCKS, WIDTH),
            scratch(2, 2, BLOCKS, HALF), scratch(2, 2, BLOCKS, HALF),
            scratch(TOKENS, QKV_COLS), scratch(2, TOKENS, TOKENS, dtype=F32), scratch(TOKENS, FFN), scratch(TOKENS, FFN),
            scratch(TOKENS, TOKENS), scratch(BLOCKS, WIDTH), scratch(BLOCKS, WIDTH), scratch(BLOCKS, WIDTH, dtype=F32),
            scratch(BLOCKS, 4, LANES, dtype=F32), scratch(8, 4, LANES, dtype=F32), scratch(4, 4, LANES, dtype=F32), scratch(4, 4, 4, LANES, dtype=F32),
            scratch(BLOCKS, 4, LANES, dtype=F32),
            dma((2, 11 + 7 * ReduceScatter.pieces)), dma((2, 1 + BLOCKS * Gather.pieces)), dma((2, 7)), dma((9,)),
        ],
        compiler_params=pltpu.CompilerParams(collective_id=0, has_side_effects=True, vmem_limit_bytes=LAYER_VMEM),
        name='layer',
    )(
        x_in.reshape(blocks), d_y.reshape(blocks), gain_one, gain_two, seg_ids, w_qkv, w_out.reshape(TOKENS, WIDTH), w_up, w_down,
    )


TILE = 1024


def weight_grad_kernel(
    a, dqkv, o, dr, b1, du, gelu, dy, y, dx, dg1, dg2,
    dwqkv_hbm, dwo_hbm, dw1_hbm, dw2_hbm, y_out, dx_out, dg1_out, dg2_out,
    dwqkv, dwo, dw1, dw2, gelu_t, o_t, out_sems,
):
    stores = []

    def store(src, dst):
        cp = pltpu.make_async_copy(src, dst, out_sems.at[len(stores)])
        cp.start()
        stores.append(cp)

    def by_rows(lhs, rhs, out, out_hbm):
        for i in range(WIDTH // TILE):
            c = pl.ds(i * TILE, TILE)
            out[c, :] = lax.dot_general(lhs[:, c], rhs[...], (((0,), (0,)), ((), ())), preferred_element_type=F32).astype(BF16)
            store(out.at[c], out_hbm.at[c])

    def by_columns(lhs_t, rhs, out, out_hbm):
        for i in range(WIDTH // TILE):
            c = pl.ds(i * TILE, TILE)
            out[:, c] = dot_nn(lhs_t[...], rhs[:, c]).astype(BF16)
            store(out.at[:, c], out_hbm.at[:, c])

    store(y, y_out)
    store(dx, dx_out)
    store(dg1, dg1_out)
    store(dg2, dg2_out)
    by_rows(a, dqkv, dwqkv, dwqkv_hbm)
    by_rows(b1, du, dw1, dw1_hbm)
    gelu_t[...] = gelu[...].T
    by_columns(gelu_t, dy, dw2, dw2_hbm)
    o_t[...] = o[...].T
    by_columns(o_t, dr, dwo, dwo_hbm)
    for cp in stores:
        cp.wait()


def weight_grads(*operands):
    hbm = pl.BlockSpec(memory_space=pl.ANY)
    vmem = pl.BlockSpec(memory_space=pltpu.VMEM)
    big = (TOKENS, WIDTH)
    ins = [big, (TOKENS, QKV_COLS), (TOKENS, TOKENS), big, big, (TOKENS, FFN), (TOKENS, FFN), big, big, big, (WIDTH,), (WIDTH,)]
    outs = [(WIDTH, QKV_COLS), big, (WIDTH, FFN), (FFN, WIDTH), big, big, (WIDTH,), (WIDTH,)]
    return pl.pallas_call(
        weight_grad_kernel,
        out_shape=[jax.ShapeDtypeStruct(dims, BF16) for dims in outs],
        in_specs=[vmem] * len(ins),
        out_specs=[hbm] * len(outs),
        scratch_shapes=[pltpu.VMEM(dims, BF16) for dims in outs[:4] + [(FFN, TOKENS), (TOKENS, TOKENS)]] + [pltpu.SemaphoreType.DMA((20,))],
        compiler_params=pltpu.CompilerParams(vmem_limit_bytes=GRADS_VMEM),
        name='weight_grads',
    )(*[v.reshape(dims) for v, dims in zip(operands, ins)])


def solution(mesh):
    def local_step(x_in, seg_ids, gain_one, w_qkv, w_out, gain_two, w_up, w_down, d_y):
        y, d_x, gains_one, gains_two, normed_one, d_qkv, attn_out, d_resid, normed_two, d_up, gelu_out, d_y_here = layer(
            x_in, d_y, gain_one, gain_two, seg_ids, w_qkv, w_out, w_up, w_down)
        d_w_qkv, d_w_out, d_w_up, d_w_down, y_out, d_x_out, d_gain_one, d_gain_two = weight_grads(
            normed_one, d_qkv, attn_out, d_resid, normed_two, d_up, gelu_out, d_y_here, y, d_x, gains_one, gains_two)
        return y_out.reshape(x_in.shape), d_x_out.reshape(x_in.shape), d_w_qkv, d_w_out.reshape(w_out.shape), d_w_up, d_w_down, d_gain_one, d_gain_two

    in_specs = (P('data'), P('data'), P(), P(None, 'model'), P('model'), P(), P(None, 'model'), P('model'), P('data'))
    out_specs = (P('data'), P('data'), P('data', 'model'), P(('data', 'model')), P('data', 'model'), P(('data', 'model')), P('data'), P('data'))
    return jax.shard_map(local_step, mesh=mesh, in_specs=in_specs, out_specs=out_specs, check_vma=False)
```

```python
import jax
import jax.numpy as jnp
from jax import lax
from jax.experimental import pallas as pl
from jax.experimental.pallas import tpu as pltpu
from jax.sharding import PartitionSpec as P

LN_EPS = 1e-5
MESH = pl.DeviceIdType.MESH
BF16 = jnp.bfloat16
F32 = jnp.float32
WIDTH = 4096
CHUNK = 512
LAYER_VMEM = 49 * 2 ** 20
GRADS_VMEM = 28 * 2 ** 20
TOKENS = 256
LANES = 128
BLOCKS = 16
FFN = 896
QKV_COLS = 768
CHUNKS = WIDTH // CHUNK
HALF = WIDTH // 2
CORE_ORDER = [(3, 1), (1, 1), (1, 0), (2, 1), (3, 0), (0, 1), (2, 0), (0, 0)]
SCALE = LANES ** -0.5
GELU_A = 0.7978845608028654
GELU_B = 0.044715


def flip(z, k):
    high, low = lax.div(z, 2), lax.rem(z, 2)
    return (1 - high if k >= 2 else high) * 2 + (1 - low if k % 2 else low)


def dot_nn(a, b):
    return jnp.dot(a, b, preferred_element_type=F32)


def dot_nt(a, b):
    return lax.dot_general(a, b, (((1,), (1,)), ((), ())), preferred_element_type=F32)


def span(j):
    return pl.ds(j * CHUNK, CHUNK)


class Exchange:
    pieces = 2

    def __init__(self, place, sems):
        self.place, self.sems = place, sems
        self.all = range(self.pieces)
        self.low, self.high = self.all[:self.pieces // 2], self.all[self.pieces // 2:]
        self.width = WIDTH // self.pieces

    def piece(self, h):
        return pl.ds(h * self.width, self.width)

    def spans(self, h):
        n = CHUNKS // self.pieces
        return [span(h * n + j) for j in range(n)]

    def remote(self, src, dst, i, dev):
        cp = pltpu.make_async_remote_copy(src_ref=src, dst_ref=dst, send_sem=self.sems.at[0], recv_sem=self.sems.at[1 + i], device_id=dev, device_id_type=MESH)
        cp.start()
        return cp

    def drain(self):
        sent = self.whole.at[pl.ds(0, BLOCKS - 1)]
        pltpu.make_async_copy(sent, sent, self.sems.at[0]).wait()


def fold(v):
    return sum(v[..., i * LANES:(i + 1) * LANES] for i in range(CHUNK // LANES))


def row_stats(wide):
    total = sum(fold(wide(j)) for j in range(CHUNKS))
    mean = jnp.sum(total, axis=-1, keepdims=True) / WIDTH

    def square(j):
        centered = wide(j) - mean
        return fold(centered * centered)
    total = sum(square(j) for j in range(CHUNKS))
    var = jnp.sum(total, axis=-1, keepdims=True) / WIDTH
    return mean, lax.rsqrt(var + LN_EPS)


class Place:
    def __init__(self):
        me = lax.axis_index('model')
        self.core, self.y, self.z = lax.rem(me, 2), lax.rem(lax.div(me, 2), 2), lax.div(me, 4)
        self.partner = {'model': me + 1 - 2 * self.core}
        self.y_peer = {'model': me + 2 - 4 * self.y}
        self.z_at = [flip(self.z, k) for k in range(4)]
        self.z_peers = [{'model': me + (at - self.z) * 4} for at in self.z_at]
        self.blocks = {
            (i, j, k): (1 - self.core if i else self.core) * 8 + (1 - self.y if j else self.y) * 4 + self.z_at[k]
            for i in (0, 1) for j in (0, 1) for k in range(4)
        }
        self.own = self.blocks[0, 0, 0]

    def block(self, i, j, k):
        return self.blocks[i, j, k]


class ReduceScatter(Exchange):
    def __init__(self, place, part, bufs, sems):
        super().__init__(place, sems)
        self.part = self.whole = part
        self.buf_core, self.out_y, self.buf_y, self.out_z, self.buf_z, self.out_first, self.buf_first = bufs
        self.core_in, self.y_in, self.z_in, self.first_in = {}, {}, {}, {}
        self.ready, self.first_ready = set(), False

    def block(self, k, j):
        return self.place.block(0, j, k)

    def start(self, h):
        p = self.place
        for k, j in CORE_ORDER:
            b = p.block(1, j, k)
            self.core_in[k, j, h] = self.remote(self.part.at[b, :, self.piece(h)], self.buf_core.at[k, j, :, self.piece(h)], (k * 2 + j) * 2 + h, p.partner)

    def core_ready(self, k, j, h):
        if (k, j, h) not in self.ready:
            self.core_in[k, j, h].wait_recv()
            self.ready.add((k, j, h))

    def pair_sum(self, k, j, c):
        return self.part[self.block(k, j), :, c].astype(F32) + self.buf_core[k, j, :, c].astype(F32)

    def chip_sum(self, k, c):
        return self.pair_sum(k, 0, c) + self.buf_y[k, :, c].astype(F32)

    def send_y(self, k, h):
        self.core_ready(k, 1, h)
        with_first = k == 0 and h in self.high
        if with_first and not self.first_ready:
            self.first_in[1].wait_recv()
            self.first_ready = True
        for c in self.spans(h):
            t = self.pair_sum(k, 1, c)
            if with_first:
                t = t + self.buf_first[1, :, pl.ds(c.start - HALF, CHUNK)].astype(F32)
            self.out_y[k, :, c] = t.astype(BF16)
        self.y_in[k, h] = self.remote(self.out_y.at[k, :, self.piece(h)], self.buf_y.at[k, :, self.piece(h)], BLOCKS + k * self.pieces + h, self.place.y_peer)

    def send_first(self):
        for j in (1, 0):
            self.core_ready(1, j, 1)
            for j2 in range(CHUNKS // 2):
                self.out_first[j, :, span(j2)] = self.pair_sum(1, j, span(CHUNKS // 2 + j2)).astype(BF16)
            self.first_in[j] = self.remote(self.out_first.at[j], self.buf_first.at[j], BLOCKS + 7 * self.pieces + j, self.place.z_peers[1])

    def send_z(self, k, h):
        self.core_ready(k, 0, h)
        self.y_in[k, h].wait_recv()
        if k == 2:
            self.z_in[3, h].wait_recv()
        for c in self.spans(h):
            t = self.chip_sum(k, c)
            if k == 2:
                t = t + self.buf_z[2, :, c].astype(F32)
            self.out_z[k - 1, :, c] = t.astype(BF16)
        i = BLOCKS + (3 + k) * self.pieces + h
        self.z_in[k, h] = self.remote(self.out_z.at[k - 1, :, self.piece(h)], self.buf_z.at[k - 1, :, self.piece(h)], i, self.place.z_peers[2 if k == 2 else 1])

    def head(self):
        y = {(k, h): (lambda k=k, h=h: self.send_y(k, h)) for k in range(4) for h in self.all}
        return [y[3, 0], y[3, 1], self.send_first, y[2, 0], y[2, 1], y[1, 0], y[0, 0]]

    def tail(self):
        z = {(k, h): (lambda k=k, h=h: self.send_z(k, h)) for k in range(4) for h in self.all}
        return [z[3, 0], z[3, 1], lambda: self.send_y(0, 1), z[2, 0], z[2, 1], z[1, 0]]

    def finish(self):
        for h in self.all:
            self.core_ready(0, 0, h)
            self.y_in[0, h].wait_recv()
        self.first_in[0].wait_recv()
        for h in self.low:
            self.z_in[1, h].wait_recv()
        for h in self.all:
            self.z_in[2, h].wait_recv()

    def total(self, j):
        c = span(j)
        near = self.buf_z[0, :, c] if j < CHUNKS // 2 else self.buf_first[0, :, span(j - CHUNKS // 2)]
        return self.chip_sum(0, c) + near.astype(F32) + self.buf_z[1, :, c].astype(F32)


class Gather(Exchange):
    def __init__(self, place, full, sems):
        super().__init__(place, sems)
        self.full = self.whole = full
        self.z_in, self.y_in, self.core_in, self.last_in = {}, {}, {}, {}

    def send(self, j, k, h, i, dev):
        b = self.place.block(0, j, k)
        ref = self.full.at[b] if h is None else self.full.at[b, :, self.piece(h)]
        return self.remote(ref, ref, i, dev)

    def to_core(self, j, k, h):
        self.core_in[j, k, h] = self.send(j, k, h, (8 + j * 4 + k) * self.pieces + h, self.place.partner)

    def to_y(self, k, h):
        self.y_in[k, h] = self.send(0, k, h, (4 + k) * self.pieces + h, self.place.y_peer)

    def to_z(self, k, h):
        self.z_in[k, h] = self.send(0, 2 if k == 3 else 0, h, k * self.pieces + h, self.place.z_peers[2 if k == 2 else 1])

    def start_far(self):
        for h in self.all:
            self.to_z(2, h)

    def start_near(self):
        for h in self.all:
            self.to_y(0, h)
            self.to_z(1, h)
        self.core_in[0, 0, None] = self.send(0, 0, None, 8 * self.pieces, self.place.partner)

    def from_z(self, k, h):
        self.z_in[k, h].wait_recv()
        if k == 2:
            self.to_z(3, h)
        if k != 1 or h in self.low:
            self.to_y(k, h)
        self.to_core(0, k, h)

    def from_y(self, k, h):
        self.y_in[k, h].wait_recv()
        self.to_core(1, k, h)

    def send_last(self):
        for h in self.high:
            self.last_in[h] = self.send(1, 0, h, h - self.pieces // 2, self.place.z_peers[1])

    def from_last(self):
        for h in self.high:
            self.last_in[h].wait_recv()
            self.to_core(1, 1, h)

    def steps(self):
        y = {(k, h): (lambda k=k, h=h: self.from_y(k, h)) for k in range(4) for h in self.all}
        z = {(k, h): (lambda k=k, h=h: self.from_z(k, h)) for k in range(4) for h in self.all}
        return [
            y[0, 0], z[2, 0], y[0, 1], z[2, 1], self.send_last, z[1, 0], z[1, 1], y[2, 0], y[2, 1], z[3, 0],
            y[1, 0], z[3, 1], self.from_last, y[3, 0], y[3, 1],
        ]

    def late_steps(self):
        near = [(lambda h=h: self.from_y(0, h)) for h in self.all] + [(lambda h=h: self.from_z(1, h)) for h in self.all]
        far = [(lambda h=h: self.from_z(2, h)) for h in self.all]
        end = [(lambda h=h: self.from_y(1, h)) for h in self.low] + [(lambda h=h: self.from_z(3, h)) for h in self.all]
        end += [(lambda h=h: self.from_y(2, h)) for h in self.all] + [self.from_last] + [(lambda h=h: self.from_y(3, h)) for h in self.all]
        return near, far, end

    def finish(self, h=None):
        for (_, _, at), cp in self.core_in.items():
            if h is None or (at or 0) == h:
                cp.wait_recv()


def run(steps):
    for step in steps:
        step()


def layer_kernel(
    x_hbm, dy_hbm, g1, g2, seg, wqkv_hbm, wo_hbm, w1_hbm, w2_hbm,
    fy, fx, dg1_out, dg2_out, a, dqkv, o, f2, f1, d_up, gelu, dy,
    x, wqkv, wo, w1, w2, part1, part3, part_y,
    core_buf, yout_buf, y_buf, zout_buf, z_buf, fout_buf, first_buf,
    qkv, prob, up, wide_up, d_gelu, d_attn, x1, d_res, wide, dg_part, dg_core, dg_y, dg_z, dg_full,
    rs_sems, ag_sems, dg_sems, in_sems,
):
    place = Place()
    own = place.own

    loads = [
        pltpu.make_async_copy(src, dst, in_sems.at[i])
        for i, (src, dst) in enumerate(
            [(x_hbm.at[pl.ds(r * 4, 4)], x.at[pl.ds(r * 4, 4)]) for r in range(4)]
            + [(wqkv_hbm.at[pl.ds(r * 1024, 1024)], wqkv.at[pl.ds(r * 1024, 1024)]) for r in range(4)]
            + [(wo_hbm, wo), (dy_hbm, dy), (w2_hbm, w2), (w1_hbm, w1)])
    ]
    load_x, load_wqkv, (load_wo, load_dy, load_w2, load_w1) = loads[:4], loads[4:8], loads[8:]
    for cp in load_x + load_wqkv:
        cp.start()
    barrier = pltpu.get_barrier_semaphore()
    for dev in [place.partner, place.y_peer] + place.z_peers[1:]:
        pl.semaphore_signal(barrier, inc=1, device_id=dev, device_id_type=MESH)

    def rs_set(i, part):
        bufs = [ref.at[i] for ref in (core_buf, yout_buf, y_buf, zout_buf, z_buf, fout_buf, first_buf)]
        return ReduceScatter(place, part, bufs, rs_sems.at[i])

    rs1, rs3, rsy, rs4 = rs_set(0, part1), rs_set(0, part3), rs_set(1, part_y), rs_set(0, part1)
    ag1, ag3, agy, ag4 = [Gather(place, ref, ag_sems.at[i]) for i, ref in ((0, f1), (0, f2), (1, fy), (0, fx))]

    def gain(ref, j):
        return ref[span(j)].astype(F32).reshape(1, CHUNK)

    def ln_one(i, carry):
        rows = pl.ds(i * 2, 2)
        mean, rstd = row_stats(lambda j: x[rows, :, span(j)].astype(F32))
        for j in range(CHUNKS):
            c = span(j)
            normed = (x[rows, :, c].astype(F32) - mean) * rstd * gain(g1, j)[None]
            a[rows, :, c] = normed.astype(BF16)
        return carry
    for r in range(4):
        load_x[r].wait()
        lax.fori_loop(r * 2, r * 2 + 2, ln_one, 0)
    for cp in (load_wo, load_dy, load_w2, load_w1):
        cp.start()

    for cp in load_wqkv:
        cp.wait()
    qkv[...] = dot_nn(a[...].reshape(TOKENS, WIDTH), wqkv[...]).astype(BF16)

    q_pos = lax.broadcasted_iota(jnp.int32, (TOKENS, TOKENS), 0)
    k_pos = lax.broadcasted_iota(jnp.int32, (TOKENS, TOKENS), 1)
    seg_keys = jnp.broadcast_to(seg[...].astype(F32), (TOKENS, TOKENS))
    allowed = (q_pos >= k_pos) & (seg_keys.T == seg_keys)
    for h in range(2):
        q, k, v = [qkv[:, pl.ds(h * 384 + i * LANES, LANES)] for i in range(3)]
        scores = jnp.where(allowed, dot_nt(q, k) * SCALE, -1e30)
        exp_scores = jnp.exp(scores - jnp.max(scores, axis=-1, keepdims=True))
        p = exp_scores / jnp.sum(exp_scores, axis=-1, keepdims=True)
        prob[h] = p
        o[:, pl.ds(h * LANES, LANES)] = dot_nn(p.astype(BF16), v).astype(BF16)

    def project(lhs, weight, part, tile, transposed, lo=0, hi=WIDTH):
        def step(i, carry):
            c = pl.ds(pl.multiple_of(lo + i * tile, tile), tile)
            r = dot_nt(lhs[...], weight[c, :]) if transposed else dot_nn(lhs[...], weight[:, c])
            part[:, :, c] = r.astype(BF16).reshape(BLOCKS, BLOCKS, tile)
            return carry
        lax.fori_loop(0, (hi - lo) // tile, step, 0)

    load_wo.wait()
    pl.semaphore_wait(barrier, 5)
    project(o, wo, part1, HALF, False, 0, HALF)
    rs1.start(0)
    project(o, wo, part1, HALF, False, HALF)

    rs1.start(1)
    run(rs1.head())

    def d_gelu_tile(lo, n):
        c = pl.ds(lo, n)
        d_gelu[:, c] = dot_nt(dy[...].reshape(TOKENS, WIDTH), w2[c, :]).astype(BF16)
    load_dy.wait()
    load_w2.wait()
    tail = rs1.tail()
    d_gelu_tile(0, TOKENS)
    d_gelu_tile(TOKENS, TOKENS)
    run(tail[:3])
    d_gelu_tile(512, TOKENS)
    run(tail[3:])
    d_gelu_tile(QKV_COLS, LANES)
    rs1.finish()

    for j in range(CHUNKS):
        c = span(j)
        x1[:, c] = (x[own, :, c].astype(F32) + rs1.total(j)).astype(BF16)
    mean2, rstd2 = row_stats(lambda j: x1[:, span(j)].astype(F32))
    for j in range(CHUNKS):
        c = span(j)
        f1[own, :, c] = ((x1[:, c].astype(F32) - mean2) * rstd2 * gain(g2, j)).astype(BF16)
    ag1.start_far()
    ag1.start_near()
    run(ag1.steps())
    load_w1.wait()
    left, right = pl.ds(0, HALF), pl.ds(HALF, HALF)
    ag1.finish(0)
    wide_up[...] = dot_nn(f1[:, :, left].reshape(TOKENS, HALF), w1[left, :])
    ag1.finish(1)
    rs1.drain()
    up[...] = (wide_up[...] + dot_nn(f1[:, :, right].reshape(TOKENS, HALF), w1[right, :])).astype(BF16)

    def activation(i, carry):
        rows = pl.ds(pl.multiple_of(i * BLOCKS, BLOCKS), BLOCKS)
        u = up[rows, :].astype(F32)
        t = jnp.tanh(GELU_A * (u + GELU_B * (u * u * u)))
        gelu[rows, :] = (0.5 * u * (1.0 + t)).astype(BF16)
        slope = 0.5 * (1.0 + t) + 0.5 * u * (1.0 - t * t) * (GELU_A * (1.0 + 3.0 * GELU_B * (u * u)))
        d_up[rows, :] = (d_gelu[rows, :].astype(F32) * slope).astype(BF16)
        return carry
    lax.fori_loop(0, BLOCKS, activation, 0)
    project(d_up, w1, part3, HALF, True, 0, HALF)
    rs3.start(0)
    project(d_up, w1, part3, HALF, True, HALF)

    rs3.start(1)
    run(rs3.head())
    tail, y_head, y_tail = rs3.tail(), rsy.head(), rsy.tail()
    project(gelu, w2, part_y, HALF, False, 0, HALF)
    rsy.start(0)
    project(gelu, w2, part_y, HALF, False, HALF)
    rsy.start(1)
    run(tail[:5])
    run(y_head[:2])
    run(tail[5:])
    run(y_head[2:4])
    rs3.finish()

    def ln_backward(rs, z, mean, rstd, gain_ref, dg_row):
        sum_a = jnp.zeros((BLOCKS, LANES), F32)
        sum_b = jnp.zeros((BLOCKS, LANES), F32)
        for j in range(CHUNKS):
            d_norm = rs.total(j).astype(BF16).astype(F32)
            x_hat = (z(j) - mean) * rstd
            grad_row = jnp.sum(d_norm * x_hat, axis=0, keepdims=True)
            for i in range(CHUNK // LANES):
                at = j * (CHUNK // LANES) + i
                dg_part[at // 2, pl.ds(dg_row + at % 2, 1), :] = grad_row[:, i * LANES:(i + 1) * LANES]
            scaled = d_norm * gain(gain_ref, j)
            wide[:, span(j)] = scaled
            sum_a = sum_a + fold(scaled)
            sum_b = sum_b + fold(scaled * x_hat)
        mean_a = jnp.sum(sum_a, axis=-1, keepdims=True) / WIDTH
        mean_b = jnp.sum(sum_b, axis=-1, keepdims=True) / WIDTH
        for j in range(CHUNKS):
            c = span(j)
            x_hat = (z(j) - mean) * rstd
            wide[:, c] = rstd * (wide[:, c] - mean_a - x_hat * mean_b)

    ln_backward(rs3, lambda j: x1[:, span(j)].astype(F32), mean2, rstd2, g2, 2)
    for j in range(CHUNKS):
        c = span(j)
        value = (dy[own, :, c].astype(F32) + wide[:, c].astype(BF16).astype(F32)).astype(BF16)
        d_res[:, c] = value
        f2[own, :, c] = value
    ag1.drain()
    ag3.start_far()
    ag3.start_near()
    steps = ag3.steps()
    last = steps.index(ag3.from_last)
    run(steps[:last])
    run(y_head[4:])
    run(y_tail[:2])
    run(steps[last:])
    ag3.finish(0)
    wide_attn = dot_nt(f2[:, :, left].reshape(TOKENS, HALF), wo[:, left])
    ag3.finish(1)
    d_attn[...] = (wide_attn + dot_nt(f2[:, :, right].reshape(TOKENS, HALF), wo[:, right])).astype(BF16)
    run(y_tail[2:5])
    for h in range(2):
        q, k, v = [qkv[:, pl.ds(h * 384 + i * LANES, LANES)] for i in range(3)]
        d_o = d_attn[:, pl.ds(h * LANES, LANES)]
        p = prob[h]
        d_prob = dot_nt(d_o, v)
        d_score = p * (d_prob - jnp.sum(p * d_prob, axis=-1, keepdims=True)) * SCALE
        dqkv[:, pl.ds(h * 384, LANES)] = dot_nn(d_score.astype(BF16), k).astype(BF16)
        dqkv[:, pl.ds(h * 384 + LANES, LANES)] = dot_nn(d_score.T.astype(BF16), q).astype(BF16)
        dqkv[:, pl.ds(h * 384 + TOKENS, LANES)] = dot_nn(p.T.astype(BF16), d_o).astype(BF16)
    run(y_tail[5:])
    rs3.drain()
    project(dqkv, wqkv, part1, HALF, True, 0, HALF)
    rs4.start(0)
    project(dqkv, wqkv, part1, HALF, True, HALF)

    rs4.start(1)
    run(rs4.head())
    tail = rs4.tail()
    run(tail[:3])
    rsy.finish()
    for j in range(CHUNKS):
        c = span(j)
        fy[own, :, c] = (x1[:, c].astype(F32) + rsy.total(j)).astype(BF16)
    run(tail[3:])
    agy.start_near()
    rs4.finish()
    mean1, rstd1 = row_stats(lambda j: x[own, :, span(j)].astype(F32))
    ln_backward(rs4, lambda j: x[own, :, span(j)].astype(F32), mean1, rstd1, g1, 0)
    for j in range(CHUNKS):
        c = span(j)
        fx[own, :, c] = (d_res[:, c].astype(F32) + wide[:, c].astype(BF16).astype(F32)).astype(BF16)
    dg_copies = []

    def dg_send(src, dst, i, dev):
        cp = pltpu.make_async_remote_copy(src_ref=src, dst_ref=dst, send_sem=dg_sems.at[0, i], recv_sem=dg_sems.at[1, i], device_id=dev, device_id_type=MESH)
        cp.start()
        dg_copies.append(cp)
        return cp
    in_core = dg_send(dg_part.at[pl.ds((1 - place.core) * 8, 8)], dg_core, 0, place.partner)
    ag3.drain()
    ag4.start_far()
    agy.start_far()
    ag4.start_near()
    steps = ag4.steps()
    near, far, end = agy.late_steps()
    last, mid = steps.index(ag4.from_last), steps.index(ag4.send_last)
    in_core.wait_recv()
    dg_core[...] = dg_core[...] + dg_part[pl.ds(place.core * 8, 8)]
    in_y = dg_send(dg_core.at[pl.ds((1 - place.y) * 4, 4)], dg_y, 6, place.y_peer)
    run(near)
    run(steps[:mid + 1])
    in_y.wait_recv()
    quarter = pl.ds(place.core * 8 + place.y * 4, 4)
    dg_z[place.z] = dg_core[pl.ds(place.y * 4, 4)] + dg_y[...]
    in_z = [dg_send(dg_z.at[place.z], dg_z.at[place.z], k, place.z_peers[k]) for k in (1, 2, 3)]
    run(steps[mid + 1:mid + 3])
    run(far)
    agy.send_last()
    run(steps[mid + 3:last - 2])
    run(end[:2 // 2])
    for cp in in_z:
        cp.wait_recv()
    dg_full[quarter] = dg_z[0] + dg_z[1] + dg_z[2] + dg_z[3]
    in_y = dg_send(dg_full.at[quarter], dg_full.at[quarter], 4, place.y_peer)
    run(steps[last - 2:last + 1])
    run(end[2 // 2:2 * 2])
    in_y.wait_recv()
    mine = pl.ds(place.core * 8, 8)
    in_core = dg_send(dg_full.at[mine], dg_full.at[mine], 5, place.partner)
    run(steps[last + 1:])
    in_core.wait_recv()
    for i in range(32):
        for row, out in ((0, dg1_out), (2, dg2_out)):
            out[pl.ds(i * LANES, LANES)] = dg_full[i // 2, row + i % 2].astype(BF16)
    ag4.finish()
    run(end[2 * 2:])
    agy.finish()

    for exchange in (rs4, ag4, rsy, agy):
        exchange.drain()
    for cp in dg_copies:
        cp.wait_send()


def layer(x_in, d_y, gain_one, gain_two, seg_ids, w_qkv, w_out, w_up, w_down):
    hbm = pl.BlockSpec(memory_space=pl.ANY)
    vmem = pl.BlockSpec(memory_space=pltpu.VMEM)
    dma = pltpu.SemaphoreType.DMA

    def shape(*dims):
        return pltpu.VMEM(dims, BF16)

    def scratch(*dims, dtype=BF16):
        return pltpu.VMEM(dims, dtype)
    blocks = (BLOCKS, BLOCKS, WIDTH)
    return pl.pallas_call(
        layer_kernel,
        out_shape=[
            shape(*blocks), shape(*blocks), shape(WIDTH), shape(WIDTH), shape(*blocks), shape(TOKENS, QKV_COLS), shape(TOKENS, TOKENS), shape(*blocks),
            shape(*blocks), shape(TOKENS, FFN), shape(TOKENS, FFN), shape(*blocks),
        ],
        in_specs=[hbm, hbm, vmem, vmem, vmem, hbm, hbm, hbm, hbm],
        out_specs=[vmem] * 12,
        scratch_shapes=[
            scratch(*blocks), scratch(WIDTH, QKV_COLS), scratch(TOKENS, WIDTH), scratch(WIDTH, FFN), scratch(FFN, WIDTH),
        ] + [scratch(*blocks)] * 3 + [
            scratch(2, 4, 2, BLOCKS, WIDTH), scratch(2, 4, BLOCKS, WIDTH), scratch(2, 4, BLOCKS, WIDTH), scratch(2, 3, BLOCKS, WIDTH), scratch(2, 3, BLOCKS, WIDTH),
            scratch(2, 2, BLOCKS, HALF), scratch(2, 2, BLOCKS, HALF),
            scratch(TOKENS, QKV_COLS), scratch(2, TOKENS, TOKENS, dtype=F32), scratch(TOKENS, FFN), scratch(TOKENS, FFN, dtype=F32), scratch(TOKENS, FFN),
            scratch(TOKENS, TOKENS), scratch(BLOCKS, WIDTH), scratch(BLOCKS, WIDTH), scratch(BLOCKS, WIDTH, dtype=F32),
            scratch(BLOCKS, 4, LANES, dtype=F32), scratch(8, 4, LANES, dtype=F32), scratch(4, 4, LANES, dtype=F32), scratch(4, 4, 4, LANES, dtype=F32),
            scratch(BLOCKS, 4, LANES, dtype=F32),
            dma((2, BLOCKS + 3 + 7 * ReduceScatter.pieces)), dma((2, 1 + BLOCKS * Gather.pieces)), dma((2, 7)), dma((12,)),
        ],
        compiler_params=pltpu.CompilerParams(collective_id=0, has_side_effects=True, vmem_limit_bytes=LAYER_VMEM),
        name='layer',
    )(
        x_in.reshape(blocks), d_y.reshape(blocks), gain_one, gain_two, seg_ids, w_qkv, w_out.reshape(TOKENS, WIDTH), w_up, w_down,
    )


TILE = 1024


def weight_grad_kernel(
    a, dqkv, o, dr, b1, du, gelu, dy, y, dx, dg1, dg2,
    dwqkv_hbm, dwo_hbm, dw1_hbm, dw2_hbm, y_out, dx_out, dg1_out, dg2_out,
    dwqkv, dwo, dw1, dw2, gelu_t, o_t, out_sems,
):
    stores = []

    def store(src, dst):
        cp = pltpu.make_async_copy(src, dst, out_sems.at[len(stores)])
        cp.start()
        stores.append(cp)

    def by_rows(lhs, rhs, out, out_hbm):
        for i in range(WIDTH // TILE):
            c = pl.ds(i * TILE, TILE)
            out[c, :] = lax.dot_general(lhs[:, c], rhs[...], (((0,), (0,)), ((), ())), preferred_element_type=F32).astype(BF16)
            store(out.at[c], out_hbm.at[c])

    def by_columns(lhs_t, rhs, out, out_hbm):
        for i in range(WIDTH // TILE):
            c = pl.ds(i * TILE, TILE)
            out[:, c] = dot_nn(lhs_t[...], rhs[:, c]).astype(BF16)
            store(out.at[:, c], out_hbm.at[:, c])

    store(y, y_out)
    store(dx, dx_out)
    store(dg1, dg1_out)
    store(dg2, dg2_out)
    by_rows(a, dqkv, dwqkv, dwqkv_hbm)
    by_rows(b1, du, dw1, dw1_hbm)
    gelu_t[...] = gelu[...].T
    by_columns(gelu_t, dy, dw2, dw2_hbm)
    o_t[...] = o[...].T
    by_columns(o_t, dr, dwo, dwo_hbm)
    for cp in stores:
        cp.wait()


def weight_grads(*operands):
    hbm = pl.BlockSpec(memory_space=pl.ANY)
    vmem = pl.BlockSpec(memory_space=pltpu.VMEM)
    big = (TOKENS, WIDTH)
    ins = [big, (TOKENS, QKV_COLS), (TOKENS, TOKENS), big, big, (TOKENS, FFN), (TOKENS, FFN), big, big, big, (WIDTH,), (WIDTH,)]
    outs = [(WIDTH, QKV_COLS), big, (WIDTH, FFN), (FFN, WIDTH), big, big, (WIDTH,), (WIDTH,)]
    return pl.pallas_call(
        weight_grad_kernel,
        out_shape=[jax.ShapeDtypeStruct(dims, BF16) for dims in outs],
        in_specs=[vmem] * len(ins),
        out_specs=[hbm] * len(outs),
        scratch_shapes=[pltpu.VMEM(dims, BF16) for dims in outs[:4] + [(FFN, TOKENS), (TOKENS, TOKENS)]] + [pltpu.SemaphoreType.DMA((20,))],
        compiler_params=pltpu.CompilerParams(vmem_limit_bytes=GRADS_VMEM),
        name='weight_grads',
    )(*[v.reshape(dims) for v, dims in zip(operands, ins)])


def solution(mesh):
    def local_step(x_in, seg_ids, gain_one, w_qkv, w_out, gain_two, w_up, w_down, d_y):
        y, d_x, gains_one, gains_two, normed_one, d_qkv, attn_out, d_resid, normed_two, d_up, gelu_out, d_y_here = layer(
            x_in, d_y, gain_one, gain_two, seg_ids, w_qkv, w_out, w_up, w_down)
        d_w_qkv, d_w_out, d_w_up, d_w_down, y_out, d_x_out, d_gain_one, d_gain_two = weight_grads(
            normed_one, d_qkv, attn_out, d_resid, normed_two, d_up, gelu_out, d_y_here, y, d_x, gains_one, gains_two)
        return y_out.reshape(x_in.shape), d_x_out.reshape(x_in.shape), d_w_qkv, d_w_out.reshape(w_out.shape), d_w_up, d_w_down, d_gain_one, d_gain_two

    in_specs = (P('data'), P('data'), P(), P(None, 'model'), P('model'), P(), P(None, 'model'), P('model'), P('data'))
    out_specs = (P('data'), P('data'), P('data', 'model'), P(('data', 'model')), P('data', 'model'), P(('data', 'model')), P('data'), P('data'))
    return jax.shard_map(local_step, mesh=mesh, in_specs=in_specs, out_specs=out_specs, check_vma=False)
```

```python
import jax
import jax.numpy as jnp
from jax import lax
from jax.experimental import pallas as pl
from jax.experimental.pallas import tpu as pltpu
from jax.sharding import PartitionSpec as P

LN_EPS = 1e-5
MESH = pl.DeviceIdType.MESH
BF16 = jnp.bfloat16
F32 = jnp.float32
WIDTH = 4096
CHUNK = 512
LAYER_VMEM = 49 * 2 ** 20
GRADS_VMEM = 28 * 2 ** 20
TOKENS = 256
LANES = 128
BLOCKS = 16
FFN = 896
QKV_COLS = 768
CHUNKS = WIDTH // CHUNK
HALF = WIDTH // 2
CORE_ORDER = [(3, 1), (1, 1), (1, 0), (2, 1), (3, 0), (0, 1), (2, 0), (0, 0)]
SCALE = LANES ** -0.5
GELU_A = 0.7978845608028654
GELU_B = 0.044715


def flip(z, k):
    high, low = lax.div(z, 2), lax.rem(z, 2)
    return (1 - high if k >= 2 else high) * 2 + (1 - low if k % 2 else low)


def dot_nn(a, b):
    return jnp.dot(a, b, preferred_element_type=F32)


def dot_nt(a, b):
    return lax.dot_general(a, b, (((1,), (1,)), ((), ())), preferred_element_type=F32)


def span(j):
    return pl.ds(j * CHUNK, CHUNK)


class Exchange:
    pieces = 2

    def __init__(self, place, sems):
        self.place, self.sems = place, sems
        self.all = range(self.pieces)
        self.low, self.high = self.all[:self.pieces // 2], self.all[self.pieces // 2:]
        self.width = WIDTH // self.pieces

    def piece(self, h):
        return pl.ds(h * self.width, self.width)

    def spans(self, h):
        n = CHUNKS // self.pieces
        return [span(h * n + j) for j in range(n)]

    def remote(self, src, dst, i, dev):
        cp = pltpu.make_async_remote_copy(src_ref=src, dst_ref=dst, send_sem=self.sems.at[0], recv_sem=self.sems.at[1 + i], device_id=dev, device_id_type=MESH)
        cp.start()
        return cp

    def drain(self):
        sent = self.whole.at[pl.ds(0, BLOCKS - 1)]
        pltpu.make_async_copy(sent, sent, self.sems.at[0]).wait()


def fold(v):
    return sum(v[..., i * LANES:(i + 1) * LANES] for i in range(CHUNK // LANES))


def row_stats(wide):
    total = sum(fold(wide(j)) for j in range(CHUNKS))
    mean = jnp.sum(total, axis=-1, keepdims=True) / WIDTH

    def square(j):
        centered = wide(j) - mean
        return fold(centered * centered)
    total = sum(square(j) for j in range(CHUNKS))
    var = jnp.sum(total, axis=-1, keepdims=True) / WIDTH
    return mean, lax.rsqrt(var + LN_EPS)


class Place:
    def __init__(self):
        me = lax.axis_index('model')
        self.core, self.y, self.z = lax.rem(me, 2), lax.rem(lax.div(me, 2), 2), lax.div(me, 4)
        self.partner = {'model': me + 1 - 2 * self.core}
        self.y_peer = {'model': me + 2 - 4 * self.y}
        self.z_at = [flip(self.z, k) for k in range(4)]
        self.z_peers = [{'model': me + (at - self.z) * 4} for at in self.z_at]
        self.blocks = {
            (i, j, k): (1 - self.core if i else self.core) * 8 + (1 - self.y if j else self.y) * 4 + self.z_at[k]
            for i in (0, 1) for j in (0, 1) for k in range(4)
        }
        self.own = self.blocks[0, 0, 0]

    def block(self, i, j, k):
        return self.blocks[i, j, k]


class ReduceScatter(Exchange):
    def __init__(self, place, part, bufs, sems):
        super().__init__(place, sems)
        self.part = self.whole = part
        self.buf_core, self.out_y, self.buf_y, self.out_z, self.buf_z, self.out_first, self.buf_first = bufs
        self.core_in, self.y_in, self.z_in, self.first_in = {}, {}, {}, {}
        self.ready, self.first_ready = set(), False

    def block(self, k, j):
        return self.place.block(0, j, k)

    def start(self, h):
        p = self.place
        for k, j in CORE_ORDER:
            b = p.block(1, j, k)
            self.core_in[k, j, h] = self.remote(self.part.at[b, :, self.piece(h)], self.buf_core.at[k, j, :, self.piece(h)], (k * 2 + j) * 2 + h, p.partner)

    def core_ready(self, k, j, h):
        if (k, j, h) not in self.ready:
            self.core_in[k, j, h].wait_recv()
            self.ready.add((k, j, h))

    def pair_sum(self, k, j, c):
        return self.part[self.block(k, j), :, c].astype(F32) + self.buf_core[k, j, :, c].astype(F32)

    def chip_sum(self, k, c):
        return self.pair_sum(k, 0, c) + self.buf_y[k, :, c].astype(F32)

    def send_y(self, k, h):
        self.core_ready(k, 1, h)
        with_first = k == 0 and h in self.high
        if with_first and not self.first_ready:
            self.first_in[1].wait_recv()
            self.first_ready = True
        for c in self.spans(h):
            t = self.pair_sum(k, 1, c)
            if with_first:
                t = t + self.buf_first[1, :, pl.ds(c.start - HALF, CHUNK)].astype(F32)
            self.out_y[k, :, c] = t.astype(BF16)
        self.y_in[k, h] = self.remote(self.out_y.at[k, :, self.piece(h)], self.buf_y.at[k, :, self.piece(h)], BLOCKS + k * self.pieces + h, self.place.y_peer)

    def send_first(self):
        for j in (1, 0):
            self.core_ready(1, j, 1)
            for j2 in range(CHUNKS // 2):
                self.out_first[j, :, span(j2)] = self.pair_sum(1, j, span(CHUNKS // 2 + j2)).astype(BF16)
            self.first_in[j] = self.remote(self.out_first.at[j], self.buf_first.at[j], BLOCKS + 7 * self.pieces + j, self.place.z_peers[1])

    def send_z(self, k, h):
        self.core_ready(k, 0, h)
        self.y_in[k, h].wait_recv()
        if k == 2:
            self.z_in[3, h].wait_recv()
        for c in self.spans(h):
            t = self.chip_sum(k, c)
            if k == 2:
                t = t + self.buf_z[2, :, c].astype(F32)
            self.out_z[k - 1, :, c] = t.astype(BF16)
        i = BLOCKS + (3 + k) * self.pieces + h
        self.z_in[k, h] = self.remote(self.out_z.at[k - 1, :, self.piece(h)], self.buf_z.at[k - 1, :, self.piece(h)], i, self.place.z_peers[2 if k == 2 else 1])

    def head(self):
        y = {(k, h): (lambda k=k, h=h: self.send_y(k, h)) for k in range(4) for h in self.all}
        return [y[3, 0], y[3, 1], self.send_first, y[2, 0], y[2, 1], y[1, 0], y[0, 0]]

    def tail(self):
        z = {(k, h): (lambda k=k, h=h: self.send_z(k, h)) for k in range(4) for h in self.all}
        return [z[3, 0], z[3, 1], lambda: self.send_y(0, 1), z[2, 0], z[2, 1], z[1, 0]]

    def finish(self):
        for h in self.all:
            self.core_ready(0, 0, h)
            self.y_in[0, h].wait_recv()
        self.first_in[0].wait_recv()
        for h in self.low:
            self.z_in[1, h].wait_recv()
        for h in self.all:
            self.z_in[2, h].wait_recv()

    def total(self, j):
        c = span(j)
        near = self.buf_z[0, :, c] if j < CHUNKS // 2 else self.buf_first[0, :, span(j - CHUNKS // 2)]
        return self.chip_sum(0, c) + near.astype(F32) + self.buf_z[1, :, c].astype(F32)


class Gather(Exchange):
    def __init__(self, place, full, sems):
        super().__init__(place, sems)
        self.full = self.whole = full
        self.z_in, self.y_in, self.core_in, self.last_in = {}, {}, {}, {}

    def send(self, j, k, h, i, dev):
        b = self.place.block(0, j, k)
        ref = self.full.at[b] if h is None else self.full.at[b, :, self.piece(h)]
        return self.remote(ref, ref, i, dev)

    def to_core(self, j, k, h):
        self.core_in[j, k, h] = self.send(j, k, h, (8 + j * 4 + k) * self.pieces + h, self.place.partner)

    def to_y(self, k, h):
        self.y_in[k, h] = self.send(0, k, h, (4 + k) * self.pieces + h, self.place.y_peer)

    def to_z(self, k, h):
        self.z_in[k, h] = self.send(0, 2 if k == 3 else 0, h, k * self.pieces + h, self.place.z_peers[2 if k == 2 else 1])

    def start_far(self):
        for h in self.all:
            self.to_z(2, h)

    def start_near(self):
        for h in self.all:
            self.to_y(0, h)
            self.to_z(1, h)
        self.core_in[0, 0, None] = self.send(0, 0, None, 8 * self.pieces, self.place.partner)

    def from_z(self, k, h):
        self.z_in[k, h].wait_recv()
        if k == 2:
            self.to_z(3, h)
        if k != 1 or h in self.low:
            self.to_y(k, h)
        self.to_core(0, k, h)

    def from_y(self, k, h):
        self.y_in[k, h].wait_recv()
        self.to_core(1, k, h)

    def send_last(self):
        for h in self.high:
            self.last_in[h] = self.send(1, 0, h, h - self.pieces // 2, self.place.z_peers[1])

    def from_last(self):
        for h in self.high:
            self.last_in[h].wait_recv()
            self.to_core(1, 1, h)

    def steps(self):
        y = {(k, h): (lambda k=k, h=h: self.from_y(k, h)) for k in range(4) for h in self.all}
        z = {(k, h): (lambda k=k, h=h: self.from_z(k, h)) for k in range(4) for h in self.all}
        return [
            y[0, 0], z[2, 0], y[0, 1], z[2, 1], self.send_last, z[1, 0], z[1, 1], y[2, 0], y[2, 1], z[3, 0],
            y[1, 0], z[3, 1], self.from_last, y[3, 0], y[3, 1],
        ]

    def late_steps(self):
        near = [(lambda h=h: self.from_y(0, h)) for h in self.all] + [(lambda h=h: self.from_z(1, h)) for h in self.all]
        far = [(lambda h=h: self.from_z(2, h)) for h in self.all]
        end = [(lambda h=h: self.from_y(1, h)) for h in self.low] + [(lambda h=h: self.from_z(3, h)) for h in self.all]
        end += [(lambda h=h: self.from_y(2, h)) for h in self.all] + [self.from_last] + [(lambda h=h: self.from_y(3, h)) for h in self.all]
        return near, far, end

    def finish(self, h=None):
        for (_, _, at), cp in self.core_in.items():
            if h is None or (at or 0) == h:
                cp.wait_recv()


def run(steps):
    for step in steps:
        step()


def layer_kernel(
    x_hbm, dy_hbm, g1, g2, seg, wqkv_hbm, wo_hbm, w1_hbm, w2_hbm,
    fy, fx, dg1_out, dg2_out, a, dqkv, o, f2, f1, d_up, gelu, dy,
    x, wqkv, wo, w1, w2, part1, part3, part_y,
    core_buf, yout_buf, y_buf, zout_buf, z_buf, fout_buf, first_buf,
    qkv, prob, up, wide_up, d_gelu, d_attn, x1, d_res, wide, dg_part, dg_core, dg_y, dg_z, dg_full,
    rs_sems, ag_sems, dg_sems, in_sems,
):
    place = Place()
    own = place.own

    loads = [
        pltpu.make_async_copy(src, dst, in_sems.at[i])
        for i, (src, dst) in enumerate(
            [(x_hbm.at[pl.ds(r * 4, 4)], x.at[pl.ds(r * 4, 4)]) for r in range(4)]
            + [(wqkv_hbm.at[pl.ds(r * 1024, 1024)], wqkv.at[pl.ds(r * 1024, 1024)]) for r in range(4)]
            + [(wo_hbm, wo), (dy_hbm, dy), (w2_hbm, w2), (w1_hbm, w1)])
    ]
    load_x, load_wqkv, (load_wo, load_dy, load_w2, load_w1) = loads[:4], loads[4:8], loads[8:]
    for cp in load_x + load_wqkv:
        cp.start()
    barrier = pltpu.get_barrier_semaphore()
    for dev in [place.partner, place.y_peer] + place.z_peers[1:]:
        pl.semaphore_signal(barrier, inc=1, device_id=dev, device_id_type=MESH)

    def rs_set(i, part):
        bufs = [ref.at[i] for ref in (core_buf, yout_buf, y_buf, zout_buf, z_buf, fout_buf, first_buf)]
        return ReduceScatter(place, part, bufs, rs_sems.at[i])

    rs1, rs3, rsy, rs4 = rs_set(0, part1), rs_set(0, part3), rs_set(1, part_y), rs_set(0, part1)
    ag1, ag3, agy, ag4 = [Gather(place, ref, ag_sems.at[i]) for i, ref in ((0, f1), (0, f2), (1, fy), (0, fx))]

    def gain(ref, j):
        return ref[span(j)].astype(F32).reshape(1, CHUNK)

    def ln_one(i):
        rows = pl.ds(i * 4, 4)
        mean, rstd = row_stats(lambda j: x[rows, :, span(j)].astype(F32))
        for j in range(CHUNKS):
            c = span(j)
            normed = (x[rows, :, c].astype(F32) - mean) * rstd * gain(g1, j)[None]
            a[rows, :, c] = normed.astype(BF16)
    for r in range(4):
        load_x[r].wait()
        ln_one(r)
    for cp in (load_wo, load_dy, load_w2, load_w1):
        cp.start()

    left, right = pl.ds(0, HALF), pl.ds(HALF, HALF)
    for cp in load_wqkv[:2]:
        cp.wait()
    wide_up[:, pl.ds(0, QKV_COLS)] = dot_nn(a[:, :, left].reshape(TOKENS, HALF), wqkv[left, :])
    for cp in load_wqkv[2:]:
        cp.wait()
    qkv[...] = (wide_up[:, pl.ds(0, QKV_COLS)] + dot_nn(a[:, :, right].reshape(TOKENS, HALF), wqkv[right, :])).astype(BF16)

    q_pos = lax.broadcasted_iota(jnp.int32, (TOKENS, TOKENS), 0)
    k_pos = lax.broadcasted_iota(jnp.int32, (TOKENS, TOKENS), 1)
    seg_keys = jnp.broadcast_to(seg[...].astype(F32), (TOKENS, TOKENS))
    allowed = (q_pos >= k_pos) & (seg_keys.T == seg_keys)
    for h in range(2):
        q, k, v = [qkv[:, pl.ds(h * 384 + i * LANES, LANES)] for i in range(3)]
        scores = jnp.where(allowed, dot_nt(q, k) * SCALE, -1e30)
        exp_scores = jnp.exp(scores - jnp.max(scores, axis=-1, keepdims=True))
        p = exp_scores / jnp.sum(exp_scores, axis=-1, keepdims=True)
        prob[h] = p
        o[:, pl.ds(h * LANES, LANES)] = dot_nn(p.astype(BF16), v).astype(BF16)

    def project(lhs, weight, part, tile, transposed, lo=0, hi=WIDTH):
        def step(i, carry):
            c = pl.ds(pl.multiple_of(lo + i * tile, tile), tile)
            r = dot_nt(lhs[...], weight[c, :]) if transposed else dot_nn(lhs[...], weight[:, c])
            part[:, :, c] = r.astype(BF16).reshape(BLOCKS, BLOCKS, tile)
            return carry
        lax.fori_loop(0, (hi - lo) // tile, step, 0)

    load_wo.wait()
    pl.semaphore_wait(barrier, 5)
    project(o, wo, part1, HALF, False, 0, HALF)
    rs1.start(0)
    project(o, wo, part1, HALF, False, HALF)

    rs1.start(1)
    run(rs1.head())

    def d_gelu_tile(lo, n):
        c = pl.ds(lo, n)
        d_gelu[:, c] = dot_nt(dy[...].reshape(TOKENS, WIDTH), w2[c, :]).astype(BF16)
    load_dy.wait()
    load_w2.wait()
    tail = rs1.tail()
    d_gelu_tile(0, TOKENS)
    d_gelu_tile(TOKENS, TOKENS)
    run(tail[:3])
    d_gelu_tile(512, TOKENS)
    run(tail[3:])
    d_gelu_tile(QKV_COLS, LANES)
    rs1.finish()

    for j in range(CHUNKS):
        c = span(j)
        x1[:, c] = (x[own, :, c].astype(F32) + rs1.total(j)).astype(BF16)
    mean2, rstd2 = row_stats(lambda j: x1[:, span(j)].astype(F32))
    for j in range(CHUNKS):
        c = span(j)
        f1[own, :, c] = ((x1[:, c].astype(F32) - mean2) * rstd2 * gain(g2, j)).astype(BF16)
    ag1.start_far()
    ag1.start_near()
    run(ag1.steps())
    load_w1.wait()
    ag1.finish(0)
    wide_up[...] = dot_nn(f1[:, :, left].reshape(TOKENS, HALF), w1[left, :])
    ag1.finish(1)
    rs1.drain()
    up[...] = (wide_up[...] + dot_nn(f1[:, :, right].reshape(TOKENS, HALF), w1[right, :])).astype(BF16)

    def activation(i, carry):
        rows = pl.ds(pl.multiple_of(i * 32, 32), 32)
        u = up[rows, :].astype(F32)
        t = jnp.tanh(GELU_A * (u + GELU_B * (u * u * u)))
        gelu[rows, :] = (0.5 * u * (1.0 + t)).astype(BF16)
        slope = 0.5 * (1.0 + t) + 0.5 * u * (1.0 - t * t) * (GELU_A * (1.0 + 3.0 * GELU_B * (u * u)))
        d_up[rows, :] = (d_gelu[rows, :].astype(F32) * slope).astype(BF16)
        return carry
    lax.fori_loop(0, 8, activation, 0)
    project(d_up, w1, part3, HALF, True, 0, HALF)
    rs3.start(0)
    project(d_up, w1, part3, HALF, True, HALF)

    rs3.start(1)
    run(rs3.head())
    tail, y_head, y_tail = rs3.tail(), rsy.head(), rsy.tail()
    project(gelu, w2, part_y, HALF, False, 0, HALF)
    rsy.start(0)
    project(gelu, w2, part_y, HALF, False, HALF)
    rsy.start(1)
    run(tail[:5])
    run(y_head[:2])
    run(tail[5:])
    run(y_head[2:5])
    rs3.finish()

    def ln_backward(rs, z, mean, rstd, gain_ref, dg_row):
        sum_a = jnp.zeros((BLOCKS, LANES), F32)
        sum_b = jnp.zeros((BLOCKS, LANES), F32)
        for j in range(CHUNKS):
            d_norm = rs.total(j).astype(BF16).astype(F32)
            x_hat = (z(j) - mean) * rstd
            grad_row = jnp.sum(d_norm * x_hat, axis=0, keepdims=True)
            for i in range(CHUNK // LANES):
                at = j * (CHUNK // LANES) + i
                dg_part[at // 2, pl.ds(dg_row + at % 2, 1), :] = grad_row[:, i * LANES:(i + 1) * LANES]
            scaled = d_norm * gain(gain_ref, j)
            wide[:, span(j)] = scaled
            sum_a = sum_a + fold(scaled)
            sum_b = sum_b + fold(scaled * x_hat)
        mean_a = jnp.sum(sum_a, axis=-1, keepdims=True) / WIDTH
        mean_b = jnp.sum(sum_b, axis=-1, keepdims=True) / WIDTH
        for j in range(CHUNKS):
            c = span(j)
            x_hat = (z(j) - mean) * rstd
            wide[:, c] = rstd * (wide[:, c] - mean_a - x_hat * mean_b)

    ln_backward(rs3, lambda j: x1[:, span(j)].astype(F32), mean2, rstd2, g2, 2)
    for j in range(CHUNKS):
        c = span(j)
        value = (dy[own, :, c].astype(F32) + wide[:, c].astype(BF16).astype(F32)).astype(BF16)
        d_res[:, c] = value
        f2[own, :, c] = value
    ag1.drain()
    ag3.start_far()
    ag3.start_near()
    steps = ag3.steps()
    last = steps.index(ag3.from_last)
    run(steps[:last])
    run(y_head[5:])
    run(y_tail[:2])
    run(steps[last:])
    ag3.finish(0)
    wide_attn = dot_nt(f2[:, :, left].reshape(TOKENS, HALF), wo[:, left])
    ag3.finish(1)
    d_attn[...] = (wide_attn + dot_nt(f2[:, :, right].reshape(TOKENS, HALF), wo[:, right])).astype(BF16)
    run(y_tail[2:5])
    for h in range(2):
        q, k, v = [qkv[:, pl.ds(h * 384 + i * LANES, LANES)] for i in range(3)]
        d_o = d_attn[:, pl.ds(h * LANES, LANES)]
        p = prob[h]
        d_prob = dot_nt(d_o, v)
        d_score = p * (d_prob - jnp.sum(p * d_prob, axis=-1, keepdims=True)) * SCALE
        dqkv[:, pl.ds(h * 384, LANES)] = dot_nn(d_score.astype(BF16), k).astype(BF16)
        dqkv[:, pl.ds(h * 384 + LANES, LANES)] = dot_nn(d_score.T.astype(BF16), q).astype(BF16)
        dqkv[:, pl.ds(h * 384 + TOKENS, LANES)] = dot_nn(p.T.astype(BF16), d_o).astype(BF16)
    run(y_tail[5:])
    rs3.drain()
    project(dqkv, wqkv, part1, HALF, True, 0, HALF)
    rs4.start(0)
    project(dqkv, wqkv, part1, HALF, True, HALF)

    rs4.start(1)
    run(rs4.head())
    tail = rs4.tail()
    run(tail[:3])
    rsy.finish()
    for j in range(CHUNKS):
        c = span(j)
        fy[own, :, c] = (x1[:, c].astype(F32) + rsy.total(j)).astype(BF16)
    run(tail[3:])
    agy.start_near()
    rs4.finish()
    mean1, rstd1 = row_stats(lambda j: x[own, :, span(j)].astype(F32))
    ln_backward(rs4, lambda j: x[own, :, span(j)].astype(F32), mean1, rstd1, g1, 0)
    for j in range(CHUNKS):
        c = span(j)
        fx[own, :, c] = (d_res[:, c].astype(F32) + wide[:, c].astype(BF16).astype(F32)).astype(BF16)
    dg_copies = []

    def dg_send(src, dst, i, dev):
        cp = pltpu.make_async_remote_copy(src_ref=src, dst_ref=dst, send_sem=dg_sems.at[0, i], recv_sem=dg_sems.at[1, i], device_id=dev, device_id_type=MESH)
        cp.start()
        dg_copies.append(cp)
        return cp
    in_core = dg_send(dg_part.at[pl.ds((1 - place.core) * 8, 8)], dg_core, 0, place.partner)
    ag3.drain()
    ag4.start_far()
    agy.start_far()
    ag4.start_near()
    steps = ag4.steps()
    near, far, end = agy.late_steps()
    last, mid = steps.index(ag4.from_last), steps.index(ag4.send_last)
    in_core.wait_recv()
    dg_core[...] = dg_core[...] + dg_part[pl.ds(place.core * 8, 8)]
    in_y = dg_send(dg_core.at[pl.ds((1 - place.y) * 4, 4)], dg_y, 6, place.y_peer)
    run(near)
    run(steps[:mid + 1])
    in_y.wait_recv()
    quarter = pl.ds(place.core * 8 + place.y * 4, 4)
    dg_z[place.z] = dg_core[pl.ds(place.y * 4, 4)] + dg_y[...]
    in_z = [dg_send(dg_z.at[place.z], dg_z.at[place.z], k, place.z_peers[k]) for k in (1, 2, 3)]
    run(steps[mid + 1:mid + 3])
    run(far)
    agy.send_last()
    run(steps[mid + 3:last - 2])
    run(end[:2 // 2])
    for cp in in_z:
        cp.wait_recv()
    dg_full[quarter] = dg_z[0] + dg_z[1] + dg_z[2] + dg_z[3]
    in_y = dg_send(dg_full.at[quarter], dg_full.at[quarter], 4, place.y_peer)
    run(steps[last - 2:last + 1])
    run(end[2 // 2:2 * 2])
    in_y.wait_recv()
    mine = pl.ds(place.core * 8, 8)
    in_core = dg_send(dg_full.at[mine], dg_full.at[mine], 5, place.partner)
    run(steps[last + 1:])
    in_core.wait_recv()
    for i in range(32):
        for row, out in ((0, dg1_out), (2, dg2_out)):
            out[pl.ds(i * LANES, LANES)] = dg_full[i // 2, row + i % 2].astype(BF16)
    ag4.finish()
    run(end[2 * 2:])
    agy.finish()

    for exchange in (rs4, ag4, rsy, agy):
        exchange.drain()
    for cp in dg_copies:
        cp.wait_send()


def layer(x_in, d_y, gain_one, gain_two, seg_ids, w_qkv, w_out, w_up, w_down):
    hbm = pl.BlockSpec(memory_space=pl.ANY)
    vmem = pl.BlockSpec(memory_space=pltpu.VMEM)
    dma = pltpu.SemaphoreType.DMA

    def shape(*dims):
        return pltpu.VMEM(dims, BF16)

    def scratch(*dims, dtype=BF16):
        return pltpu.VMEM(dims, dtype)
    blocks = (BLOCKS, BLOCKS, WIDTH)
    return pl.pallas_call(
        layer_kernel,
        out_shape=[
            shape(*blocks), shape(*blocks), shape(WIDTH), shape(WIDTH), shape(*blocks), shape(TOKENS, QKV_COLS), shape(TOKENS, TOKENS), shape(*blocks),
            shape(*blocks), shape(TOKENS, FFN), shape(TOKENS, FFN), shape(*blocks),
        ],
        in_specs=[hbm, hbm, vmem, vmem, vmem, hbm, hbm, hbm, hbm],
        out_specs=[vmem] * 12,
        scratch_shapes=[
            scratch(*blocks), scratch(WIDTH, QKV_COLS), scratch(TOKENS, WIDTH), scratch(WIDTH, FFN), scratch(FFN, WIDTH),
        ] + [scratch(*blocks)] * 3 + [
            scratch(2, 4, 2, BLOCKS, WIDTH), scratch(2, 4, BLOCKS, WIDTH), scratch(2, 4, BLOCKS, WIDTH), scratch(2, 3, BLOCKS, WIDTH), scratch(2, 3, BLOCKS, WIDTH),
            scratch(2, 2, BLOCKS, HALF), scratch(2, 2, BLOCKS, HALF),
            scratch(TOKENS, QKV_COLS), scratch(2, TOKENS, TOKENS, dtype=F32), scratch(TOKENS, FFN), scratch(TOKENS, FFN, dtype=F32), scratch(TOKENS, FFN),
            scratch(TOKENS, TOKENS), scratch(BLOCKS, WIDTH), scratch(BLOCKS, WIDTH), scratch(BLOCKS, WIDTH, dtype=F32),
            scratch(BLOCKS, 4, LANES, dtype=F32), scratch(8, 4, LANES, dtype=F32), scratch(4, 4, LANES, dtype=F32), scratch(4, 4, 4, LANES, dtype=F32),
            scratch(BLOCKS, 4, LANES, dtype=F32),
            dma((2, BLOCKS + 3 + 7 * ReduceScatter.pieces)), dma((2, 1 + BLOCKS * Gather.pieces)), dma((2, 7)), dma((12,)),
        ],
        compiler_params=pltpu.CompilerParams(collective_id=0, has_side_effects=True, vmem_limit_bytes=LAYER_VMEM),
        name='layer',
    )(
        x_in.reshape(blocks), d_y.reshape(blocks), gain_one, gain_two, seg_ids, w_qkv, w_out.reshape(TOKENS, WIDTH), w_up, w_down,
    )


TILE = 1024


def weight_grad_kernel(
    a, dqkv, o, dr, b1, du, gelu, dy, y, dx, dg1, dg2,
    dwqkv_hbm, dwo_hbm, dw1_hbm, dw2_hbm, y_out, dx_out, dg1_out, dg2_out,
    dwqkv, dwo, dw1, dw2, gelu_t, o_t, out_sems,
):
    stores = []

    def store(src, dst):
        cp = pltpu.make_async_copy(src, dst, out_sems.at[len(stores)])
        cp.start()
        stores.append(cp)

    def by_rows(lhs, rhs, out, out_hbm):
        for i in range(WIDTH // TILE):
            c = pl.ds(i * TILE, TILE)
            out[c, :] = lax.dot_general(lhs[:, c], rhs[...], (((0,), (0,)), ((), ())), preferred_element_type=F32).astype(BF16)
            store(out.at[c], out_hbm.at[c])

    def by_columns(lhs_t, rhs, out, out_hbm):
        for i in range(WIDTH // TILE):
            c = pl.ds(i * TILE, TILE)
            out[:, c] = dot_nn(lhs_t[...], rhs[:, c]).astype(BF16)
            store(out.at[:, c], out_hbm.at[:, c])

    store(y, y_out)
    store(dx, dx_out)
    store(dg1, dg1_out)
    store(dg2, dg2_out)
    by_rows(a, dqkv, dwqkv, dwqkv_hbm)
    by_rows(b1, du, dw1, dw1_hbm)
    gelu_t[...] = gelu[...].T
    by_columns(gelu_t, dy, dw2, dw2_hbm)
    o_t[...] = o[...].T
    by_columns(o_t, dr, dwo, dwo_hbm)
    for cp in stores:
        cp.wait()


def weight_grads(*operands):
    hbm = pl.BlockSpec(memory_space=pl.ANY)
    vmem = pl.BlockSpec(memory_space=pltpu.VMEM)
    big = (TOKENS, WIDTH)
    ins = [big, (TOKENS, QKV_COLS), (TOKENS, TOKENS), big, big, (TOKENS, FFN), (TOKENS, FFN), big, big, big, (WIDTH,), (WIDTH,)]
    outs = [(WIDTH, QKV_COLS), big, (WIDTH, FFN), (FFN, WIDTH), big, big, (WIDTH,), (WIDTH,)]
    return pl.pallas_call(
        weight_grad_kernel,
        out_shape=[jax.ShapeDtypeStruct(dims, BF16) for dims in outs],
        in_specs=[vmem] * len(ins),
        out_specs=[hbm] * len(outs),
        scratch_shapes=[pltpu.VMEM(dims, BF16) for dims in outs[:4] + [(FFN, TOKENS), (TOKENS, TOKENS)]] + [pltpu.SemaphoreType.DMA((20,))],
        compiler_params=pltpu.CompilerParams(vmem_limit_bytes=GRADS_VMEM),
        name='weight_grads',
    )(*[v.reshape(dims) for v, dims in zip(operands, ins)])


def solution(mesh):
    def local_step(x_in, seg_ids, gain_one, w_qkv, w_out, gain_two, w_up, w_down, d_y):
        y, d_x, gains_one, gains_two, normed_one, d_qkv, attn_out, d_resid, normed_two, d_up, gelu_out, d_y_here = layer(
            x_in, d_y, gain_one, gain_two, seg_ids, w_qkv, w_out, w_up, w_down)
        d_w_qkv, d_w_out, d_w_up, d_w_down, y_out, d_x_out, d_gain_one, d_gain_two = weight_grads(
            normed_one, d_qkv, attn_out, d_resid, normed_two, d_up, gelu_out, d_y_here, y, d_x, gains_one, gains_two)
        return y_out.reshape(x_in.shape), d_x_out.reshape(x_in.shape), d_w_qkv, d_w_out.reshape(w_out.shape), d_w_up, d_w_down, d_gain_one, d_gain_two

    in_specs = (P('data'), P('data'), P(), P(None, 'model'), P('model'), P(), P(None, 'model'), P('model'), P('data'))
    out_specs = (P('data'), P('data'), P('data', 'model'), P(('data', 'model')), P('data', 'model'), P(('data', 'model')), P('data'), P('data'))
    return jax.shard_map(local_step, mesh=mesh, in_specs=in_specs, out_specs=out_specs, check_vma=False)
```

```python
import jax
import jax.numpy as jnp
from jax import lax
from jax.experimental import pallas as pl
from jax.experimental.pallas import tpu as pltpu
from jax.sharding import PartitionSpec as P

LN_EPS = 1e-5
MESH = pl.DeviceIdType.MESH
BF16 = jnp.bfloat16
F32 = jnp.float32
WIDTH = 4096
CHUNK = 512
LAYER_VMEM = 49 * 2 ** 20
GRADS_VMEM = 28 * 2 ** 20
TOKENS = 256
LANES = 128
BLOCKS = 16
FFN = 896
QKV_COLS = 768
CHUNKS = WIDTH // CHUNK
HALF = WIDTH // 2
CORE_ORDER = [(3, 1), (1, 1), (1, 0), (2, 1), (3, 0), (0, 1), (2, 0), (0, 0)]
SCALE = LANES ** -0.5
GELU_A = 0.7978845608028654
GELU_B = 0.044715


def flip(z, k):
    high, low = lax.div(z, 2), lax.rem(z, 2)
    return (1 - high if k >= 2 else high) * 2 + (1 - low if k % 2 else low)


def dot_nn(a, b):
    return jnp.dot(a, b, preferred_element_type=F32)


def dot_nt(a, b):
    return lax.dot_general(a, b, (((1,), (1,)), ((), ())), preferred_element_type=F32)


def span(j):
    return pl.ds(j * CHUNK, CHUNK)


class Exchange:
    pieces = 2

    def __init__(self, place, sems):
        self.place, self.sems = place, sems
        self.all = range(self.pieces)
        self.low, self.high = self.all[:self.pieces // 2], self.all[self.pieces // 2:]
        self.width = WIDTH // self.pieces

    def piece(self, h):
        return pl.ds(h * self.width, self.width)

    def spans(self, h):
        n = CHUNKS // self.pieces
        return [span(h * n + j) for j in range(n)]

    def remote(self, src, dst, i, dev):
        cp = pltpu.make_async_remote_copy(src_ref=src, dst_ref=dst, send_sem=self.sems.at[0], recv_sem=self.sems.at[1 + i], device_id=dev, device_id_type=MESH)
        cp.start()
        return cp

    def drain(self):
        sent = self.whole.at[pl.ds(0, BLOCKS - 1)]
        pltpu.make_async_copy(sent, sent, self.sems.at[0]).wait()


def fold(v):
    return sum(v[..., i * LANES:(i + 1) * LANES] for i in range(CHUNK // LANES))


def row_stats(wide):
    total = sum(fold(wide(j)) for j in range(CHUNKS))
    mean = jnp.sum(total, axis=-1, keepdims=True) / WIDTH

    def square(j):
        centered = wide(j) - mean
        return fold(centered * centered)
    total = sum(square(j) for j in range(CHUNKS))
    var = jnp.sum(total, axis=-1, keepdims=True) / WIDTH
    return mean, lax.rsqrt(var + LN_EPS)


class Place:
    def __init__(self):
        me = lax.axis_index('model')
        self.core, self.y, self.z = lax.rem(me, 2), lax.rem(lax.div(me, 2), 2), lax.div(me, 4)
        self.partner = {'model': me + 1 - 2 * self.core}
        self.y_peer = {'model': me + 2 - 4 * self.y}
        self.z_at = [flip(self.z, k) for k in range(4)]
        self.z_peers = [{'model': me + (at - self.z) * 4} for at in self.z_at]
        self.blocks = {
            (i, j, k): (1 - self.core if i else self.core) * 8 + (1 - self.y if j else self.y) * 4 + self.z_at[k]
            for i in (0, 1) for j in (0, 1) for k in range(4)
        }
        self.own = self.blocks[0, 0, 0]

    def block(self, i, j, k):
        return self.blocks[i, j, k]


class ReduceScatter(Exchange):
    def __init__(self, place, part, bufs, sems):
        super().__init__(place, sems)
        self.part = self.whole = part
        self.buf_core, self.out_y, self.buf_y, self.out_z, self.buf_z, self.out_first, self.buf_first = bufs
        self.core_in, self.y_in, self.z_in, self.first_in = {}, {}, {}, {}
        self.ready, self.first_ready = set(), False

    def block(self, k, j):
        return self.place.block(0, j, k)

    def start(self, h):
        p = self.place
        for k, j in CORE_ORDER:
            b = p.block(1, j, k)
            self.core_in[k, j, h] = self.remote(self.part.at[b, :, self.piece(h)], self.buf_core.at[k, j, :, self.piece(h)], (k * 2 + j) * 2 + h, p.partner)

    def core_ready(self, k, j, h):
        if (k, j, h) not in self.ready:
            self.core_in[k, j, h].wait_recv()
            self.ready.add((k, j, h))

    def pair_sum(self, k, j, c):
        return self.part[self.block(k, j), :, c].astype(F32) + self.buf_core[k, j, :, c].astype(F32)

    def chip_sum(self, k, c):
        return self.pair_sum(k, 0, c) + self.buf_y[k, :, c].astype(F32)

    def send_y(self, k, h):
        self.core_ready(k, 1, h)
        with_first = k == 0 and h in self.high
        if with_first and not self.first_ready:
            self.first_in[1].wait_recv()
            self.first_ready = True
        for c in self.spans(h):
            t = self.pair_sum(k, 1, c)
            if with_first:
                t = t + self.buf_first[1, :, pl.ds(c.start - HALF, CHUNK)].astype(F32)
            self.out_y[k, :, c] = t.astype(BF16)
        self.y_in[k, h] = self.remote(self.out_y.at[k, :, self.piece(h)], self.buf_y.at[k, :, self.piece(h)], BLOCKS + k * self.pieces + h, self.place.y_peer)

    def send_first(self):
        for j in (1, 0):
            self.core_ready(1, j, 1)
            for j2 in range(CHUNKS // 2):
                self.out_first[j, :, span(j2)] = self.pair_sum(1, j, span(CHUNKS // 2 + j2)).astype(BF16)
            self.first_in[j] = self.remote(self.out_first.at[j], self.buf_first.at[j], BLOCKS + 7 * self.pieces + j, self.place.z_peers[1])

    def send_z(self, k, h):
        self.core_ready(k, 0, h)
        self.y_in[k, h].wait_recv()
        if k == 2:
            self.z_in[3, h].wait_recv()
        for c in self.spans(h):
            t = self.chip_sum(k, c)
            if k == 2:
                t = t + self.buf_z[2, :, c].astype(F32)
            self.out_z[k - 1, :, c] = t.astype(BF16)
        i = BLOCKS + (3 + k) * self.pieces + h
        self.z_in[k, h] = self.remote(self.out_z.at[k - 1, :, self.piece(h)], self.buf_z.at[k - 1, :, self.piece(h)], i, self.place.z_peers[2 if k == 2 else 1])

    def head(self):
        y = {(k, h): (lambda k=k, h=h: self.send_y(k, h)) for k in range(4) for h in self.all}
        return [y[3, 0], y[3, 1], self.send_first, y[2, 0], y[2, 1], y[1, 0], y[0, 0]]

    def tail(self):
        z = {(k, h): (lambda k=k, h=h: self.send_z(k, h)) for k in range(4) for h in self.all}
        return [z[3, 0], z[3, 1], lambda: self.send_y(0, 1), z[2, 0], z[2, 1], z[1, 0]]

    def finish(self):
        for h in self.all:
            self.core_ready(0, 0, h)
            self.y_in[0, h].wait_recv()
        self.first_in[0].wait_recv()
        for h in self.low:
            self.z_in[1, h].wait_recv()
        for h in self.all:
            self.z_in[2, h].wait_recv()

    def total(self, j):
        c = span(j)
        near = self.buf_z[0, :, c] if j < CHUNKS // 2 else self.buf_first[0, :, span(j - CHUNKS // 2)]
        return self.chip_sum(0, c) + near.astype(F32) + self.buf_z[1, :, c].astype(F32)


class Gather(Exchange):
    def __init__(self, place, full, sems):
        super().__init__(place, sems)
        self.full = self.whole = full
        self.z_in, self.y_in, self.core_in, self.last_in = {}, {}, {}, {}

    def send(self, j, k, h, i, dev):
        b = self.place.block(0, j, k)
        ref = self.full.at[b] if h is None else self.full.at[b, :, self.piece(h)]
        return self.remote(ref, ref, i, dev)

    def to_core(self, j, k, h):
        self.core_in[j, k, h] = self.send(j, k, h, (8 + j * 4 + k) * self.pieces + h, self.place.partner)

    def to_y(self, k, h):
        self.y_in[k, h] = self.send(0, k, h, (4 + k) * self.pieces + h, self.place.y_peer)

    def to_z(self, k, h):
        self.z_in[k, h] = self.send(0, 2 if k == 3 else 0, h, k * self.pieces + h, self.place.z_peers[2 if k == 2 else 1])

    def start_far(self):
        for h in self.all:
            self.to_z(2, h)

    def start_near(self):
        for h in self.all:
            self.to_y(0, h)
            self.to_z(1, h)
        self.core_in[0, 0, None] = self.send(0, 0, None, 8 * self.pieces, self.place.partner)

    def from_z(self, k, h):
        self.z_in[k, h].wait_recv()
        if k == 2:
            self.to_z(3, h)
        if k != 1 or h in self.low:
            self.to_y(k, h)
        self.to_core(0, k, h)

    def from_y(self, k, h):
        self.y_in[k, h].wait_recv()
        self.to_core(1, k, h)

    def send_last(self):
        for h in self.high:
            self.last_in[h] = self.send(1, 0, h, h - self.pieces // 2, self.place.z_peers[1])

    def from_last(self):
        for h in self.high:
            self.last_in[h].wait_recv()
            self.to_core(1, 1, h)

    def steps(self):
        y = {(k, h): (lambda k=k, h=h: self.from_y(k, h)) for k in range(4) for h in self.all}
        z = {(k, h): (lambda k=k, h=h: self.from_z(k, h)) for k in range(4) for h in self.all}
        return [
            y[0, 0], z[2, 0], y[0, 1], z[2, 1], self.send_last, z[1, 0], z[1, 1], y[2, 0], y[2, 1], z[3, 0],
            y[1, 0], z[3, 1], self.from_last, y[3, 0], y[3, 1],
        ]

    def late_steps(self):
        near = [(lambda h=h: self.from_y(0, h)) for h in self.all] + [(lambda h=h: self.from_z(1, h)) for h in self.all]
        far = [(lambda h=h: self.from_z(2, h)) for h in self.all]
        end = [(lambda h=h: self.from_y(1, h)) for h in self.low] + [(lambda h=h: self.from_z(3, h)) for h in self.all]
        end += [(lambda h=h: self.from_y(2, h)) for h in self.all] + [self.from_last] + [(lambda h=h: self.from_y(3, h)) for h in self.all]
        return near, far, end

    def finish(self, h=None):
        for (_, _, at), cp in self.core_in.items():
            if h is None or (at or 0) == h:
                cp.wait_recv()


def run(steps):
    for step in steps:
        step()


def layer_kernel(
    x_hbm, dy_hbm, g1, g2, seg, wqkv_hbm, wo_hbm, w1_hbm, w2_hbm,
    fy, fx, dg1_out, dg2_out, a, dqkv, o, f2, f1, d_up, gelu, dy,
    x, wqkv, wo, w1, w2, part1, part3, part_y,
    core_buf, yout_buf, y_buf, zout_buf, z_buf, fout_buf, first_buf,
    qkv, prob, up, wide_up, d_gelu, d_attn, x1, d_res, wide, dg_part, dg_core, dg_y, dg_z, dg_full,
    rs_sems, ag_sems, dg_sems, in_sems,
):
    place = Place()
    own = place.own

    loads = [
        pltpu.make_async_copy(src, dst, in_sems.at[i])
        for i, (src, dst) in enumerate(
            [(x_hbm.at[pl.ds(r * 4, 4)], x.at[pl.ds(r * 4, 4)]) for r in range(4)]
            + [(wqkv_hbm.at[pl.ds(r * 1024, 1024)], wqkv.at[pl.ds(r * 1024, 1024)]) for r in range(4)]
            + [(wo_hbm, wo), (dy_hbm, dy), (w2_hbm, w2), (w1_hbm, w1)])
    ]
    load_x, load_wqkv, (load_wo, load_dy, load_w2, load_w1) = loads[:4], loads[4:8], loads[8:]
    for cp in load_x + load_wqkv:
        cp.start()
    barrier = pltpu.get_barrier_semaphore()
    for dev in [place.partner, place.y_peer] + place.z_peers[1:]:
        pl.semaphore_signal(barrier, inc=1, device_id=dev, device_id_type=MESH)

    def rs_set(i, part):
        bufs = [ref.at[i] for ref in (core_buf, yout_buf, y_buf, zout_buf, z_buf, fout_buf, first_buf)]
        return ReduceScatter(place, part, bufs, rs_sems.at[i])

    rs1, rs3, rsy, rs4 = rs_set(0, part1), rs_set(0, part3), rs_set(1, part_y), rs_set(0, part1)
    ag1, ag3, agy, ag4 = [Gather(place, ref, ag_sems.at[i]) for i, ref in ((0, f1), (0, f2), (1, fy), (0, fx))]

    def gain(ref, j):
        return ref[span(j)].astype(F32).reshape(1, CHUNK)

    def ln_one(i):
        rows = pl.ds(i * 4, 4)
        mean, rstd = row_stats(lambda j: x[rows, :, span(j)].astype(F32))
        for j in range(CHUNKS):
            c = span(j)
            normed = (x[rows, :, c].astype(F32) - mean) * rstd * gain(g1, j)[None]
            a[rows, :, c] = normed.astype(BF16)
    for r in range(4):
        load_x[r].wait()
        ln_one(r)
    for cp in (load_wo, load_dy, load_w2, load_w1):
        cp.start()

    left, right = pl.ds(0, HALF), pl.ds(HALF, HALF)
    for cp in load_wqkv[:2]:
        cp.wait()
    wide_up[:, pl.ds(0, QKV_COLS)] = dot_nn(a[:, :, left].reshape(TOKENS, HALF), wqkv[left, :])
    for cp in load_wqkv[2:]:
        cp.wait()
    qkv[...] = (wide_up[:, pl.ds(0, QKV_COLS)] + dot_nn(a[:, :, right].reshape(TOKENS, HALF), wqkv[right, :])).astype(BF16)

    q_pos = lax.broadcasted_iota(jnp.int32, (TOKENS, TOKENS), 0)
    k_pos = lax.broadcasted_iota(jnp.int32, (TOKENS, TOKENS), 1)
    seg_keys = jnp.broadcast_to(seg[...].astype(F32), (TOKENS, TOKENS))
    allowed = (q_pos >= k_pos) & (seg_keys.T == seg_keys)
    for h in range(2):
        q, k, v = [qkv[:, pl.ds(h * 384 + i * LANES, LANES)] for i in range(3)]
        scores = jnp.where(allowed, dot_nt(q, k) * SCALE, -1e30)
        exp_scores = jnp.exp(scores - jnp.max(scores, axis=-1, keepdims=True))
        p = exp_scores / jnp.sum(exp_scores, axis=-1, keepdims=True)
        prob[h] = p
        o[:, pl.ds(h * LANES, LANES)] = dot_nn(p.astype(BF16), v).astype(BF16)

    def project(lhs, weight, part, tile, transposed, lo=0, hi=WIDTH):
        def step(i, carry):
            c = pl.ds(pl.multiple_of(lo + i * tile, tile), tile)
            r = dot_nt(lhs[...], weight[c, :]) if transposed else dot_nn(lhs[...], weight[:, c])
            part[:, :, c] = r.astype(BF16).reshape(BLOCKS, BLOCKS, tile)
            return carry
        lax.fori_loop(0, (hi - lo) // tile, step, 0)

    load_wo.wait()
    pl.semaphore_wait(barrier, 5)
    project(o, wo, part1, HALF, False, 0, HALF)
    rs1.start(0)
    project(o, wo, part1, HALF, False, HALF)

    rs1.start(1)
    run(rs1.head())

    def d_gelu_tile(lo, n):
        c = pl.ds(lo, n)
        d_gelu[:, c] = dot_nt(dy[...].reshape(TOKENS, WIDTH), w2[c, :]).astype(BF16)
    load_dy.wait()
    load_w2.wait()
    tail = rs1.tail()
    d_gelu_tile(0, TOKENS)
    d_gelu_tile(TOKENS, TOKENS)
    run(tail[:3])
    d_gelu_tile(512, TOKENS)
    run(tail[3:])
    d_gelu_tile(QKV_COLS, LANES)
    rs1.finish()

    for j in range(CHUNKS):
        c = span(j)
        x1[:, c] = (x[own, :, c].astype(F32) + rs1.total(j)).astype(BF16)
    mean2, rstd2 = row_stats(lambda j: x1[:, span(j)].astype(F32))
    for j in range(CHUNKS):
        c = span(j)
        f1[own, :, c] = ((x1[:, c].astype(F32) - mean2) * rstd2 * gain(g2, j)).astype(BF16)
    ag1.start_far()
    ag1.start_near()
    run(ag1.steps())
    load_w1.wait()
    ag1.finish(0)
    wide_up[...] = dot_nn(f1[:, :, left].reshape(TOKENS, HALF), w1[left, :])
    ag1.finish(1)
    rs1.drain()
    up[...] = (wide_up[...] + dot_nn(f1[:, :, right].reshape(TOKENS, HALF), w1[right, :])).astype(BF16)

    def activation(i, carry):
        rows = pl.ds(pl.multiple_of(i * 32, 32), 32)
        u = up[rows, :].astype(F32)
        t = jnp.tanh(GELU_A * (u + GELU_B * (u * u * u)))
        gelu[rows, :] = (0.5 * u * (1.0 + t)).astype(BF16)
        slope = 0.5 * (1.0 + t) + 0.5 * u * (1.0 - t * t) * (GELU_A * (1.0 + 3.0 * GELU_B * (u * u)))
        d_up[rows, :] = (d_gelu[rows, :].astype(F32) * slope).astype(BF16)
        return carry
    lax.fori_loop(0, 8, activation, 0)
    project(d_up, w1, part3, HALF, True, 0, HALF)
    rs3.start(0)
    project(d_up, w1, part3, HALF, True, HALF)

    rs3.start(1)
    run(rs3.head())
    tail, y_head, y_tail = rs3.tail(), rsy.head(), rsy.tail()
    project(gelu, w2, part_y, HALF, False, 0, HALF)
    rsy.start(0)
    project(gelu, w2, part_y, HALF, False, HALF)
    rsy.start(1)
    run(tail[:5])
    run(y_head[:2])
    run(tail[5:])
    run(y_head[2:6])
    rs3.finish()

    def ln_backward(rs, z, mean, rstd, gain_ref, dg_row):
        sum_a = jnp.zeros((BLOCKS, LANES), F32)
        sum_b = jnp.zeros((BLOCKS, LANES), F32)
        for j in range(CHUNKS):
            d_norm = rs.total(j).astype(BF16).astype(F32)
            x_hat = (z(j) - mean) * rstd
            grad_row = jnp.sum(d_norm * x_hat, axis=0, keepdims=True)
            for i in range(CHUNK // LANES):
                at = j * (CHUNK // LANES) + i
                dg_part[at // 2, pl.ds(dg_row + at % 2, 1), :] = grad_row[:, i * LANES:(i + 1) * LANES]
            scaled = d_norm * gain(gain_ref, j)
            wide[:, span(j)] = scaled
            sum_a = sum_a + fold(scaled)
            sum_b = sum_b + fold(scaled * x_hat)
        mean_a = jnp.sum(sum_a, axis=-1, keepdims=True) / WIDTH
        mean_b = jnp.sum(sum_b, axis=-1, keepdims=True) / WIDTH
        for j in range(CHUNKS):
            c = span(j)
            x_hat = (z(j) - mean) * rstd
            wide[:, c] = rstd * (wide[:, c] - mean_a - x_hat * mean_b)

    ln_backward(rs3, lambda j: x1[:, span(j)].astype(F32), mean2, rstd2, g2, 2)
    for j in range(CHUNKS):
        c = span(j)
        value = (dy[own, :, c].astype(F32) + wide[:, c].astype(BF16).astype(F32)).astype(BF16)
        d_res[:, c] = value
        f2[own, :, c] = value
    ag1.drain()
    ag3.start_far()
    ag3.start_near()
    steps = ag3.steps()
    last = steps.index(ag3.from_last)
    run(steps[:last])
    run(y_head[6:])
    run(y_tail[:2])
    run(steps[last:])
    ag3.finish(0)
    wide_attn = dot_nt(f2[:, :, left].reshape(TOKENS, HALF), wo[:, left])
    ag3.finish(1)
    d_attn[...] = (wide_attn + dot_nt(f2[:, :, right].reshape(TOKENS, HALF), wo[:, right])).astype(BF16)
    run(y_tail[2:5])
    for h in range(2):
        q, k, v = [qkv[:, pl.ds(h * 384 + i * LANES, LANES)] for i in range(3)]
        d_o = d_attn[:, pl.ds(h * LANES, LANES)]
        p = prob[h]
        d_prob = dot_nt(d_o, v)
        d_score = p * (d_prob - jnp.sum(p * d_prob, axis=-1, keepdims=True)) * SCALE
        dqkv[:, pl.ds(h * 384, LANES)] = dot_nn(d_score.astype(BF16), k).astype(BF16)
        dqkv[:, pl.ds(h * 384 + LANES, LANES)] = dot_nn(d_score.T.astype(BF16), q).astype(BF16)
        dqkv[:, pl.ds(h * 384 + TOKENS, LANES)] = dot_nn(p.T.astype(BF16), d_o).astype(BF16)
    run(y_tail[5:])
    rs3.drain()
    project(dqkv, wqkv, part1, HALF, True, 0, HALF)
    rs4.start(0)
    project(dqkv, wqkv, part1, HALF, True, HALF)

    rs4.start(1)
    run(rs4.head())
    tail = rs4.tail()
    run(tail[:3])
    rsy.finish()
    for j in range(CHUNKS):
        c = span(j)
        fy[own, :, c] = (x1[:, c].astype(F32) + rsy.total(j)).astype(BF16)
    run(tail[3:])
    agy.start_near()
    rs4.finish()
    mean1, rstd1 = row_stats(lambda j: x[own, :, span(j)].astype(F32))
    ln_backward(rs4, lambda j: x[own, :, span(j)].astype(F32), mean1, rstd1, g1, 0)
    for j in range(CHUNKS):
        c = span(j)
        fx[own, :, c] = (d_res[:, c].astype(F32) + wide[:, c].astype(BF16).astype(F32)).astype(BF16)
    dg_copies = []

    def dg_send(src, dst, i, dev):
        cp = pltpu.make_async_remote_copy(src_ref=src, dst_ref=dst, send_sem=dg_sems.at[0, i], recv_sem=dg_sems.at[1, i], device_id=dev, device_id_type=MESH)
        cp.start()
        dg_copies.append(cp)
        return cp
    in_core = dg_send(dg_part.at[pl.ds((1 - place.core) * 8, 8)], dg_core, 0, place.partner)
    ag3.drain()
    ag4.start_far()
    agy.start_far()
    ag4.start_near()
    steps = ag4.steps()
    near, far, end = agy.late_steps()
    last, mid = steps.index(ag4.from_last), steps.index(ag4.send_last)
    in_core.wait_recv()
    dg_core[...] = dg_core[...] + dg_part[pl.ds(place.core * 8, 8)]
    in_y = dg_send(dg_core.at[pl.ds((1 - place.y) * 4, 4)], dg_y, 6, place.y_peer)
    run(near)
    run(steps[:mid + 1])
    in_y.wait_recv()
    quarter = pl.ds(place.core * 8 + place.y * 4, 4)
    dg_z[place.z] = dg_core[pl.ds(place.y * 4, 4)] + dg_y[...]
    in_z = [dg_send(dg_z.at[place.z], dg_z.at[place.z], k, place.z_peers[k]) for k in (1, 2, 3)]
    run(steps[mid + 1:mid + 3])
    run(far)
    agy.send_last()
    run(steps[mid + 3:last - 2])
    run(end[:2 // 2])
    for cp in in_z:
        cp.wait_recv()
    dg_full[quarter] = dg_z[0] + dg_z[1] + dg_z[2] + dg_z[3]
    in_y = dg_send(dg_full.at[quarter], dg_full.at[quarter], 4, place.y_peer)
    run(steps[last - 2:last + 1])
    run(end[2 // 2:2 * 2])
    in_y.wait_recv()
    mine = pl.ds(place.core * 8, 8)
    in_core = dg_send(dg_full.at[mine], dg_full.at[mine], 5, place.partner)
    run(steps[last + 1:])
    run(end[2 * 2:])
    in_core.wait_recv()
    for i in range(32):
        for row, out in ((0, dg1_out), (2, dg2_out)):
            out[pl.ds(i * LANES, LANES)] = dg_full[i // 2, row + i % 2].astype(BF16)
    ag4.finish()
    agy.finish()

    for exchange in (rs4, ag4, rsy, agy):
        exchange.drain()
    for cp in dg_copies:
        cp.wait_send()


def layer(x_in, d_y, gain_one, gain_two, seg_ids, w_qkv, w_out, w_up, w_down):
    hbm = pl.BlockSpec(memory_space=pl.ANY)
    vmem = pl.BlockSpec(memory_space=pltpu.VMEM)
    dma = pltpu.SemaphoreType.DMA

    def shape(*dims):
        return pltpu.VMEM(dims, BF16)

    def scratch(*dims, dtype=BF16):
        return pltpu.VMEM(dims, dtype)
    blocks = (BLOCKS, BLOCKS, WIDTH)
    return pl.pallas_call(
        layer_kernel,
        out_shape=[
            shape(*blocks), shape(*blocks), shape(WIDTH), shape(WIDTH), shape(*blocks), shape(TOKENS, QKV_COLS), shape(TOKENS, TOKENS), shape(*blocks),
            shape(*blocks), shape(TOKENS, FFN), shape(TOKENS, FFN), shape(*blocks),
        ],
        in_specs=[hbm, hbm, vmem, vmem, vmem, hbm, hbm, hbm, hbm],
        out_specs=[vmem] * 12,
        scratch_shapes=[
            scratch(*blocks), scratch(WIDTH, QKV_COLS), scratch(TOKENS, WIDTH), scratch(WIDTH, FFN), scratch(FFN, WIDTH),
        ] + [scratch(*blocks)] * 3 + [
            scratch(2, 4, 2, BLOCKS, WIDTH), scratch(2, 4, BLOCKS, WIDTH), scratch(2, 4, BLOCKS, WIDTH), scratch(2, 3, BLOCKS, WIDTH), scratch(2, 3, BLOCKS, WIDTH),
            scratch(2, 2, BLOCKS, HALF), scratch(2, 2, BLOCKS, HALF),
            scratch(TOKENS, QKV_COLS), scratch(2, TOKENS, TOKENS, dtype=F32), scratch(TOKENS, FFN), scratch(TOKENS, FFN, dtype=F32), scratch(TOKENS, FFN),
            scratch(TOKENS, TOKENS), scratch(BLOCKS, WIDTH), scratch(BLOCKS, WIDTH), scratch(BLOCKS, WIDTH, dtype=F32),
            scratch(BLOCKS, 4, LANES, dtype=F32), scratch(8, 4, LANES, dtype=F32), scratch(4, 4, LANES, dtype=F32), scratch(4, 4, 4, LANES, dtype=F32),
            scratch(BLOCKS, 4, LANES, dtype=F32),
            dma((2, BLOCKS + 3 + 7 * ReduceScatter.pieces)), dma((2, 1 + BLOCKS * Gather.pieces)), dma((2, 7)), dma((12,)),
        ],
        compiler_params=pltpu.CompilerParams(collective_id=0, has_side_effects=True, vmem_limit_bytes=LAYER_VMEM),
        name='layer',
    )(
        x_in.reshape(blocks), d_y.reshape(blocks), gain_one, gain_two, seg_ids, w_qkv, w_out.reshape(TOKENS, WIDTH), w_up, w_down,
    )


TILE = 1024


def weight_grad_kernel(
    a, dqkv, o, dr, b1, du, gelu, dy, y, dx, dg1, dg2,
    dwqkv_hbm, dwo_hbm, dw1_hbm, dw2_hbm, y_out, dx_out, dg1_out, dg2_out,
    dwqkv, dwo, dw1, dw2, gelu_t, o_t, out_sems,
):
    stores = []

    def store(src, dst):
        cp = pltpu.make_async_copy(src, dst, out_sems.at[len(stores)])
        cp.start()
        stores.append(cp)

    def by_rows(lhs, rhs, out, out_hbm):
        for i in range(WIDTH // TILE):
            c = pl.ds(i * TILE, TILE)
            out[c, :] = lax.dot_general(lhs[:, c], rhs[...], (((0,), (0,)), ((), ())), preferred_element_type=F32).astype(BF16)
            store(out.at[c], out_hbm.at[c])

    def by_columns(lhs_t, rhs, out, out_hbm):
        for i in range(WIDTH // TILE):
            c = pl.ds(i * TILE, TILE)
            out[:, c] = dot_nn(lhs_t[...], rhs[:, c]).astype(BF16)
            store(out.at[:, c], out_hbm.at[:, c])

    store(y, y_out)
    store(dx, dx_out)
    store(dg1, dg1_out)
    store(dg2, dg2_out)
    by_rows(a, dqkv, dwqkv, dwqkv_hbm)
    by_rows(b1, du, dw1, dw1_hbm)
    gelu_t[...] = gelu[...].T
    by_columns(gelu_t, dy, dw2, dw2_hbm)
    o_t[...] = o[...].T
    by_columns(o_t, dr, dwo, dwo_hbm)
    for cp in stores:
        cp.wait()


def weight_grads(*operands):
    hbm = pl.BlockSpec(memory_space=pl.ANY)
    vmem = pl.BlockSpec(memory_space=pltpu.VMEM)
    big = (TOKENS, WIDTH)
    ins = [big, (TOKENS, QKV_COLS), (TOKENS, TOKENS), big, big, (TOKENS, FFN), (TOKENS, FFN), big, big, big, (WIDTH,), (WIDTH,)]
    outs = [(WIDTH, QKV_COLS), big, (WIDTH, FFN), (FFN, WIDTH), big, big, (WIDTH,), (WIDTH,)]
    return pl.pallas_call(
        weight_grad_kernel,
        out_shape=[jax.ShapeDtypeStruct(dims, BF16) for dims in outs],
        in_specs=[vmem] * len(ins),
        out_specs=[hbm] * len(outs),
        scratch_shapes=[pltpu.VMEM(dims, BF16) for dims in outs[:4] + [(FFN, TOKENS), (TOKENS, TOKENS)]] + [pltpu.SemaphoreType.DMA((20,))],
        compiler_params=pltpu.CompilerParams(vmem_limit_bytes=GRADS_VMEM),
        name='weight_grads',
    )(*[v.reshape(dims) for v, dims in zip(operands, ins)])


def solution(mesh):
    def local_step(x_in, seg_ids, gain_one, w_qkv, w_out, gain_two, w_up, w_down, d_y):
        y, d_x, gains_one, gains_two, normed_one, d_qkv, attn_out, d_resid, normed_two, d_up, gelu_out, d_y_here = layer(
            x_in, d_y, gain_one, gain_two, seg_ids, w_qkv, w_out, w_up, w_down)
        d_w_qkv, d_w_out, d_w_up, d_w_down, y_out, d_x_out, d_gain_one, d_gain_two = weight_grads(
            normed_one, d_qkv, attn_out, d_resid, normed_two, d_up, gelu_out, d_y_here, y, d_x, gains_one, gains_two)
        return y_out.reshape(x_in.shape), d_x_out.reshape(x_in.shape), d_w_qkv, d_w_out.reshape(w_out.shape), d_w_up, d_w_down, d_gain_one, d_gain_two

    in_specs = (P('data'), P('data'), P(), P(None, 'model'), P('model'), P(), P(None, 'model'), P('model'), P('data'))
    out_specs = (P('data'), P('data'), P('data', 'model'), P(('data', 'model')), P('data', 'model'), P(('data', 'model')), P('data'), P('data'))
    return jax.shard_map(local_step, mesh=mesh, in_specs=in_specs, out_specs=out_specs, check_vma=False)
```
